8 devices in a mesh: dp: 1 (over z), ty: 2 (over y), tx: 4 (over x, core).
Axes of the slice: x: 2, y: 2, z: 1, core: 2. Of those that a mesh axis runs over, the one named last changes fastest.
Arguments:
- x_in: bfloat16 [2, 64, 5120], P(('dp', 'ty'), None, 'tx')
- w_q: bfloat16 [5120, 5120], P('tx', 'ty')
- w_k: bfloat16 [5120, 5120], P('tx', 'ty')
- w_v: bfloat16 [5120, 5120], P('tx', 'ty')
- w_o: bfloat16 [5120, 5120], P('ty', 'tx')
- w_gate: bfloat16 [5120, 13824], P('tx', 'ty')
- w_up: bfloat16 [5120, 13824], P('tx', 'ty')
- w_down: bfloat16 [13824, 5120], P('ty', 'tx')
Outputs:
- output: bfloat16 [2, 64, 5120], P(('dp', 'ty'), None, 'tx')
All inputs are finite; a program needn't handle non-finite values.
Results may differ from the reference program's by a relative error of at most 0.0197486.
Values are sent between devices in bfloat16 or wider.
A program may use at most 1 GiB of HBM per device.

```python
import jax
import jax.numpy as jnp
from jax import lax

NSEQ = 2
SEQ = 64
D = 5120
FF = 13824
HEADS = 40

HEAD_DIM = D // HEADS
EPS = 1e-5
THETA = 10000.0


def setup_inputs(seed: int = 0, part: int = 0) -> dict:
    root_key = jax.random.key(seed)
    act_root, weight_root = jax.random.split(root_key)
    part_key = jax.random.fold_in(act_root, part)
    key_tok, key_scale, key_shift, key_slope, key_walk = jax.random.split(part_key, 5)
    tok_noise = jax.random.normal(key_tok, (NSEQ, SEQ, D), jnp.float32)
    tok_scale = jax.random.uniform(key_scale, (NSEQ, SEQ, 1), jnp.float32, 0.5, 2.0)
    tok_shift = 0.5 * jax.random.normal(key_shift, (NSEQ, SEQ, 1), jnp.float32)
    col_slope = jax.random.uniform(key_slope, (), jnp.float32, 1.0, 2.0)
    col_pos = jnp.arange(D, dtype=jnp.float32) / D - 0.5
    col_walk = jnp.cumsum(jax.random.normal(key_walk, (D,), jnp.float32)) * (1.5 * D ** -0.5)
    col_offset = 2.0 * col_slope * col_pos + col_walk
    x_in = (tok_scale * tok_noise + tok_shift + col_offset).astype(jnp.bfloat16)
    weight_keys = jax.random.split(weight_root, 7)

    def draw_weight(key_w, fan_in, fan_out, gain_mul):
        return (gain_mul * fan_in ** -0.5 * jax.random.normal(key_w, (fan_in, fan_out), jnp.float32)).astype(jnp.bfloat16)

    return {
        "x_in": x_in,
        "w_q": draw_weight(weight_keys[0], D, D, 1.5),
        "w_k": draw_weight(weight_keys[1], D, D, 1.5),
        "w_v": draw_weight(weight_keys[2], D, D, 1.0),
        "w_o": draw_weight(weight_keys[3], D, D, 2.5),
        "w_gate": draw_weight(weight_keys[4], D, FF, 1.0),
        "w_up": draw_weight(weight_keys[5], D, FF, 1.0),
        "w_down": draw_weight(weight_keys[6], FF, D, 2.0),
    }


def layer_norm(values_bf):
    values = values_bf.astype(jnp.float32)
    mean_val = jnp.mean(values, axis=-1, keepdims=True)
    var_val = jnp.mean(values * values, axis=-1, keepdims=True) - mean_val * mean_val
    return ((values - mean_val) * lax.rsqrt(var_val + EPS)).astype(jnp.bfloat16)


def rotary(heads_bf):
    seq_len = heads_bf.shape[1]
    half_dim = HEAD_DIM // 2
    inv_freq = THETA ** (-2.0 * jnp.arange(half_dim, dtype=jnp.float32) / HEAD_DIM)
    angles = jnp.arange(seq_len, dtype=jnp.float32)[:, None] * inv_freq[None, :]
    cos_t = jnp.cos(angles)[:, None, :]
    sin_t = jnp.sin(angles)[:, None, :]
    values = heads_bf.astype(jnp.float32)
    lower_half = values[..., :half_dim]
    upper_half = values[..., half_dim:]
    return jnp.concatenate([lower_half * cos_t - upper_half * sin_t, upper_half * cos_t + lower_half * sin_t], axis=-1).astype(jnp.bfloat16)


def causal_attention(q_heads, k_heads, v_heads):
    seq_len = q_heads.shape[1]
    q_block = min(seq_len, 128)
    key_pos = jnp.arange(seq_len)
    k_vals = k_heads.astype(jnp.float32)
    v_vals = v_heads.astype(jnp.float32)

    def one_block(block_idx, out_acc):
        q_start = block_idx * q_block
        q_blk = lax.dynamic_slice_in_dim(q_heads, q_start, q_block, axis=1).astype(jnp.float32)
        scores = jnp.einsum("nqhd,nkhd->nhqk", q_blk, k_vals) * HEAD_DIM ** -0.5
        q_pos = q_start + jnp.arange(q_block)
        allowed = q_pos[:, None] >= key_pos[None, :]
        scores = jnp.where(allowed, scores, -1e30)
        prob_blk = jax.nn.softmax(scores, axis=-1).astype(jnp.bfloat16).astype(jnp.float32)
        blk_out = jnp.einsum("nhqk,nkhd->nqhd", prob_blk, v_vals).astype(jnp.bfloat16)
        return lax.dynamic_update_slice_in_dim(out_acc, blk_out, q_start, axis=1)

    return lax.fori_loop(0, seq_len // q_block, one_block, jnp.zeros_like(q_heads))


def project(rows_bf, weight):
    return jnp.dot(rows_bf, weight, preferred_element_type=jnp.float32).astype(jnp.bfloat16)


def reference(x_in, w_q, w_k, w_v, w_o, w_gate, w_up, w_down):
    n_seqs, seq_len, d_model = x_in.shape
    head_shape = (n_seqs, seq_len, HEADS, HEAD_DIM)
    x_rows = x_in.reshape(n_seqs * seq_len, d_model)
    normed = layer_norm(x_rows)
    q_heads = rotary(project(normed, w_q).reshape(head_shape))
    k_heads = rotary(project(normed, w_k).reshape(head_shape))
    v_heads = project(normed, w_v).reshape(head_shape)
    attn_heads = causal_attention(q_heads, k_heads, v_heads)
    attn_out = project(attn_heads.reshape(n_seqs * seq_len, d_model), w_o)
    resid_h = (x_rows.astype(jnp.float32) + attn_out.astype(jnp.float32)).astype(jnp.bfloat16)
    normed_mlp = layer_norm(resid_h)
    gate_val = project(normed_mlp, w_gate)
    up_val = project(normed_mlp, w_up)
    act_val = (jax.nn.silu(gate_val.astype(jnp.float32)) * up_val.astype(jnp.float32)).astype(jnp.bfloat16)
    mlp_out = project(act_val, w_down)
    y_out = (resid_h.astype(jnp.float32) + mlp_out.astype(jnp.float32)).astype(jnp.bfloat16)
    return y_out.reshape(n_seqs, seq_len, d_model)
```

```python
import functools

import jax
import jax.numpy as jnp
import numpy as np
from jax import lax
from jax.experimental import pallas as pl
from jax.experimental.pallas import tpu as pltpu
from jax.sharding import PartitionSpec as P

HEAD_DIM = 128
EPS = 1e-5
THETA = 10000.0
MESH = pl.DeviceIdType.MESH

S = 64
D1 = 1280
DFULL = 5120
GH = 5
GW = GH * HEAD_DIM
CH = 768
NJ = 9
NU = 2 * NJ
NP = 4
L1, L2, L3, L4 = 1, 3, 5, 6


def rotary_tables():
    half = HEAD_DIM // 2
    inv_freq = np.float32(THETA) ** (np.float32(-2.0) * np.arange(half, dtype=np.float32) / np.float32(HEAD_DIM))
    angles = np.arange(S, dtype=np.float32)[:, None] * inv_freq.astype(np.float32)[None, :]
    cos_t = np.cos(angles.astype(np.float64)).astype(np.float32)
    sin_t = np.sin(angles.astype(np.float64)).astype(np.float32)
    return np.concatenate([cos_t, cos_t], axis=1), np.concatenate([-sin_t, sin_t], axis=1)


def bdot(a, b):
    return jnp.dot(a, b, preferred_element_type=jnp.float32)


def kernel(
    x_hbm, wq, wk, wv, wo, wg, wu, wd, cos_hbm, sin_hbm, y_hbm,
    WA, WB, XB, NB, HB, ST1, ST2, PS, PO, R1, XS, R2, OF, AO, AR,
    MP, MR1, MXS, MR2, AF, ACC, DS, DR, COS, SIN, YB,
    wsem, lsem, xg_s, xg_r, st1_s, st1_r, st2_s, st2_r,
    q1_s, q1_r, q2_s, q2_r, ox_s, ox_r, od_s, od_r, ay_s, ay_r,
    m1_s, m1_r, m2_s, m2_r, ax_s, ax_r, ad_s, ad_r, dy_s, dy_r,
):
    f32, bf16 = jnp.float32, jnp.bfloat16
    ty = lax.axis_index("ty")
    tx = lax.axis_index("tx")
    c = lax.rem(tx, 2)
    xx = lax.div(tx, 2)
    co, xo = 1 - c, 1 - xx
    tyo = 1 - ty
    partner = {"tx": 2 * xx + co}
    xpeer = {"tx": 2 * xo + c}
    ypeer = {"ty": tyo}

    def rcopy(src, dst, ss, rs, dev):
        return pltpu.make_async_remote_copy(src_ref=src, dst_ref=dst, send_sem=ss, recv_sem=rs, device_id=dev, device_id_type=MESH)

    x_load = pltpu.make_async_copy(x_hbm, XB.at[0], lsem.at[0])
    x_load.start()
    cos_load = pltpu.make_async_copy(cos_hbm, COS, lsem.at[1])
    sin_load = pltpu.make_async_copy(sin_hbm, SIN, lsem.at[2])

    barrier = pltpu.get_barrier_semaphore()
    for k in range(1, 4):
        pl.semaphore_signal(barrier, inc=1, device_id={"tx": lax.rem(tx + k, 4)}, device_id_type=MESH)
    for k in range(4):
        pl.semaphore_signal(barrier, inc=1, device_id={"ty": tyo, "tx": lax.rem(tx + k, 4)}, device_id_type=MESH)

    def qkv_load(m, half):
        src = (wq, wk, wv)[m].at[:, pl.ds(half * D1, D1)]
        return pltpu.make_async_copy(src, WB.at[pl.ds((2 * m + half) * D1, D1), :], wsem.at[2 * m + half])

    def wo_load(i):
        kh, wide = i % 2, i // 2
        if wide == 0:
            return pltpu.make_async_copy(wo.at[pl.ds(kh * D1, D1), pl.ds(0, CH)], WA.at[14 + i], wsem.at[6 + i])
        return pltpu.make_async_copy(wo.at[pl.ds(kh * D1, D1), pl.ds(CH, D1 - CH)], WA.at[14 + i, :, pl.ds(0, D1 - CH)], wsem.at[6 + i])

    def gu_load(j, which):
        off = pl.multiple_of(j * CH, CH)
        return pltpu.make_async_copy((wg, wu)[which].at[:, pl.ds(off, CH)], WA.at[2 * j + which], wsem.at[10 + 2 * j + which])

    def wd_load(j):
        off = pl.multiple_of(j * CH, CH)
        return pltpu.make_async_copy(wd.at[pl.ds(off, CH), :], WB.at[pl.ds(off, CH), :], wsem.at[28 + j])

    for m in range(3):
        for half in range(2):
            qkv_load(m, half).start()
    cos_load.start()
    sin_load.start()
    for i in range(4):
        wo_load(i).start()
    for j in range(7):
        gu_load(j, 0).start()
        gu_load(j, 1).start()

    eye = lax.broadcasted_iota(jnp.int32, (S, 128), 0) == lax.broadcasted_iota(jnp.int32, (S, 128), 1)
    row8 = lax.broadcasted_iota(jnp.int32, (8, 128), 0)

    def stats_tile(v):
        s = jnp.sum(v, axis=1, keepdims=True)
        q = jnp.sum(v * v, axis=1, keepdims=True)
        srow = jnp.sum(jnp.where(eye, s, 0.0), axis=0, keepdims=True)
        qrow = jnp.sum(jnp.where(eye, q, 0.0), axis=0, keepdims=True)
        return jnp.where(row8 == 0, srow, jnp.where(row8 == 1, qrow, 0.0))

    def normalize(v, tot):
        mean = tot[0:1, :] / DFULL
        var = tot[1:2, :] / DFULL - mean * mean
        rstd = lax.rsqrt(var + EPS)
        mean_c = jnp.sum(jnp.where(eye, mean, 0.0), axis=1, keepdims=True)
        rstd_c = jnp.sum(jnp.where(eye, rstd, 0.0), axis=1, keepdims=True)
        return ((v - mean_c) * rstd_c).astype(bf16)

    x_load.wait()
    x_own = XB[0].astype(f32)
    ST1[0, 0] = stats_tile(x_own)
    pl.semaphore_wait(barrier, 7)

    def st1_copy(r, k):
        dev = {"tx": lax.rem(tx + k, 4)} if r == 0 else {"ty": tyo, "tx": lax.rem(tx + k, 4)}
        return rcopy(ST1.at[0, 0], ST1.at[r, k], st1_s.at[r, k], st1_r.at[r, k], dev)

    for k in range(1, 4):
        st1_copy(0, k).start()
    x_send = rcopy(XB.at[0], XB.at[1], xg_s.at[0], xg_r.at[0], ypeer)
    x_send.start()
    for k in range(4):
        st1_copy(1, k).start()

    def q1_copy(r, m):
        return rcopy(PS.at[r, m], R1.at[r, m], q1_s.at[r, m], q1_r.at[r, m], partner)

    def q2_copy(r, m):
        return rcopy(XS.at[r, m], R2.at[r, m], q2_s.at[r, m], q2_r.at[r, m], xpeer)

    def qkv_mm(r, m):
        if r == 0:
            qkv_load(m, 0).wait()
            qkv_load(m, 1).wait()
        n = NB[r]
        for which in range(2):
            half = co if which == 0 else c
            dst = PS if which == 0 else PO
            res = bdot(n, WB[pl.ds(pl.multiple_of((2 * m + half) * D1, D1), D1), :]).astype(bf16)
            dst[r, m, 0] = res[:, :GW]
            dst[r, m, 1] = res[:, GW:]
            if which == 0:
                q1_copy(r, m).start()

    def qkv_s1(r, m):
        q1_copy(r, m).wait_recv()
        XS[r, m] = (PO[r, m, xo].astype(f32) + R1[r, m, xo].astype(f32)).astype(bf16)
        q2_copy(r, m).start()

    for k in range(1, 4):
        st1_copy(0, k).wait_recv()
    NB[0] = normalize(x_own, ST1[0, 0] + ST1[0, 1] + ST1[0, 2] + ST1[0, 3])
    qkv_mm(0, 0)
    qkv_mm(0, 1)
    qkv_s1(0, 0)
    qkv_mm(0, 2)
    qkv_s1(0, 1)

    x_send.wait_recv()
    for k in range(4):
        st1_copy(1, k).wait_recv()
    NB[1] = normalize(XB[1].astype(f32), ST1[1, 0] + ST1[1, 1] + ST1[1, 2] + ST1[1, 3])
    qkv_mm(1, 0)
    qkv_s1(0, 2)
    qkv_mm(1, 1)
    qkv_s1(1, 0)
    qkv_mm(1, 2)
    for j in range(NJ):
        wd_load(j).start()
    qkv_s1(1, 1)
    qkv_s1(1, 2)

    cos_load.wait()
    sin_load.wait()
    causal = lax.broadcasted_iota(jnp.int32, (S, S), 0) >= lax.broadcasted_iota(jnp.int32, (S, S), 1)

    def ox_copy(r):
        return rcopy(OF.at[r, c, xx], OF.at[r, c, xx], ox_s.at[r], ox_r.at[r], xpeer)

    def ox_recv(r):
        return rcopy(OF.at[r, c, xo], OF.at[r, c, xo], ox_s.at[r], ox_r.at[r], xpeer)

    def od_copy(r):
        return rcopy(OF.at[r, c], OF.at[r, c], od_s.at[r], od_r.at[r], partner)

    def od_recv(r):
        return rcopy(OF.at[r, co], OF.at[r, co], od_s.at[r], od_r.at[r], partner)

    def attention(r):
        cos_t, sin_t = COS[...], SIN[...]
        full = []
        for m in range(3):
            q2_copy(r, m).wait_recv()
            full.append((PO[r, m, xx].astype(f32) + R1[r, m, xx].astype(f32) + R2[r, m].astype(f32)).astype(bf16))

        def rot(v):
            v = v.astype(f32)
            return (v * cos_t + pltpu.roll(v, HEAD_DIM // 2, 1) * sin_t).astype(bf16)

        outs = []
        for h in range(GH):
            cols = slice(h * HEAD_DIM, (h + 1) * HEAD_DIM)
            qh, kh, vh = rot(full[0][:, cols]), rot(full[1][:, cols]), full[2][:, cols]
            sc = lax.dot_general(qh, kh, (((1,), (1,)), ((), ())), preferred_element_type=f32) * HEAD_DIM ** -0.5
            sc = jnp.where(causal, sc, -1e30)
            e = jnp.exp(sc - jnp.max(sc, axis=1, keepdims=True))
            p = (e / jnp.sum(e, axis=1, keepdims=True)).astype(bf16)
            outs.append(bdot(p, vh).astype(bf16))
        OF[r, c, xx] = jnp.concatenate(outs, axis=1)
        ox_copy(r).start()

    def o_forward(r):
        ox_recv(r).wait_recv()
        od_copy(r).start()

    def ay_copy(r):
        return rcopy(AO.at[r], AR.at[1 - r], ay_s.at[r], ay_r.at[1 - r], ypeer)

    def out_proj(r):
        if r == 0:
            for i in range(4):
                wo_load(i).wait()
        od_recv(r).wait_recv()
        o0 = jnp.concatenate([OF[r, 0, 0], OF[r, 0, 1]], axis=1)
        o1 = jnp.concatenate([OF[r, 1, 0], OF[r, 1, 1]], axis=1)
        AO[r, :, :CH] = (bdot(o0, WA[14]) + bdot(o1, WA[15])).astype(bf16)
        AO[r, :, CH:] = (bdot(o0, WA[16, :, : D1 - CH]) + bdot(o1, WA[17, :, : D1 - CH])).astype(bf16)
        ay_copy(r).start()

    attention(0)
    attention(1)
    o_forward(0)
    out_proj(0)
    o_forward(1)
    out_proj(1)
    for j in range(7, NJ):
        gu_load(j, 0).start()
        gu_load(j, 1).start()

    def st2_copy(r, k):
        return rcopy(ST2.at[r, 0], ST2.at[r, k], st2_s.at[r, k], st2_r.at[r, k], {"tx": lax.rem(tx + k, 4)})

    def residual(r):
        ay_copy(1 - r).wait_recv()
        attn = (AO[r].astype(f32) + AR[r].astype(f32)).astype(bf16)
        h = (XB[r].astype(f32) + attn.astype(f32)).astype(bf16)
        HB[r] = h
        ST2[r, 0] = stats_tile(h.astype(f32))
        for k in range(1, 4):
            st2_copy(r, k).start()

    def norm2(r):
        for k in range(1, 4):
            st2_copy(r, k).wait_recv()
        NB[r] = normalize(HB[r].astype(f32), ST2[r, 0] + ST2[r, 1] + ST2[r, 2] + ST2[r, 3])

    residual(1)
    norm2(1)

    def m1_copy(u, j):
        return rcopy(MP.at[lax.rem(u, NP), pl.ds(2 * co, 2)], MR1.at[j], m1_s.at[j], m1_r.at[j], partner)

    def m2_copy(j):
        return rcopy(MXS.at[j], MR2.at[j], m2_s.at[j], m2_r.at[j], xpeer)

    def ax_copy(j):
        return rcopy(AF.at[j, 2 * c + xx], AF.at[j, 2 * c + xx], ax_s.at[j], ax_r.at[j], xpeer)

    def ax_recv(j):
        return rcopy(AF.at[j, 2 * c + xo], AF.at[j, 2 * c + xo], ax_s.at[j], ax_r.at[j], xpeer)

    def ad_copy(j):
        return rcopy(AF.at[j, pl.ds(2 * c, 2)], AF.at[j, pl.ds(2 * c, 2)], ad_s.at[j], ad_r.at[j], partner)

    def ad_recv(j):
        return rcopy(AF.at[j, pl.ds(2 * co, 2)], AF.at[j, pl.ds(2 * co, 2)], ad_s.at[j], ad_r.at[j], partner)

    def dy_copy():
        return rcopy(DS, DR, dy_s.at[0], dy_r.at[0], ypeer)

    def stage0(u):
        half, j = lax.div(u, NJ), lax.rem(u, NJ)

        @pl.when(u < NJ)
        def _():
            gu_load(j, 0).wait()
            gu_load(j, 1).wait()

        slot = lax.rem(u, NP)
        n = NB[1 - half]
        for which in range(2):
            res = bdot(n, WA[2 * j + which]).astype(bf16)
            for b in range(4):
                MP[slot, b, which] = res[16 * b:16 * (b + 1), :]
        m1_copy(u, j).start()

    def stage1(u):
        j, slot = lax.rem(u, NJ), lax.rem(u, NP)
        m1_copy(u, j).wait_recv()
        MXS[j] = (MP[slot, 2 * c + xo].astype(f32) + MR1[j, xo].astype(f32)).astype(bf16)
        m2_copy(j).start()

    def stage2(u):
        j, slot = lax.rem(u, NJ), lax.rem(u, NP)
        m1_copy(u, j).wait_send()
        m2_copy(j).wait_recv()
        tot = (MP[slot, 2 * c + xx].astype(f32) + MR1[j, xx].astype(f32) + MR2[j].astype(f32)).astype(bf16).astype(f32)
        gate, up = tot[0], tot[1]
        AF[j, 2 * c + xx] = (gate * jax.nn.sigmoid(gate) * up).astype(bf16)
        ax_copy(j).start()

    def stage3(u):
        j = lax.rem(u, NJ)
        m2_copy(j).wait_send()
        ax_recv(j).wait_recv()
        ad_copy(j).start()

    def stage4(u):
        j = lax.rem(u, NJ)
        ax_copy(j).wait_send()

        @pl.when(u < NJ)
        def _():
            wd_load(j).wait()

        ad_recv(j).wait_recv()
        a = jnp.concatenate([AF[j, b] for b in range(4)], axis=0)
        prod = bdot(a, WB[pl.ds(pl.multiple_of(j * CH, CH), CH), :])

        @pl.when(j == 0)
        def _():
            ACC[...] = prod

        @pl.when(j > 0)
        def _():
            ACC[...] += prod

        ad_copy(j).wait_send()

        @pl.when(u == NJ - 1)
        def _():
            DS[...] = ACC[...].astype(bf16)
            dy_copy().start()

    def step(t, carry):
        @pl.when(t == NJ - 3)
        def _():
            residual(0)

        @pl.when(t == NJ)
        def _():
            norm2(0)

        @pl.when(t < NU)
        def _():
            stage0(t)

        for lag, stage in ((L1, stage1), (L2, stage2), (L3, stage3), (L4, stage4)):
            @pl.when((t >= lag) & (t < NU + lag))
            def _(lag=lag, stage=stage):
                stage(t - lag)

        return carry

    lax.fori_loop(0, NU + L4, step, 0)

    dy_copy().wait_recv()
    mlp = (ACC[...] + DR[...].astype(f32)).astype(bf16)
    YB[...] = (HB[0].astype(f32) + mlp.astype(f32)).astype(bf16)
    y_store = pltpu.make_async_copy(YB, y_hbm, lsem.at[0])
    y_store.start()
    for k in range(1, 4):
        st1_copy(0, k).wait_send()
    for k in range(4):
        st1_copy(1, k).wait_send()
    x_send.wait_send()
    for r in range(2):
        for m in range(3):
            q1_copy(r, m).wait_send()
            q2_copy(r, m).wait_send()
        ox_copy(r).wait_send()
        od_copy(r).wait_send()
        ay_copy(r).wait_send()
        for k in range(1, 4):
            st2_copy(r, k).wait_send()
    dy_copy().wait_send()
    y_store.wait()


def layer_fn(x_blk, w_q, w_k, w_v, w_o, w_gate, w_up, w_down):
    bf16, f32 = jnp.bfloat16, jnp.float32
    cos_t, sin_t = rotary_tables()
    vm, dma = pltpu.VMEM, pltpu.SemaphoreType.DMA
    scratch = [
        vm((2 * NJ, D1, CH), bf16),
        vm((6 * D1, D1), bf16),
        vm((2, S, D1), bf16),
        vm((2, S, D1), bf16),
        vm((2, S, D1), bf16),
        vm((2, 4, 8, 128), f32),
        vm((2, 4, 8, 128), f32),
        vm((2, 3, 2, S, GW), bf16),
        vm((2, 3, 2, S, GW), bf16),
        vm((2, 3, 2, S, GW), bf16),
        vm((2, 3, S, GW), bf16),
        vm((2, 3, S, GW), bf16),
        vm((2, 2, 2, S, GW), bf16),
        vm((2, S, D1), bf16),
        vm((2, S, D1), bf16),
        vm((NP, 4, 2, 16, CH), bf16),
        vm((NJ, 2, 2, 16, CH), bf16),
        vm((NJ, 2, 16, CH), bf16),
        vm((NJ, 2, 16, CH), bf16),
        vm((NJ, 4, 16, CH), bf16),
        vm((S, D1), f32),
        vm((S, D1), bf16),
        vm((S, D1), bf16),
        vm((S, HEAD_DIM), f32),
        vm((S, HEAD_DIM), f32),
        vm((S, D1), bf16),
        dma((37,)), dma((3,)), dma((1,)), dma((1,)),
        dma((2, 4)), dma((2, 4)), dma((2, 4)), dma((2, 4)),
        dma((2, 3)), dma((2, 3)), dma((2, 3)), dma((2, 3)),
        dma((2,)), dma((2,)), dma((2,)), dma((2,)), dma((2,)), dma((2,)),
        dma((NJ,)), dma((NJ,)), dma((NJ,)), dma((NJ,)),
        dma((NJ,)), dma((NJ,)), dma((NJ,)), dma((NJ,)), dma((1,)), dma((1,)),
    ]
    y = pl.pallas_call(
        kernel,
        out_shape=jax.ShapeDtypeStruct((S, D1), bf16),
        in_specs=[pl.BlockSpec(memory_space=pl.ANY)] * 10,
        out_specs=pl.BlockSpec(memory_space=pl.ANY),
        scratch_shapes=scratch,
        compiler_params=pltpu.CompilerParams(collective_id=0, has_side_effects=True, vmem_limit_bytes=67_043_328),
    )(x_blk.reshape(S, D1), w_q, w_k, w_v, w_o, w_gate, w_up, w_down, jnp.asarray(cos_t), jnp.asarray(sin_t))
    return y.reshape(x_blk.shape)


def solution(mesh):
    act_spec = P(("dp", "ty"), None, "tx")
    col_spec = P("tx", "ty")
    row_spec = P("ty", "tx")
    return jax.shard_map(
        layer_fn,
        mesh=mesh,
        in_specs=(act_spec, col_spec, col_spec, col_spec, row_spec, col_spec, col_spec, row_spec),
        out_specs=act_spec,
        check_vma=False,
    )
```

```python
import functools

import jax
import jax.numpy as jnp
import numpy as np
from jax import lax
from jax.experimental import pallas as pl
from jax.experimental.pallas import tpu as pltpu
from jax.sharding import PartitionSpec as P

HEAD_DIM = 128
EPS = 1e-5
THETA = 10000.0
MESH = pl.DeviceIdType.MESH

S = 64
D1 = 1280
DFULL = 5120
GH = 5
GW = GH * HEAD_DIM
CH = 768
NJ = 9
NU = 2 * NJ
NP = 4
L1, L2, L3, L4 = 1, 3, 5, 6


def rotary_tables():
    half = HEAD_DIM // 2
    inv_freq = np.float32(THETA) ** (np.float32(-2.0) * np.arange(half, dtype=np.float32) / np.float32(HEAD_DIM))
    angles = np.arange(S, dtype=np.float32)[:, None] * inv_freq.astype(np.float32)[None, :]
    cos_t = np.cos(angles.astype(np.float64)).astype(np.float32)
    sin_t = np.sin(angles.astype(np.float64)).astype(np.float32)
    return np.concatenate([cos_t, cos_t], axis=1), np.concatenate([-sin_t, sin_t], axis=1)


def bdot(a, b):
    return jnp.dot(a, b, preferred_element_type=jnp.float32)


def kernel(
    x_hbm, wq, wk, wv, wo, wg, wu, wd, cos_hbm, sin_hbm, y_hbm,
    WA, WB, XB, NB, HB, ST1, ST2, PS, PO, R1, XS, R2, OF, AO, AR,
    MP, MR1, MXS, MR2, AF, ACC, DS, DR, COS, SIN, YB,
    wsem, lsem, xg_s, xg_r, st1_s, st1_r, st2_s, st2_r,
    q1_s, q1_r, q2_s, q2_r, ox_s, ox_r, od_s, od_r, ay_s, ay_r,
    m1_s, m1_r, m2_s, m2_r, ax_s, ax_r, ad_s, ad_r, dy_s, dy_r,
):
    f32, bf16 = jnp.float32, jnp.bfloat16
    ty = lax.axis_index("ty")
    tx = lax.axis_index("tx")
    c = lax.rem(tx, 2)
    xx = lax.div(tx, 2)
    co, xo = 1 - c, 1 - xx
    tyo = 1 - ty
    partner = {"tx": 2 * xx + co}
    xpeer = {"tx": 2 * xo + c}
    ypeer = {"ty": tyo}

    def rcopy(src, dst, ss, rs, dev):
        return pltpu.make_async_remote_copy(src_ref=src, dst_ref=dst, send_sem=ss, recv_sem=rs, device_id=dev, device_id_type=MESH)

    x_load = pltpu.make_async_copy(x_hbm, XB.at[0], lsem.at[0])
    x_load.start()
    cos_load = pltpu.make_async_copy(cos_hbm, COS, lsem.at[1])
    sin_load = pltpu.make_async_copy(sin_hbm, SIN, lsem.at[2])

    barrier = pltpu.get_barrier_semaphore()
    for k in range(1, 4):
        pl.semaphore_signal(barrier, inc=1, device_id={"tx": lax.rem(tx + k, 4)}, device_id_type=MESH)
    for k in range(4):
        pl.semaphore_signal(barrier, inc=1, device_id={"ty": tyo, "tx": lax.rem(tx + k, 4)}, device_id_type=MESH)

    def qkv_load(m, half):
        src = (wq, wk, wv)[m].at[:, pl.ds(half * D1, D1)]
        return pltpu.make_async_copy(src, WB.at[pl.ds((2 * m + half) * D1, D1), :], wsem.at[2 * m + half])

    def wo_load(i):
        kh, wide = i % 2, i // 2
        if wide == 0:
            return pltpu.make_async_copy(wo.at[pl.ds(kh * D1, D1), pl.ds(0, CH)], WA.at[14 + i], wsem.at[6 + i])
        return pltpu.make_async_copy(wo.at[pl.ds(kh * D1, D1), pl.ds(CH, D1 - CH)], WA.at[14 + i, :, pl.ds(0, D1 - CH)], wsem.at[6 + i])

    def gu_load(j, which):
        off = pl.multiple_of(j * CH, CH)
        return pltpu.make_async_copy((wg, wu)[which].at[:, pl.ds(off, CH)], WA.at[2 * j + which], wsem.at[10 + 2 * j + which])

    def wd_load(j):
        off = pl.multiple_of(j * CH, CH)
        return pltpu.make_async_copy(wd.at[pl.ds(off, CH), :], WB.at[pl.ds(off, CH), :], wsem.at[28 + j])

    for m in range(3):
        for half in range(2):
            qkv_load(m, half).start()
    cos_load.start()
    sin_load.start()

    eye = lax.broadcasted_iota(jnp.int32, (S, 128), 0) == lax.broadcasted_iota(jnp.int32, (S, 128), 1)
    row8 = lax.broadcasted_iota(jnp.int32, (8, 128), 0)

    def stats_tile(v):
        s = jnp.sum(v, axis=1, keepdims=True)
        q = jnp.sum(v * v, axis=1, keepdims=True)
        srow = jnp.sum(jnp.where(eye, s, 0.0), axis=0, keepdims=True)
        qrow = jnp.sum(jnp.where(eye, q, 0.0), axis=0, keepdims=True)
        return jnp.where(row8 == 0, srow, jnp.where(row8 == 1, qrow, 0.0))

    def normalize(v, tot):
        mean = tot[0:1, :] / DFULL
        var = tot[1:2, :] / DFULL - mean * mean
        rstd = lax.rsqrt(var + EPS)
        mean_c = jnp.sum(jnp.where(eye, mean, 0.0), axis=1, keepdims=True)
        rstd_c = jnp.sum(jnp.where(eye, rstd, 0.0), axis=1, keepdims=True)
        return ((v - mean_c) * rstd_c).astype(bf16)

    x_load.wait()
    x_own = XB[0].astype(f32)
    ST1[0, 0] = stats_tile(x_own)
    pl.semaphore_wait(barrier, 7)

    def st1_copy(r, k):
        dev = {"tx": lax.rem(tx + k, 4)} if r == 0 else {"ty": tyo, "tx": lax.rem(tx + k, 4)}
        return rcopy(ST1.at[0, 0], ST1.at[r, k], st1_s.at[r, k], st1_r.at[r, k], dev)

    for k in range(1, 4):
        st1_copy(0, k).start()
    x_send = rcopy(XB.at[0], XB.at[1], xg_s.at[0], xg_r.at[0], ypeer)
    x_send.start()
    for k in range(4):
        st1_copy(1, k).start()

    def q1_copy(r, m):
        return rcopy(PS.at[r, m], R1.at[r, m], q1_s.at[r, m], q1_r.at[r, m], partner)

    def q2_copy(r, m):
        return rcopy(XS.at[r, m], R2.at[r, m], q2_s.at[r, m], q2_r.at[r, m], xpeer)

    def qkv_mm(r, m, which):
        half = co if which == 0 else c
        dst = PS if which == 0 else PO
        res = bdot(NB[r], WB[pl.ds(pl.multiple_of((2 * m + half) * D1, D1), D1), :]).astype(bf16)
        dst[r, m, 0] = res[:, :GW]
        dst[r, m, 1] = res[:, GW:]
        if which == 0:
            q1_copy(r, m).start()

    def qkv_s1(r, m):
        q1_copy(r, m).wait_recv()
        XS[r, m] = (PO[r, m, xo].astype(f32) + R1[r, m, xo].astype(f32)).astype(bf16)
        q2_copy(r, m).start()

    for k in range(1, 4):
        st1_copy(0, k).wait_recv()
    NB[0] = normalize(x_own, ST1[0, 0] + ST1[0, 1] + ST1[0, 2] + ST1[0, 3])
    qkv_load(0, 0).wait()
    qkv_load(0, 1).wait()
    qkv_mm(0, 0, 0)
    qkv_mm(0, 0, 1)
    qkv_load(1, 0).wait()
    qkv_load(1, 1).wait()
    qkv_mm(0, 1, 0)
    qkv_s1(0, 0)
    qkv_mm(0, 1, 1)
    qkv_load(2, 0).wait()
    qkv_load(2, 1).wait()
    for i in range(4):
        wo_load(i).start()
    for j in range(7):
        gu_load(j, 0).start()
        gu_load(j, 1).start()
    qkv_mm(0, 2, 0)
    qkv_s1(0, 1)
    qkv_mm(0, 2, 1)

    x_send.wait_recv()
    for k in range(4):
        st1_copy(1, k).wait_recv()
    NB[1] = normalize(XB[1].astype(f32), ST1[1, 0] + ST1[1, 1] + ST1[1, 2] + ST1[1, 3])
    qkv_mm(1, 0, 0)
    qkv_s1(0, 2)
    qkv_mm(1, 0, 1)
    qkv_mm(1, 1, 0)
    qkv_s1(1, 0)
    qkv_mm(1, 1, 1)
    qkv_mm(1, 2, 0)
    qkv_s1(1, 1)
    qkv_mm(1, 2, 1)
    for j in range(NJ):
        wd_load(j).start()
    qkv_s1(1, 2)

    cos_load.wait()
    sin_load.wait()
    causal = lax.broadcasted_iota(jnp.int32, (S, S), 0) >= lax.broadcasted_iota(jnp.int32, (S, S), 1)

    def ox_copy(r):
        return rcopy(OF.at[r, c, xx], OF.at[r, c, xx], ox_s.at[r], ox_r.at[r], xpeer)

    def ox_recv(r):
        return rcopy(OF.at[r, c, xo], OF.at[r, c, xo], ox_s.at[r], ox_r.at[r], xpeer)

    def od_copy(r):
        return rcopy(OF.at[r, c], OF.at[r, c], od_s.at[r], od_r.at[r], partner)

    def od_recv(r):
        return rcopy(OF.at[r, co], OF.at[r, co], od_s.at[r], od_r.at[r], partner)

    def attention(r):
        cos_t, sin_t = COS[...], SIN[...]
        full = []
        for m in range(3):
            q2_copy(r, m).wait_recv()
            full.append((PO[r, m, xx].astype(f32) + R1[r, m, xx].astype(f32) + R2[r, m].astype(f32)).astype(bf16))

        def rot(v):
            v = v.astype(f32)
            return (v * cos_t + pltpu.roll(v, HEAD_DIM // 2, 1) * sin_t).astype(bf16)

        outs = []
        for h in range(GH):
            cols = slice(h * HEAD_DIM, (h + 1) * HEAD_DIM)
            qh, kh, vh = rot(full[0][:, cols]), rot(full[1][:, cols]), full[2][:, cols]
            sc = lax.dot_general(qh, kh, (((1,), (1,)), ((), ())), preferred_element_type=f32) * HEAD_DIM ** -0.5
            sc = jnp.where(causal, sc, -1e30)
            e = jnp.exp(sc - jnp.max(sc, axis=1, keepdims=True))
            p = (e / jnp.sum(e, axis=1, keepdims=True)).astype(bf16)
            outs.append(bdot(p, vh).astype(bf16))
        OF[r, c, xx] = jnp.concatenate(outs, axis=1)
        ox_copy(r).start()

    def o_forward(r):
        ox_recv(r).wait_recv()
        od_copy(r).start()

    def ay_copy(r):
        return rcopy(AO.at[r], AR.at[1 - r], ay_s.at[r], ay_r.at[1 - r], ypeer)

    def out_proj(r):
        if r == 0:
            for i in range(4):
                wo_load(i).wait()
        od_recv(r).wait_recv()
        o0 = jnp.concatenate([OF[r, 0, 0], OF[r, 0, 1]], axis=1)
        o1 = jnp.concatenate([OF[r, 1, 0], OF[r, 1, 1]], axis=1)
        AO[r, :, :CH] = (bdot(o0, WA[14]) + bdot(o1, WA[15])).astype(bf16)
        AO[r, :, CH:] = (bdot(o0, WA[16, :, : D1 - CH]) + bdot(o1, WA[17, :, : D1 - CH])).astype(bf16)
        ay_copy(r).start()

    attention(0)
    attention(1)
    o_forward(0)
    out_proj(0)
    o_forward(1)
    out_proj(1)
    for j in range(7, NJ):
        gu_load(j, 0).start()
        gu_load(j, 1).start()

    def st2_copy(r, k):
        return rcopy(ST2.at[r, 0], ST2.at[r, k], st2_s.at[r, k], st2_r.at[r, k], {"tx": lax.rem(tx + k, 4)})

    def residual(r):
        ay_copy(1 - r).wait_recv()
        attn = (AO[r].astype(f32) + AR[r].astype(f32)).astype(bf16)
        h = (XB[r].astype(f32) + attn.astype(f32)).astype(bf16)
        HB[r] = h
        ST2[r, 0] = stats_tile(h.astype(f32))
        for k in range(1, 4):
            st2_copy(r, k).start()

    def norm2(r):
        for k in range(1, 4):
            st2_copy(r, k).wait_recv()
        NB[r] = normalize(HB[r].astype(f32), ST2[r, 0] + ST2[r, 1] + ST2[r, 2] + ST2[r, 3])

    residual(1)
    norm2(1)

    def m1_copy(u, j):
        return rcopy(MP.at[lax.rem(u, NP), pl.ds(2 * co, 2)], MR1.at[j], m1_s.at[j], m1_r.at[j], partner)

    def m2_copy(j):
        return rcopy(MXS.at[j], MR2.at[j], m2_s.at[j], m2_r.at[j], xpeer)

    def ax_copy(j):
        return rcopy(AF.at[j, 2 * c + xx], AF.at[j, 2 * c + xx], ax_s.at[j], ax_r.at[j], xpeer)

    def ax_recv(j):
        return rcopy(AF.at[j, 2 * c + xo], AF.at[j, 2 * c + xo], ax_s.at[j], ax_r.at[j], xpeer)

    def ad_copy(j):
        return rcopy(AF.at[j, pl.ds(2 * c, 2)], AF.at[j, pl.ds(2 * c, 2)], ad_s.at[j], ad_r.at[j], partner)

    def ad_recv(j):
        return rcopy(AF.at[j, pl.ds(2 * co, 2)], AF.at[j, pl.ds(2 * co, 2)], ad_s.at[j], ad_r.at[j], partner)

    def dy_copy():
        return rcopy(DS, DR, dy_s.at[0], dy_r.at[0], ypeer)

    def stage0(u):
        half, j = lax.div(u, NJ), lax.rem(u, NJ)

        @pl.when(u < NJ)
        def _():
            gu_load(j, 0).wait()
            gu_load(j, 1).wait()

        slot = lax.rem(u, NP)
        n = NB[1 - half]
        for which in range(2):
            res = bdot(n, WA[2 * j + which]).astype(bf16)
            for b in range(4):
                MP[slot, b, which] = res[16 * b:16 * (b + 1), :]
        m1_copy(u, j).start()

    def stage1(u):
        j, slot = lax.rem(u, NJ), lax.rem(u, NP)
        m1_copy(u, j).wait_recv()
        MXS[j] = (MP[slot, 2 * c + xo].astype(f32) + MR1[j, xo].astype(f32)).astype(bf16)
        m2_copy(j).start()

    def stage2(u):
        j, slot = lax.rem(u, NJ), lax.rem(u, NP)
        m1_copy(u, j).wait_send()
        m2_copy(j).wait_recv()
        tot = (MP[slot, 2 * c + xx].astype(f32) + MR1[j, xx].astype(f32) + MR2[j].astype(f32)).astype(bf16).astype(f32)
        gate, up = tot[0], tot[1]
        AF[j, 2 * c + xx] = (gate * jax.nn.sigmoid(gate) * up).astype(bf16)
        ax_copy(j).start()

    def stage3(u):
        j = lax.rem(u, NJ)
        m2_copy(j).wait_send()
        ax_recv(j).wait_recv()
        ad_copy(j).start()

    def stage4(u):
        j = lax.rem(u, NJ)
        ax_copy(j).wait_send()

        @pl.when(u < NJ)
        def _():
            wd_load(j).wait()

        ad_recv(j).wait_recv()
        a = jnp.concatenate([AF[j, b] for b in range(4)], axis=0)
        prod = bdot(a, WB[pl.ds(pl.multiple_of(j * CH, CH), CH), :])

        @pl.when(j == 0)
        def _():
            ACC[...] = prod

        @pl.when(j > 0)
        def _():
            ACC[...] += prod

        ad_copy(j).wait_send()

        @pl.when(u == NJ - 1)
        def _():
            DS[...] = ACC[...].astype(bf16)
            dy_copy().start()

    def step(t, carry):
        @pl.when(t == NJ - 3)
        def _():
            residual(0)

        @pl.when(t == NJ)
        def _():
            norm2(0)

        @pl.when(t < NU)
        def _():
            stage0(t)

        for lag, stage in ((L1, stage1), (L2, stage2), (L3, stage3), (L4, stage4)):
            @pl.when((t >= lag) & (t < NU + lag))
            def _(lag=lag, stage=stage):
                stage(t - lag)

        return carry

    lax.fori_loop(0, NU + L4, step, 0)

    dy_copy().wait_recv()
    mlp = (ACC[...] + DR[...].astype(f32)).astype(bf16)
    YB[...] = (HB[0].astype(f32) + mlp.astype(f32)).astype(bf16)
    y_store = pltpu.make_async_copy(YB, y_hbm, lsem.at[0])
    y_store.start()
    for k in range(1, 4):
        st1_copy(0, k).wait_send()
    for k in range(4):
        st1_copy(1, k).wait_send()
    x_send.wait_send()
    for r in range(2):
        for m in range(3):
            q1_copy(r, m).wait_send()
            q2_copy(r, m).wait_send()
        ox_copy(r).wait_send()
        od_copy(r).wait_send()
        ay_copy(r).wait_send()
        for k in range(1, 4):
            st2_copy(r, k).wait_send()
    dy_copy().wait_send()
    y_store.wait()


def layer_fn(x_blk, w_q, w_k, w_v, w_o, w_gate, w_up, w_down):
    bf16, f32 = jnp.bfloat16, jnp.float32
    cos_t, sin_t = rotary_tables()
    vm, dma = pltpu.VMEM, pltpu.SemaphoreType.DMA
    scratch = [
        vm((2 * NJ, D1, CH), bf16),
        vm((6 * D1, D1), bf16),
        vm((2, S, D1), bf16),
        vm((2, S, D1), bf16),
        vm((2, S, D1), bf16),
        vm((2, 4, 8, 128), f32),
        vm((2, 4, 8, 128), f32),
        vm((2, 3, 2, S, GW), bf16),
        vm((2, 3, 2, S, GW), bf16),
        vm((2, 3, 2, S, GW), bf16),
        vm((2, 3, S, GW), bf16),
        vm((2, 3, S, GW), bf16),
        vm((2, 2, 2, S, GW), bf16),
        vm((2, S, D1), bf16),
        vm((2, S, D1), bf16),
        vm((NP, 4, 2, 16, CH), bf16),
        vm((NJ, 2, 2, 16, CH), bf16),
        vm((NJ, 2, 16, CH), bf16),
        vm((NJ, 2, 16, CH), bf16),
        vm((NJ, 4, 16, CH), bf16),
        vm((S, D1), f32),
        vm((S, D1), bf16),
        vm((S, D1), bf16),
        vm((S, HEAD_DIM), f32),
        vm((S, HEAD_DIM), f32),
        vm((S, D1), bf16),
        dma((37,)), dma((3,)), dma((1,)), dma((1,)),
        dma((2, 4)), dma((2, 4)), dma((2, 4)), dma((2, 4)),
        dma((2, 3)), dma((2, 3)), dma((2, 3)), dma((2, 3)),
        dma((2,)), dma((2,)), dma((2,)), dma((2,)), dma((2,)), dma((2,)),
        dma((NJ,)), dma((NJ,)), dma((NJ,)), dma((NJ,)),
        dma((NJ,)), dma((NJ,)), dma((NJ,)), dma((NJ,)), dma((1,)), dma((1,)),
    ]
    y = pl.pallas_call(
        kernel,
        out_shape=jax.ShapeDtypeStruct((S, D1), bf16),
        in_specs=[pl.BlockSpec(memory_space=pl.ANY)] * 10,
        out_specs=pl.BlockSpec(memory_space=pl.ANY),
        scratch_shapes=scratch,
        compiler_params=pltpu.CompilerParams(collective_id=0, has_side_effects=True, vmem_limit_bytes=67_043_328),
    )(x_blk.reshape(S, D1), w_q, w_k, w_v, w_o, w_gate, w_up, w_down, jnp.asarray(cos_t), jnp.asarray(sin_t))
    return y.reshape(x_blk.shape)


def solution(mesh):
    act_spec = P(("dp", "ty"), None, "tx")
    col_spec = P("tx", "ty")
    row_spec = P("ty", "tx")
    return jax.shard_map(
        layer_fn,
        mesh=mesh,
        in_specs=(act_spec, col_spec, col_spec, col_spec, row_spec, col_spec, col_spec, row_spec),
        out_specs=act_spec,
        check_vma=False,
    )
```

```python
import functools

import jax
import jax.numpy as jnp
import numpy as np
from jax import lax
from jax.experimental import pallas as pl
from jax.experimental.pallas import tpu as pltpu
from jax.sharding import PartitionSpec as P

HEAD_DIM = 128
EPS = 1e-5
THETA = 10000.0
MESH = pl.DeviceIdType.MESH

S = 64
D1 = 1280
DFULL = 5120
GH = 5
GW = GH * HEAD_DIM
CH = 768
NJ = 9
NU = 2 * NJ
NP = 5
L1, L2, L3, L4 = 1, 4, 7, 8


def rotary_tables():
    half = HEAD_DIM // 2
    inv_freq = np.float32(THETA) ** (np.float32(-2.0) * np.arange(half, dtype=np.float32) / np.float32(HEAD_DIM))
    angles = np.arange(S, dtype=np.float32)[:, None] * inv_freq.astype(np.float32)[None, :]
    cos_t = np.cos(angles.astype(np.float64)).astype(np.float32)
    sin_t = np.sin(angles.astype(np.float64)).astype(np.float32)
    return np.concatenate([cos_t, cos_t], axis=1), np.concatenate([-sin_t, sin_t], axis=1)


def bdot(a, b):
    return jnp.dot(a, b, preferred_element_type=jnp.float32)


def kernel(
    x_hbm, wq, wk, wv, wo, wg, wu, wd, cos_hbm, sin_hbm, y_hbm,
    WA, WB, XB, NB, HB, ST1, ST2, PS, PO, R1, XS, R2, OF, AO, AR,
    MP, MR1, MXS, MR2, AF, ACC, DS, DR, COS, SIN,
    wsem, lsem, xg_s, xg_r, st1_s, st1_r, st2_s, st2_r,
    q1_s, q1_r, q2_s, q2_r, ox_s, ox_r, od_s, od_r, ay_s, ay_r,
    m1_s, m1_r, m2_s, m2_r, ax_s, ax_r, ad_s, ad_r, dy_s, dy_r,
):
    f32, bf16 = jnp.float32, jnp.bfloat16
    ty = lax.axis_index("ty")
    tx = lax.axis_index("tx")
    c = lax.rem(tx, 2)
    xx = lax.div(tx, 2)
    co, xo = 1 - c, 1 - xx
    tyo = 1 - ty
    partner = {"tx": 2 * xx + co}
    xpeer = {"tx": 2 * xo + c}
    ypeer = {"ty": tyo}

    def rcopy(src, dst, ss, rs, dev):
        return pltpu.make_async_remote_copy(src_ref=src, dst_ref=dst, send_sem=ss, recv_sem=rs, device_id=dev, device_id_type=MESH)

    x_load = pltpu.make_async_copy(x_hbm, XB.at[0], lsem.at[0])
    x_load.start()
    cos_load = pltpu.make_async_copy(cos_hbm, COS, lsem.at[1])
    sin_load = pltpu.make_async_copy(sin_hbm, SIN, lsem.at[2])

    barrier = pltpu.get_barrier_semaphore()
    for k in range(1, 4):
        pl.semaphore_signal(barrier, inc=1, device_id={"tx": lax.rem(tx + k, 4)}, device_id_type=MESH)
    for k in range(4):
        pl.semaphore_signal(barrier, inc=1, device_id={"ty": tyo, "tx": lax.rem(tx + k, 4)}, device_id_type=MESH)

    def qkv_load(m, half):
        src = (wq, wk, wv)[m].at[:, pl.ds(half * D1, D1)]
        return pltpu.make_async_copy(src, WB.at[pl.ds((2 * m + half) * D1, D1), :], wsem.at[2 * m + half])

    def wo_load(i):
        kh, wide = i % 2, i // 2
        if wide == 0:
            return pltpu.make_async_copy(wo.at[pl.ds(kh * D1, D1), pl.ds(0, CH)], WA.at[14 + i], wsem.at[6 + i])
        return pltpu.make_async_copy(wo.at[pl.ds(kh * D1, D1), pl.ds(CH, D1 - CH)], WA.at[14 + i, :, pl.ds(0, D1 - CH)], wsem.at[6 + i])

    def gu_load(j, which):
        off = pl.multiple_of(j * CH, CH)
        return pltpu.make_async_copy((wg, wu)[which].at[:, pl.ds(off, CH)], WA.at[2 * j + which], wsem.at[10 + 2 * j + which])

    def wd_load(j):
        off = pl.multiple_of(j * CH, CH)
        return pltpu.make_async_copy(wd.at[pl.ds(off, CH), :], WB.at[pl.ds(off, CH), :], wsem.at[28 + j])

    for m in range(3):
        for half in range(2):
            qkv_load(m, half).start()
    cos_load.start()
    sin_load.start()

    eye = lax.broadcasted_iota(jnp.int32, (S, 128), 0) == lax.broadcasted_iota(jnp.int32, (S, 128), 1)
    row8 = lax.broadcasted_iota(jnp.int32, (8, 128), 0)

    def stats_tile(v):
        s = jnp.sum(v, axis=1, keepdims=True)
        q = jnp.sum(v * v, axis=1, keepdims=True)
        srow = jnp.sum(jnp.where(eye, s, 0.0), axis=0, keepdims=True)
        qrow = jnp.sum(jnp.where(eye, q, 0.0), axis=0, keepdims=True)
        return jnp.where(row8 == 0, srow, jnp.where(row8 == 1, qrow, 0.0))

    def normalize(v, tot):
        mean = tot[0:1, :] / DFULL
        var = tot[1:2, :] / DFULL - mean * mean
        rstd = lax.rsqrt(var + EPS)
        mean_c = jnp.sum(jnp.where(eye, mean, 0.0), axis=1, keepdims=True)
        rstd_c = jnp.sum(jnp.where(eye, rstd, 0.0), axis=1, keepdims=True)
        return ((v - mean_c) * rstd_c).astype(bf16)

    x_load.wait()
    x_own = XB[0].astype(f32)
    ST1[0, 0] = stats_tile(x_own)
    pl.semaphore_wait(barrier, 7)

    def st1_copy(r, k):
        dev = {"tx": lax.rem(tx + k, 4)} if r == 0 else {"ty": tyo, "tx": lax.rem(tx + k, 4)}
        return rcopy(ST1.at[0, 0], ST1.at[r, k], st1_s.at[r, k], st1_r.at[r, k], dev)

    for k in range(1, 4):
        st1_copy(0, k).start()
    x_send = rcopy(XB.at[0], XB.at[1], xg_s.at[0], xg_r.at[0], ypeer)
    x_send.start()
    for k in range(4):
        st1_copy(1, k).start()

    def q1_copy(r, m):
        return rcopy(PS.at[m], R1.at[r, m], q1_s.at[r, m], q1_r.at[r, m], partner)

    def q2_copy(r, m):
        return rcopy(XS.at[m], R2.at[r, m], q2_s.at[r, m], q2_r.at[r, m], xpeer)

    def qkv_dot(r, m, half):
        return bdot(NB[r], WB[pl.ds(pl.multiple_of((2 * m + half) * D1, D1), D1), :]).astype(bf16)

    def put_send(r, m, res):
        if r == 1:
            q1_copy(0, m).wait_send()
        PS[m, 0] = res[:, :GW]
        PS[m, 1] = res[:, GW:]
        q1_copy(r, m).start()

    def put_keep(r, m, res):
        PO[r, m, 0] = res[:, :GW]
        PO[r, m, 1] = res[:, GW:]

    def qkv_mm(r, m):
        sent, kept = qkv_dot(r, m, co), qkv_dot(r, m, c)
        put_send(r, m, sent)
        put_keep(r, m, kept)

    def qkv_s1(r, m):
        q1_copy(r, m).wait_recv()
        if r == 1:
            q2_copy(0, m).wait_send()
        XS[m] = (PO[r, m, xo].astype(f32) + R1[r, m, xo].astype(f32)).astype(bf16)
        q2_copy(r, m).start()

    for k in range(1, 4):
        st1_copy(0, k).wait_recv()
    NB[0] = normalize(x_own, ST1[0, 0] + ST1[0, 1] + ST1[0, 2] + ST1[0, 3])
    qkv_load(0, 0).wait()
    qkv_load(0, 1).wait()
    put_send(0, 0, qkv_dot(0, 0, co))
    put_keep(0, 0, qkv_dot(0, 0, c))
    qkv_load(1, 0).wait()
    qkv_load(1, 1).wait()
    qkv_s1(0, 0)
    qkv_mm(0, 1)
    qkv_load(2, 0).wait()
    qkv_load(2, 1).wait()
    for i in range(4):
        wo_load(i).start()
    for j in range(7):
        gu_load(j, 0).start()
        gu_load(j, 1).start()
    qkv_mm(0, 2)
    qkv_s1(0, 1)

    x_send.wait_recv()
    for k in range(4):
        st1_copy(1, k).wait_recv()
    NB[1] = normalize(XB[1].astype(f32), ST1[1, 0] + ST1[1, 1] + ST1[1, 2] + ST1[1, 3])
    qkv_mm(1, 0)
    qkv_s1(0, 2)
    qkv_mm(1, 1)
    qkv_s1(1, 0)
    qkv_mm(1, 2)
    for j in range(NJ):
        wd_load(j).start()
    qkv_s1(1, 1)

    cos_load.wait()
    sin_load.wait()
    causal = lax.broadcasted_iota(jnp.int32, (S, S), 0) >= lax.broadcasted_iota(jnp.int32, (S, S), 1)

    def ox_copy(r):
        return rcopy(OF.at[r, c, xx], OF.at[r, c, xx], ox_s.at[r], ox_r.at[r], xpeer)

    def ox_recv(r):
        return rcopy(OF.at[r, c, xo], OF.at[r, c, xo], ox_s.at[r], ox_r.at[r], xpeer)

    def od_copy(r):
        return rcopy(OF.at[r, c], OF.at[r, c], od_s.at[r], od_r.at[r], partner)

    def od_recv(r):
        return rcopy(OF.at[r, co], OF.at[r, co], od_s.at[r], od_r.at[r], partner)

    def attention(r):
        cos_t, sin_t = COS[...], SIN[...]
        full = []
        for m in range(3):
            q2_copy(r, m).wait_recv()
            full.append((PO[r, m, xx].astype(f32) + R1[r, m, xx].astype(f32) + R2[r, m].astype(f32)).astype(bf16))

        def rot(v):
            v = v.astype(f32)
            return (v * cos_t + pltpu.roll(v, HEAD_DIM // 2, 1) * sin_t).astype(bf16)

        outs = []
        for h in range(GH):
            cols = slice(h * HEAD_DIM, (h + 1) * HEAD_DIM)
            qh, kh, vh = rot(full[0][:, cols]), rot(full[1][:, cols]), full[2][:, cols]
            sc = lax.dot_general(qh, kh, (((1,), (1,)), ((), ())), preferred_element_type=f32) * HEAD_DIM ** -0.5
            sc = jnp.where(causal, sc, -1e30)
            e = jnp.exp(sc - jnp.max(sc, axis=1, keepdims=True))
            p = (e / jnp.sum(e, axis=1, keepdims=True)).astype(bf16)
            outs.append(bdot(p, vh).astype(bf16))
        OF[r, c, xx] = jnp.concatenate(outs, axis=1)
        ox_copy(r).start()

    def o_forward(r):
        ox_recv(r).wait_recv()
        od_copy(r).start()

    def ay_copy(r):
        return rcopy(AO.at[r], AR.at[1 - r], ay_s.at[r], ay_r.at[1 - r], ypeer)

    def out_half(r, half):
        o = jnp.concatenate([OF[r, half, 0], OF[r, half, 1]], axis=1)
        return bdot(o, WA[14 + half]), bdot(o, WA[16 + half, :, : D1 - CH])

    def out_proj(r):
        if r == 0:
            for i in range(4):
                wo_load(i).wait()
        lo, hi = out_half(r, c)
        ACC[:, :CH] = lo
        ACC[:, CH:] = hi
        od_recv(r).wait_recv()
        lo, hi = out_half(r, co)
        AO[r, :, :CH] = (ACC[:, :CH] + lo).astype(bf16)
        AO[r, :, CH:] = (ACC[:, CH:] + hi).astype(bf16)
        ay_copy(r).start()

    attention(0)
    qkv_s1(1, 2)
    o_forward(0)
    out_proj(0)
    attention(1)
    o_forward(1)
    out_proj(1)
    for j in range(7, NJ):
        gu_load(j, 0).start()
        gu_load(j, 1).start()

    def st2_copy(r, k):
        return rcopy(ST2.at[r, 0], ST2.at[r, k], st2_s.at[r, k], st2_r.at[r, k], {"tx": lax.rem(tx + k, 4)})

    def residual(r):
        ay_copy(1 - r).wait_recv()
        attn = (AO[r].astype(f32) + AR[r].astype(f32)).astype(bf16)
        h = (XB[r].astype(f32) + attn.astype(f32)).astype(bf16)
        HB[r] = h
        ST2[r, 0] = stats_tile(h.astype(f32))
        for k in range(1, 4):
            st2_copy(r, k).start()

    def norm2(r):
        for k in range(1, 4):
            st2_copy(r, k).wait_recv()
        NB[r] = normalize(HB[r].astype(f32), ST2[r, 0] + ST2[r, 1] + ST2[r, 2] + ST2[r, 3])

    residual(1)
    norm2(1)

    def m1_copy(u, j):
        return rcopy(MP.at[lax.rem(u, NP), pl.ds(2 * co, 2)], MR1.at[j], m1_s.at[j], m1_r.at[j], partner)

    def m2_copy(j):
        return rcopy(MXS.at[j], MR2.at[j], m2_s.at[j], m2_r.at[j], xpeer)

    def ax_copy(j):
        return rcopy(AF.at[j, 2 * c + xx], AF.at[j, 2 * c + xx], ax_s.at[j], ax_r.at[j], xpeer)

    def ax_recv(j):
        return rcopy(AF.at[j, 2 * c + xo], AF.at[j, 2 * c + xo], ax_s.at[j], ax_r.at[j], xpeer)

    def ad_copy(j):
        return rcopy(AF.at[j, pl.ds(2 * c, 2)], AF.at[j, pl.ds(2 * c, 2)], ad_s.at[j], ad_r.at[j], partner)

    def ad_recv(j):
        return rcopy(AF.at[j, pl.ds(2 * co, 2)], AF.at[j, pl.ds(2 * co, 2)], ad_s.at[j], ad_r.at[j], partner)

    def dy_copy():
        return rcopy(DS, DR, dy_s.at[0], dy_r.at[0], ypeer)

    def stage0(u):
        half, j = lax.div(u, NJ), lax.rem(u, NJ)

        @pl.when(u < NJ)
        def _():
            gu_load(j, 0).wait()
            gu_load(j, 1).wait()

        slot = lax.rem(u, NP)
        n = NB[1 - half]
        for which in range(2):
            res = bdot(n, WA[2 * j + which]).astype(bf16)
            for b in range(4):
                MP[slot, b, which] = res[16 * b:16 * (b + 1), :]
        m1_copy(u, j).start()

    def stage1(u):
        j, slot = lax.rem(u, NJ), lax.rem(u, NP)
        m1_copy(u, j).wait_recv()
        MXS[j] = (MP[slot, 2 * c + xo].astype(f32) + MR1[j, xo].astype(f32)).astype(bf16)
        m2_copy(j).start()

    def stage2(u):
        j, slot = lax.rem(u, NJ), lax.rem(u, NP)
        m1_copy(u, j).wait_send()
        m2_copy(j).wait_recv()
        tot = (MP[slot, 2 * c + xx].astype(f32) + MR1[j, xx].astype(f32) + MR2[j].astype(f32)).astype(bf16).astype(f32)
        gate, up = tot[0], tot[1]
        AF[j, 2 * c + xx] = (gate * jax.nn.sigmoid(gate) * up).astype(bf16)
        ax_copy(j).start()

    def stage3(u):
        j = lax.rem(u, NJ)
        m2_copy(j).wait_send()
        ax_recv(j).wait_recv()
        ad_copy(j).start()

    def stage4(u):
        j = lax.rem(u, NJ)
        ax_copy(j).wait_send()

        @pl.when(u < NJ)
        def _():
            wd_load(j).wait()

        ad_recv(j).wait_recv()
        a = jnp.concatenate([AF[j, b] for b in range(4)], axis=0)
        prod = bdot(a, WB[pl.ds(pl.multiple_of(j * CH, CH), CH), :])

        @pl.when(j == 0)
        def _():
            ACC[...] = prod

        @pl.when(j > 0)
        def _():
            ACC[...] += prod

        ad_copy(j).wait_send()

        @pl.when(u == NJ - 1)
        def _():
            DS[...] = ACC[...].astype(bf16)
            dy_copy().start()

    def step(t, carry):
        @pl.when(t == NJ - 3)
        def _():
            residual(0)

        @pl.when(t == NJ)
        def _():
            norm2(0)

        @pl.when(t < NU)
        def _():
            stage0(t)

        for lag, stage in ((L1, stage1), (L2, stage2), (L3, stage3), (L4, stage4)):
            @pl.when((t >= lag) & (t < NU + lag))
            def _(lag=lag, stage=stage):
                stage(t - lag)

        return carry

    lax.fori_loop(0, NU + L4, step, 0)

    dy_copy().wait_recv()
    mlp = (ACC[...] + DR[...].astype(f32)).astype(bf16)
    ay_copy(0).wait_send()
    AO[0] = (HB[0].astype(f32) + mlp.astype(f32)).astype(bf16)
    y_store = pltpu.make_async_copy(AO.at[0], y_hbm, lsem.at[0])
    y_store.start()
    for k in range(1, 4):
        st1_copy(0, k).wait_send()
    for k in range(4):
        st1_copy(1, k).wait_send()
    x_send.wait_send()
    for r in range(2):
        for m in range(3):
            if r == 1:
                q1_copy(r, m).wait_send()
                q2_copy(r, m).wait_send()
        ox_copy(r).wait_send()
        od_copy(r).wait_send()
        if r == 1:
            ay_copy(r).wait_send()
        for k in range(1, 4):
            st2_copy(r, k).wait_send()
    dy_copy().wait_send()
    y_store.wait()


def layer_fn(x_blk, w_q, w_k, w_v, w_o, w_gate, w_up, w_down):
    bf16, f32 = jnp.bfloat16, jnp.float32
    cos_t, sin_t = rotary_tables()
    vm, dma = pltpu.VMEM, pltpu.SemaphoreType.DMA
    scratch = [
        vm((2 * NJ, D1, CH), bf16),
        vm((6 * D1, D1), bf16),
        vm((2, S, D1), bf16),
        vm((2, S, D1), bf16),
        vm((2, S, D1), bf16),
        vm((2, 4, 8, 128), f32),
        vm((2, 4, 8, 128), f32),
        vm((3, 2, S, GW), bf16),
        vm((2, 3, 2, S, GW), bf16),
        vm((2, 3, 2, S, GW), bf16),
        vm((3, S, GW), bf16),
        vm((2, 3, S, GW), bf16),
        vm((2, 2, 2, S, GW), bf16),
        vm((2, S, D1), bf16),
        vm((2, S, D1), bf16),
        vm((NP, 4, 2, 16, CH), bf16),
        vm((NJ, 2, 2, 16, CH), bf16),
        vm((NJ, 2, 16, CH), bf16),
        vm((NJ, 2, 16, CH), bf16),
        vm((NJ, 4, 16, CH), bf16),
        vm((S, D1), f32),
        vm((S, D1), bf16),
        vm((S, D1), bf16),
        vm((S, HEAD_DIM), f32),
        vm((S, HEAD_DIM), f32),
        dma((37,)), dma((3,)), dma((1,)), dma((1,)),
        dma((2, 4)), dma((2, 4)), dma((2, 4)), dma((2, 4)),
        dma((2, 3)), dma((2, 3)), dma((2, 3)), dma((2, 3)),
        dma((2,)), dma((2,)), dma((2,)), dma((2,)), dma((2,)), dma((2,)),
        dma((NJ,)), dma((NJ,)), dma((NJ,)), dma((NJ,)),
        dma((NJ,)), dma((NJ,)), dma((NJ,)), dma((NJ,)), dma((1,)), dma((1,)),
    ]
    y = pl.pallas_call(
        kernel,
        out_shape=jax.ShapeDtypeStruct((S, D1), bf16),
        in_specs=[pl.BlockSpec(memory_space=pl.ANY)] * 10,
        out_specs=pl.BlockSpec(memory_space=pl.ANY),
        scratch_shapes=scratch,
        compiler_params=pltpu.CompilerParams(collective_id=0, has_side_effects=True, vmem_limit_bytes=67_043_328),
    )(x_blk.reshape(S, D1), w_q, w_k, w_v, w_o, w_gate, w_up, w_down, jnp.asarray(cos_t), jnp.asarray(sin_t))
    return y.reshape(x_blk.shape)


def solution(mesh):
    act_spec = P(("dp", "ty"), None, "tx")
    col_spec = P("tx", "ty")
    row_spec = P("ty", "tx")
    return jax.shard_map(
        layer_fn,
        mesh=mesh,
        in_specs=(act_spec, col_spec, col_spec, col_spec, row_spec, col_spec, col_spec, row_spec),
        out_specs=act_spec,
        check_vma=False,
    )
```

```python
import functools

import jax
import jax.numpy as jnp
import numpy as np
from jax import lax
from jax.experimental import pallas as pl
from jax.experimental.pallas import tpu as pltpu
from jax.sharding import PartitionSpec as P

HEAD_DIM = 128
EPS = 1e-5
THETA = 10000.0
MESH = pl.DeviceIdType.MESH

S = 64
D1 = 1280
DFULL = 5120
GH = 5
GW = GH * HEAD_DIM
CH = 768
NJ = 9
NU = 2 * NJ
NP = 5
PARTS = ((0, 384), (384, 256))
L1, L2, L3, L4 = 1, 4, 7, 8


def rotary_tables():
    half = HEAD_DIM // 2
    inv_freq = np.float32(THETA) ** (np.float32(-2.0) * np.arange(half, dtype=np.float32) / np.float32(HEAD_DIM))
    angles = np.arange(S, dtype=np.float32)[:, None] * inv_freq.astype(np.float32)[None, :]
    cos_t = np.cos(angles.astype(np.float64)).astype(np.float32)
    sin_t = np.sin(angles.astype(np.float64)).astype(np.float32)
    return np.concatenate([cos_t, cos_t], axis=1), np.concatenate([-sin_t, sin_t], axis=1)


def bdot(a, b):
    return jnp.dot(a, b, preferred_element_type=jnp.float32)


def kernel(
    x_hbm, wq, wk, wv, wo, wg, wu, wd, cos_hbm, sin_hbm, y_hbm,
    WA, WB, XB, NB, HB, ST1, ST2, PS, PO, R1, XS, R2, OF, AO, AR,
    MP, MR1, MXS, MR2, AF, ACC, DS, DR, COS, SIN, PR,
    wsem, lsem, xg_s, xg_r, st1_s, st1_r, st2_s, st2_r,
    q1_s, q1_r, q2_s, q2_r, ox_s, ox_r, od_s, od_r, ay_s, ay_r,
    m1_s, m1_r, m2_s, m2_r, ax_s, ax_r, ad_s, ad_r, dy_s, dy_r,
):
    f32, bf16 = jnp.float32, jnp.bfloat16
    ty = lax.axis_index("ty")
    tx = lax.axis_index("tx")
    c = lax.rem(tx, 2)
    xx = lax.div(tx, 2)
    co, xo = 1 - c, 1 - xx
    tyo = 1 - ty
    partner = {"tx": 2 * xx + co}
    xpeer = {"tx": 2 * xo + c}
    ypeer = {"ty": tyo}

    def rcopy(src, dst, ss, rs, dev):
        return pltpu.make_async_remote_copy(src_ref=src, dst_ref=dst, send_sem=ss, recv_sem=rs, device_id=dev, device_id_type=MESH)

    x_load = pltpu.make_async_copy(x_hbm, XB.at[0], lsem.at[0])
    x_load.start()
    cos_load = pltpu.make_async_copy(cos_hbm, COS, lsem.at[1])
    sin_load = pltpu.make_async_copy(sin_hbm, SIN, lsem.at[2])

    barrier = pltpu.get_barrier_semaphore()
    for k in range(1, 4):
        pl.semaphore_signal(barrier, inc=1, device_id={"tx": lax.rem(tx + k, 4)}, device_id_type=MESH)
    for k in range(4):
        pl.semaphore_signal(barrier, inc=1, device_id={"ty": tyo, "tx": lax.rem(tx + k, 4)}, device_id_type=MESH)

    def qkv_load(m, half):
        src = (wq, wk, wv)[m].at[:, pl.ds(half * D1, D1)]
        return pltpu.make_async_copy(src, WB.at[pl.ds((2 * m + half) * D1, D1), :], wsem.at[2 * m + half])

    def wo_load(i):
        kh, wide = i % 2, i // 2
        if wide == 0:
            return pltpu.make_async_copy(wo.at[pl.ds(kh * D1, D1), pl.ds(0, CH)], WA.at[14 + i], wsem.at[6 + i])
        return pltpu.make_async_copy(wo.at[pl.ds(kh * D1, D1), pl.ds(CH, D1 - CH)], WA.at[14 + i, :, pl.ds(0, D1 - CH)], wsem.at[6 + i])

    def gu_load(j, which):
        off = pl.multiple_of(j * CH, CH)
        return pltpu.make_async_copy((wg, wu)[which].at[:, pl.ds(off, CH)], WA.at[2 * j + which], wsem.at[10 + 2 * j + which])

    def wd_load(j):
        off = pl.multiple_of(j * CH, CH)
        return pltpu.make_async_copy(wd.at[pl.ds(off, CH), :], WB.at[pl.ds(off, CH), :], wsem.at[28 + j])

    for m in range(3):
        for half in range(2):
            qkv_load(m, half).start()
    cos_load.start()
    sin_load.start()

    eye = lax.broadcasted_iota(jnp.int32, (S, 128), 0) == lax.broadcasted_iota(jnp.int32, (S, 128), 1)
    row8 = lax.broadcasted_iota(jnp.int32, (8, 128), 0)

    def stats_tile(v):
        s = jnp.sum(v, axis=1, keepdims=True)
        q = jnp.sum(v * v, axis=1, keepdims=True)
        srow = jnp.sum(jnp.where(eye, s, 0.0), axis=0, keepdims=True)
        qrow = jnp.sum(jnp.where(eye, q, 0.0), axis=0, keepdims=True)
        return jnp.where(row8 == 0, srow, jnp.where(row8 == 1, qrow, 0.0))

    def normalize(v, tot):
        mean = tot[0:1, :] / DFULL
        var = tot[1:2, :] / DFULL - mean * mean
        rstd = lax.rsqrt(var + EPS)
        mean_c = jnp.sum(jnp.where(eye, mean, 0.0), axis=1, keepdims=True)
        rstd_c = jnp.sum(jnp.where(eye, rstd, 0.0), axis=1, keepdims=True)
        return ((v - mean_c) * rstd_c).astype(bf16)

    x_load.wait()
    x_own = XB[0].astype(f32)
    ST1[0, 0] = stats_tile(x_own)
    pl.semaphore_wait(barrier, 7)

    def st1_copy(r, k):
        dev = {"tx": lax.rem(tx + k, 4)} if r == 0 else {"ty": tyo, "tx": lax.rem(tx + k, 4)}
        return rcopy(ST1.at[0, 0], ST1.at[r, k], st1_s.at[r, k], st1_r.at[r, k], dev)

    for k in range(1, 4):
        st1_copy(0, k).start()
    x_send = rcopy(XB.at[0], XB.at[1], xg_s.at[0], xg_r.at[0], ypeer)
    x_send.start()
    for k in range(4):
        st1_copy(1, k).start()

    def q1_copy(r, m):
        return rcopy(PS.at[m], R1.at[r, m], q1_s.at[r, m], q1_r.at[r, m], partner)

    def q2_copy(r, m, p=0):
        lanes = pl.ds(*(PARTS[p] if r == 1 and m == 2 else (0, GW)))
        return rcopy(XS.at[m, :, lanes], R2.at[r, m, :, lanes], q2_s.at[r, m + p], q2_r.at[r, m + p], xpeer)

    def qkv_dot(r, m, half):
        return bdot(NB[r], WB[pl.ds(pl.multiple_of((2 * m + half) * D1, D1), D1), :]).astype(bf16)

    def put_send(r, m, res):
        if r == 1:
            q1_copy(0, m).wait_send()
        PS[m, 0] = res[:, :GW]
        PS[m, 1] = res[:, GW:]
        q1_copy(r, m).start()

    def put_keep(r, m, res):
        PO[r, m, 0] = res[:, :GW]
        PO[r, m, 1] = res[:, GW:]

    def qkv_mm(r, m):
        if r == 0:
            qkv_load(m, 0).wait()
            qkv_load(m, 1).wait()
        put_send(r, m, qkv_dot(r, m, co))
        put_keep(r, m, qkv_dot(r, m, c))

    def qkv_mm_both(r, m):
        sent, kept = qkv_dot(r, m, co), qkv_dot(r, m, c)
        put_send(r, m, sent)
        put_keep(r, m, kept)

    def qkv_s1(r, m):
        q1_copy(r, m).wait_recv()
        if r == 1:
            q2_copy(0, m).wait_send()
        XS[m] = (PO[r, m, xo].astype(f32) + R1[r, m, xo].astype(f32)).astype(bf16)
        q2_copy(r, m).start()
        if r == 1 and m == 2:
            q2_copy(r, m, 1).start()

    cos_load.wait()
    sin_load.wait()
    causal = lax.broadcasted_iota(jnp.int32, (S, S), 0) >= lax.broadcasted_iota(jnp.int32, (S, S), 1)

    def o_lanes(r, p):
        return pl.ds(*(PARTS[p] if r == 1 else (0, GW)))

    def ox_copy(r, p=0):
        ref = OF.at[r, c, xx, :, o_lanes(r, p)]
        return rcopy(ref, ref, ox_s.at[r + p], ox_r.at[r + p], xpeer)

    def ox_recv(r, p=0):
        ref = OF.at[r, c, xo, :, o_lanes(r, p)]
        return rcopy(ref, ref, ox_s.at[r + p], ox_r.at[r + p], xpeer)

    def od_copy(r, p=0):
        ref = OF.at[r, c, :, :, o_lanes(r, p)]
        return rcopy(ref, ref, od_s.at[r + p], od_r.at[r + p], partner)

    def od_recv(r, p=0):
        ref = OF.at[r, co, :, :, o_lanes(r, p)]
        return rcopy(ref, ref, od_s.at[r + p], od_r.at[r + p], partner)

    def total(r, m, lanes):
        return (PO[r, m, xx, :, lanes].astype(f32) + R1[r, m, xx, :, lanes].astype(f32) + R2[r, m, :, lanes].astype(f32)).astype(bf16)

    def scores(r):
        cos_t, sin_t = COS[...], SIN[...]
        q2_copy(r, 0).wait_recv()
        q2_copy(r, 1).wait_recv()

        def rot(m, h):
            v = total(r, m, pl.ds(h * HEAD_DIM, HEAD_DIM)).astype(f32)
            return (v * cos_t + pltpu.roll(v, HEAD_DIM // 2, 1) * sin_t).astype(bf16)

        qs, ks = [rot(0, h) for h in range(GH)], [rot(1, h) for h in range(GH)]
        sc = [lax.dot_general(q, k, (((1,), (1,)), ((), ())), preferred_element_type=f32) * HEAD_DIM ** -0.5 for q, k in zip(qs, ks)]
        sc = [jnp.where(causal, v, -1e30) for v in sc]
        ex = [jnp.exp(v - jnp.max(v, axis=1, keepdims=True)) for v in sc]
        for h in range(GH):
            PR[h] = (ex[h] / jnp.sum(ex[h], axis=1, keepdims=True)).astype(bf16)

    def values(r, p=0):
        q2_copy(r, 2, p).wait_recv()
        off, size = PARTS[p] if r == 1 else (0, GW)
        heads = range(off // HEAD_DIM, (off + size) // HEAD_DIM)
        outs = [bdot(PR[h], total(r, 2, pl.ds(h * HEAD_DIM, HEAD_DIM))).astype(bf16) for h in heads]
        OF[r, c, xx, :, off:off + size] = jnp.concatenate(outs, axis=1)
        ox_copy(r, p).start()

    def o_forward(r, p=0):
        ox_recv(r, p).wait_recv()
        od_copy(r, p).start()

    def ay_copy(r):
        return rcopy(AO.at[r], AR.at[1 - r], ay_s.at[r], ay_r.at[1 - r], ypeer)

    def out_half(r, half):
        o = jnp.concatenate([OF[r, half, 0], OF[r, half, 1]], axis=1)
        return bdot(o, WA[14 + half]), bdot(o, WA[16 + half, :, : D1 - CH])

    def out_proj(r):
        if r == 0:
            for i in range(4):
                wo_load(i).wait()
        lo, hi = out_half(r, c)
        ACC[:, :CH] = lo
        ACC[:, CH:] = hi
        od_recv(r).wait_recv()
        if r == 1:
            od_recv(r, 1).wait_recv()
        lo, hi = out_half(r, co)
        AO[r, :, :CH] = (ACC[:, :CH] + lo).astype(bf16)
        AO[r, :, CH:] = (ACC[:, CH:] + hi).astype(bf16)
        ay_copy(r).start()

    for k in range(1, 4):
        st1_copy(0, k).wait_recv()
    NB[0] = normalize(x_own, ST1[0, 0] + ST1[0, 1] + ST1[0, 2] + ST1[0, 3])
    qkv_mm(0, 0)
    qkv_s1(0, 0)
    qkv_mm(0, 1)
    qkv_s1(0, 1)
    qkv_mm(0, 2)
    for i in range(4):
        wo_load(i).start()
    for j in range(7):
        gu_load(j, 0).start()
        gu_load(j, 1).start()
    x_send.wait_recv()
    for k in range(4):
        st1_copy(1, k).wait_recv()
    NB[1] = normalize(XB[1].astype(f32), ST1[1, 0] + ST1[1, 1] + ST1[1, 2] + ST1[1, 3])
    qkv_s1(0, 2)
    qkv_mm(1, 0)
    qkv_s1(1, 0)
    scores(0)
    qkv_mm_both(1, 1)
    values(0)
    qkv_s1(1, 1)
    qkv_mm_both(1, 2)
    for j in range(NJ):
        wd_load(j).start()
    qkv_s1(1, 2)
    o_forward(0)
    out_proj(0)
    scores(1)
    values(1, 0)
    values(1, 1)
    o_forward(1, 0)
    o_forward(1, 1)
    out_proj(1)
    for j in range(7, NJ):
        gu_load(j, 0).start()
        gu_load(j, 1).start()

    def st2_copy(r, k):
        return rcopy(ST2.at[r, 0], ST2.at[r, k], st2_s.at[r, k], st2_r.at[r, k], {"tx": lax.rem(tx + k, 4)})

    def residual(r):
        ay_copy(1 - r).wait_recv()
        attn = (AO[r].astype(f32) + AR[r].astype(f32)).astype(bf16)
        h = (XB[r].astype(f32) + attn.astype(f32)).astype(bf16)
        HB[r] = h
        ST2[r, 0] = stats_tile(h.astype(f32))
        for k in range(1, 4):
            st2_copy(r, k).start()

    def norm2(r):
        for k in range(1, 4):
            st2_copy(r, k).wait_recv()
        NB[r] = normalize(HB[r].astype(f32), ST2[r, 0] + ST2[r, 1] + ST2[r, 2] + ST2[r, 3])

    residual(1)
    norm2(1)

    def m1_copy(u, j):
        return rcopy(MP.at[lax.rem(u, NP), pl.ds(2 * co, 2)], MR1.at[j], m1_s.at[j], m1_r.at[j], partner)

    def m2_copy(j):
        return rcopy(MXS.at[j], MR2.at[j], m2_s.at[j], m2_r.at[j], xpeer)

    def ax_copy(j):
        return rcopy(AF.at[j, 2 * c + xx], AF.at[j, 2 * c + xx], ax_s.at[j], ax_r.at[j], xpeer)

    def ax_recv(j):
        return rcopy(AF.at[j, 2 * c + xo], AF.at[j, 2 * c + xo], ax_s.at[j], ax_r.at[j], xpeer)

    def ad_copy(j):
        return rcopy(AF.at[j, pl.ds(2 * c, 2)], AF.at[j, pl.ds(2 * c, 2)], ad_s.at[j], ad_r.at[j], partner)

    def ad_recv(j):
        return rcopy(AF.at[j, pl.ds(2 * co, 2)], AF.at[j, pl.ds(2 * co, 2)], ad_s.at[j], ad_r.at[j], partner)

    def dy_copy():
        return rcopy(DS, DR, dy_s.at[0], dy_r.at[0], ypeer)

    def stage0(u):
        half, j = lax.div(u, NJ), lax.rem(u, NJ)

        @pl.when(u < NJ)
        def _():
            gu_load(j, 0).wait()
            gu_load(j, 1).wait()

        slot = lax.rem(u, NP)
        n = NB[1 - half]
        for which in range(2):
            res = bdot(n, WA[2 * j + which]).astype(bf16)
            for b in range(4):
                MP[slot, b, which] = res[16 * b:16 * (b + 1), :]
        m1_copy(u, j).start()

    def stage1(u):
        j, slot = lax.rem(u, NJ), lax.rem(u, NP)
        m1_copy(u, j).wait_recv()
        MXS[j] = (MP[slot, 2 * c + xo].astype(f32) + MR1[j, xo].astype(f32)).astype(bf16)
        m2_copy(j).start()

    def stage2(u):
        j, slot = lax.rem(u, NJ), lax.rem(u, NP)
        m1_copy(u, j).wait_send()
        m2_copy(j).wait_recv()
        tot = (MP[slot, 2 * c + xx].astype(f32) + MR1[j, xx].astype(f32) + MR2[j].astype(f32)).astype(bf16).astype(f32)
        gate, up = tot[0], tot[1]
        AF[j, 2 * c + xx] = (gate * jax.nn.sigmoid(gate) * up).astype(bf16)
        ax_copy(j).start()

    def stage3(u):
        j = lax.rem(u, NJ)
        m2_copy(j).wait_send()
        ax_recv(j).wait_recv()
        ad_copy(j).start()

    def stage4(u):
        j = lax.rem(u, NJ)
        ax_copy(j).wait_send()

        @pl.when(u < NJ)
        def _():
            wd_load(j).wait()

        ad_recv(j).wait_recv()
        a = jnp.concatenate([AF[j, b] for b in range(4)], axis=0)
        prod = bdot(a, WB[pl.ds(pl.multiple_of(j * CH, CH), CH), :])

        @pl.when(j == 0)
        def _():
            ACC[...] = prod

        @pl.when(j > 0)
        def _():
            ACC[...] += prod

        ad_copy(j).wait_send()

        @pl.when(u == NJ - 1)
        def _():
            DS[...] = ACC[...].astype(bf16)
            dy_copy().start()

    def step(t, carry):
        @pl.when(t == NJ - 3)
        def _():
            residual(0)

        @pl.when(t == NJ)
        def _():
            norm2(0)

        @pl.when(t < NU)
        def _():
            stage0(t)

        for lag, stage in ((L1, stage1), (L2, stage2), (L3, stage3), (L4, stage4)):
            @pl.when((t >= lag) & (t < NU + lag))
            def _(lag=lag, stage=stage):
                stage(t - lag)

        return carry

    lax.fori_loop(0, NU + L4, step, 0)

    dy_copy().wait_recv()
    mlp = (ACC[...] + DR[...].astype(f32)).astype(bf16)
    ay_copy(0).wait_send()
    AO[0] = (HB[0].astype(f32) + mlp.astype(f32)).astype(bf16)
    y_store = pltpu.make_async_copy(AO.at[0], y_hbm, lsem.at[0])
    y_store.start()
    for k in range(1, 4):
        st1_copy(0, k).wait_send()
    for k in range(4):
        st1_copy(1, k).wait_send()
    x_send.wait_send()
    for r in range(2):
        for m in range(3):
            if r == 1:
                q1_copy(r, m).wait_send()
                q2_copy(r, m).wait_send()
        if r == 1:
            q2_copy(1, 2, 1).wait_send()
        for p in range(r + 1):
            ox_copy(r, p).wait_send()
            od_copy(r, p).wait_send()
        if r == 1:
            ay_copy(r).wait_send()
        for k in range(1, 4):
            st2_copy(r, k).wait_send()
    dy_copy().wait_send()
    y_store.wait()


def layer_fn(x_blk, w_q, w_k, w_v, w_o, w_gate, w_up, w_down):
    bf16, f32 = jnp.bfloat16, jnp.float32
    cos_t, sin_t = rotary_tables()
    vm, dma = pltpu.VMEM, pltpu.SemaphoreType.DMA
    scratch = [
        vm((2 * NJ, D1, CH), bf16),
        vm((6 * D1, D1), bf16),
        vm((2, S, D1), bf16),
        vm((2, S, D1), bf16),
        vm((2, S, D1), bf16),
        vm((2, 4, 8, 128), f32),
        vm((2, 4, 8, 128), f32),
        vm((3, 2, S, GW), bf16),
        vm((2, 3, 2, S, GW), bf16),
        vm((2, 3, 2, S, GW), bf16),
        vm((3, S, GW), bf16),
        vm((2, 3, S, GW), bf16),
        vm((2, 2, 2, S, GW), bf16),
        vm((2, S, D1), bf16),
        vm((2, S, D1), bf16),
        vm((NP, 4, 2, 16, CH), bf16),
        vm((NJ, 2, 2, 16, CH), bf16),
        vm((NJ, 2, 16, CH), bf16),
        vm((NJ, 2, 16, CH), bf16),
        vm((NJ, 4, 16, CH), bf16),
        vm((S, D1), f32),
        vm((S, D1), bf16),
        vm((S, D1), bf16),
        vm((S, HEAD_DIM), f32),
        vm((S, HEAD_DIM), f32),
        vm((GH, S, S), bf16),
        dma((37,)), dma((3,)), dma((1,)), dma((1,)),
        dma((2, 4)), dma((2, 4)), dma((2, 4)), dma((2, 4)),
        dma((2, 3)), dma((2, 3)), dma((2, 4)), dma((2, 4)),
        dma((3,)), dma((3,)), dma((3,)), dma((3,)), dma((2,)), dma((2,)),
        dma((NJ,)), dma((NJ,)), dma((NJ,)), dma((NJ,)),
        dma((NJ,)), dma((NJ,)), dma((NJ,)), dma((NJ,)), dma((1,)), dma((1,)),
    ]
    y = pl.pallas_call(
        kernel,
        out_shape=jax.ShapeDtypeStruct((S, D1), bf16),
        in_specs=[pl.BlockSpec(memory_space=pl.ANY)] * 10,
        out_specs=pl.BlockSpec(memory_space=pl.ANY),
        scratch_shapes=scratch,
        compiler_params=pltpu.CompilerParams(collective_id=0, has_side_effects=True, vmem_limit_bytes=67_043_328),
    )(x_blk.reshape(S, D1), w_q, w_k, w_v, w_o, w_gate, w_up, w_down, jnp.asarray(cos_t), jnp.asarray(sin_t))
    return y.reshape(x_blk.shape)


def solution(mesh):
    act_spec = P(("dp", "ty"), None, "tx")
    col_spec = P("tx", "ty")
    row_spec = P("ty", "tx")
    return jax.shard_map(
        layer_fn,
        mesh=mesh,
        in_specs=(act_spec, col_spec, col_spec, col_spec, row_spec, col_spec, col_spec, row_spec),
        out_specs=act_spec,
        check_vma=False,
    )
```

```python
import functools

import jax
import jax.numpy as jnp
import numpy as np
from jax import lax
from jax.experimental import pallas as pl
from jax.experimental.pallas import tpu as pltpu
from jax.sharding import PartitionSpec as P

HEAD_DIM = 128
EPS = 1e-5
THETA = 10000.0
MESH = pl.DeviceIdType.MESH

S = 64
D1 = 1280
DFULL = 5120
GH = 5
GW = GH * HEAD_DIM
CH = 768
NJ = 9
NU = 2 * NJ
NP = 5
PARTS = ((0, 384), (384, 256))
L1, L2, L3, L4 = 1, 4, 7, 9


def rotary_tables():
    half = HEAD_DIM // 2
    inv_freq = np.float32(THETA) ** (np.float32(-2.0) * np.arange(half, dtype=np.float32) / np.float32(HEAD_DIM))
    angles = np.arange(S, dtype=np.float32)[:, None] * inv_freq.astype(np.float32)[None, :]
    cos_t = np.cos(angles.astype(np.float64)).astype(np.float32)
    sin_t = np.sin(angles.astype(np.float64)).astype(np.float32)
    return np.concatenate([cos_t, cos_t], axis=1), np.concatenate([-sin_t, sin_t], axis=1)


def bdot(a, b):
    return jnp.dot(a, b, preferred_element_type=jnp.float32)


def kernel(
    x_hbm, wq, wk, wv, wo, wg, wu, wd, cos_hbm, sin_hbm, y_hbm,
    WA, WB, XB, NB, HB, ST1, ST2, PS, PO, R1, XS, R2, OF, AO, AR,
    MP, MR1, MXS, MR2, AF, ACC, DS, DR, COS, SIN, PR,
    wsem, lsem, xg_s, xg_r, st1_s, st1_r, st2_s, st2_r,
    q1_s, q1_r, q2_s, q2_r, ox_s, ox_r, od_s, od_r, ay_s, ay_r,
    m1_s, m1_r, m2_s, m2_r, ax_s, ax_r, ad_s, ad_r, dy_s, dy_r,
):
    f32, bf16 = jnp.float32, jnp.bfloat16
    ty = lax.axis_index("ty")
    tx = lax.axis_index("tx")
    c = lax.rem(tx, 2)
    xx = lax.div(tx, 2)
    co, xo = 1 - c, 1 - xx
    tyo = 1 - ty
    partner = {"tx": 2 * xx + co}
    xpeer = {"tx": 2 * xo + c}
    ypeer = {"ty": tyo}

    def rcopy(src, dst, ss, rs, dev):
        return pltpu.make_async_remote_copy(src_ref=src, dst_ref=dst, send_sem=ss, recv_sem=rs, device_id=dev, device_id_type=MESH)

    x_load = pltpu.make_async_copy(x_hbm, XB.at[0], lsem.at[0])
    x_load.start()
    cos_load = pltpu.make_async_copy(cos_hbm, COS, lsem.at[1])
    sin_load = pltpu.make_async_copy(sin_hbm, SIN, lsem.at[2])

    barrier = pltpu.get_barrier_semaphore()
    for k in range(1, 4):
        pl.semaphore_signal(barrier, inc=1, device_id={"tx": lax.rem(tx + k, 4)}, device_id_type=MESH)
    for k in range(4):
        pl.semaphore_signal(barrier, inc=1, device_id={"ty": tyo, "tx": lax.rem(tx + k, 4)}, device_id_type=MESH)

    def qkv_load(m, half):
        src = (wq, wk, wv)[m].at[:, pl.ds(half * D1, D1)]
        return pltpu.make_async_copy(src, WB.at[pl.ds((2 * m + half) * D1, D1), :], wsem.at[m])

    def wo_load(i):
        kh, wide = i % 2, i // 2
        if wide == 0:
            return pltpu.make_async_copy(wo.at[pl.ds(kh * D1, D1), pl.ds(0, CH)], WA.at[14 + i], wsem.at[3])
        return pltpu.make_async_copy(wo.at[pl.ds(kh * D1, D1), pl.ds(CH, D1 - CH)], WA.at[14 + i, :, pl.ds(0, D1 - CH)], wsem.at[4])

    def gu_load(j, which):
        group = 5 if j < 2 else 6 if j < 7 else 7
        return pltpu.make_async_copy((wg, wu)[which].at[:, pl.ds(j * CH, CH)], WA.at[2 * j + which], wsem.at[group])

    def wd_load():
        return pltpu.make_async_copy(wd, WB.at[pl.ds(0, NJ * CH), :], wsem.at[8])

    def await_all(ref, sem):
        pltpu.make_async_copy(ref, ref, wsem.at[sem]).wait()

    for m in range(3):
        for half in range(2):
            qkv_load(m, half).start()
    cos_load.start()
    sin_load.start()

    eye = lax.broadcasted_iota(jnp.int32, (S, 128), 0) == lax.broadcasted_iota(jnp.int32, (S, 128), 1)
    row8 = lax.broadcasted_iota(jnp.int32, (8, 128), 0)

    def stats_tile(v):
        s = jnp.sum(v, axis=1, keepdims=True)
        q = jnp.sum(v * v, axis=1, keepdims=True)
        srow = jnp.sum(jnp.where(eye, s, 0.0), axis=0, keepdims=True)
        qrow = jnp.sum(jnp.where(eye, q, 0.0), axis=0, keepdims=True)
        return jnp.where(row8 == 0, srow, jnp.where(row8 == 1, qrow, 0.0))

    def normalize(v, tot):
        mean = tot[0:1, :] / DFULL
        var = tot[1:2, :] / DFULL - mean * mean
        rstd = lax.rsqrt(var + EPS)
        mean_c = jnp.sum(jnp.where(eye, mean, 0.0), axis=1, keepdims=True)
        rstd_c = jnp.sum(jnp.where(eye, rstd, 0.0), axis=1, keepdims=True)
        return ((v - mean_c) * rstd_c).astype(bf16)

    x_load.wait()
    x_own = XB[0].astype(f32)
    ST1[0] = stats_tile(x_own)
    pl.semaphore_wait(barrier, 7)

    def st1_copy(r, k):
        dev = {"tx": lax.rem(tx + k, 4)} if r == 0 else {"ty": tyo, "tx": lax.rem(tx + k, 4)}
        return rcopy(ST1.at[0], ST1.at[4 * r + k], st1_s.at[0], st1_r.at[r], dev)

    def st1_all(first, count, r):
        ref = ST1.at[pl.ds(first, count)]
        return rcopy(ref, ref, st1_s.at[0], st1_r.at[r], partner)

    for k in range(1, 4):
        st1_copy(0, k).start()
    x_send = rcopy(XB.at[0], XB.at[1], xg_s.at[0], xg_r.at[0], ypeer)
    x_send.start()
    for k in range(4):
        st1_copy(1, k).start()

    def q1_copy(r, m):
        return rcopy(PS.at[m], R1.at[r, m], q1_s.at[m], q1_r.at[r, m], partner)

    def q2_copy(r, m, p=0):
        lanes = pl.ds(*(PARTS[p] if r == 1 and m == 2 else (0, GW)))
        return rcopy(XS.at[m, :, lanes], R2.at[r, m, :, lanes], q2_s.at[m + p], q2_r.at[3 * r + m + p], xpeer)

    def qkv_dot(r, m, half):
        return bdot(NB[r], WB[pl.ds(pl.multiple_of((2 * m + half) * D1, D1), D1), :]).astype(bf16)

    def put_send(r, m, res):
        if r == 1:
            q1_copy(0, m).wait_send()
        PS[m, 0] = res[:, :GW]
        PS[m, 1] = res[:, GW:]
        q1_copy(r, m).start()

    def put_keep(r, m, res):
        PO[r, m, 0] = res[:, :GW]
        PO[r, m, 1] = res[:, GW:]

    def qkv_mm(r, m):
        if r == 0:
            await_all(WB.at[pl.ds(2 * m * D1, 2 * D1), :], m)
        put_send(r, m, qkv_dot(r, m, co))
        put_keep(r, m, qkv_dot(r, m, c))

    def qkv_mm_both(r, m):
        sent, kept = qkv_dot(r, m, co), qkv_dot(r, m, c)
        put_send(r, m, sent)
        put_keep(r, m, kept)

    def qkv_s1(r, m):
        q1_copy(r, m).wait_recv()
        if r == 1:
            q2_copy(0, m).wait_send()
        XS[m] = (PO[r, m, xo].astype(f32) + R1[r, m, xo].astype(f32)).astype(bf16)
        q2_copy(r, m).start()
        if r == 1 and m == 2:
            q2_copy(r, m, 1).start()

    causal = lax.broadcasted_iota(jnp.int32, (S, S), 0) >= lax.broadcasted_iota(jnp.int32, (S, S), 1)

    def o_lanes(r, p):
        return pl.ds(*(PARTS[p] if r == 1 else (0, GW)))

    def ox_copy(r, p=0):
        ref = OF.at[r, c, xx, :, o_lanes(r, p)]
        return rcopy(ref, ref, ox_s.at[r + p], ox_r.at[r + p], xpeer)

    def ox_recv(r, p=0):
        ref = OF.at[r, c, xo, :, o_lanes(r, p)]
        return rcopy(ref, ref, ox_s.at[r + p], ox_r.at[r + p], xpeer)

    def od_copy(r, p=0):
        ref = OF.at[r, c, :, :, o_lanes(r, p)]
        return rcopy(ref, ref, od_s.at[r + p], od_r.at[r + p], partner)

    def od_recv(r, p=0):
        ref = OF.at[r, co, :, :, o_lanes(r, p)]
        return rcopy(ref, ref, od_s.at[r + p], od_r.at[r + p], partner)

    def total(r, m, lanes):
        return (PO[r, m, xx, :, lanes].astype(f32) + R1[r, m, xx, :, lanes].astype(f32) + R2[r, m, :, lanes].astype(f32)).astype(bf16)

    def scores(r):
        if r == 0:
            cos_load.wait()
            sin_load.wait()
        cos_t, sin_t = COS[...], SIN[...]
        q2_copy(r, 0).wait_recv()
        q2_copy(r, 1).wait_recv()

        def rot(m, h):
            v = total(r, m, pl.ds(h * HEAD_DIM, HEAD_DIM)).astype(f32)
            return (v * cos_t + pltpu.roll(v, HEAD_DIM // 2, 1) * sin_t).astype(bf16)

        qs, ks = [rot(0, h) for h in range(GH)], [rot(1, h) for h in range(GH)]
        sc = [lax.dot_general(q, k, (((1,), (1,)), ((), ())), preferred_element_type=f32) * HEAD_DIM ** -0.5 for q, k in zip(qs, ks)]
        sc = [jnp.where(causal, v, -1e30) for v in sc]
        ex = [jnp.exp(v - jnp.max(v, axis=1, keepdims=True)) for v in sc]
        for h in range(GH):
            PR[h] = (ex[h] / jnp.sum(ex[h], axis=1, keepdims=True)).astype(bf16)

    def values(r, p=0):
        q2_copy(r, 2, p).wait_recv()
        off, size = PARTS[p] if r == 1 else (0, GW)
        heads = range(off // HEAD_DIM, (off + size) // HEAD_DIM)
        outs = [bdot(PR[h], total(r, 2, pl.ds(h * HEAD_DIM, HEAD_DIM))).astype(bf16) for h in heads]
        OF[r, c, xx, :, off:off + size] = jnp.concatenate(outs, axis=1)
        ox_copy(r, p).start()

    def o_forward(r, p=0):
        ox_recv(r, p).wait_recv()
        od_copy(r, p).start()

    def ay_copy(r):
        return rcopy(AO.at[r], AR.at[1 - r], ay_s.at[r], ay_r.at[1 - r], ypeer)

    def out_half(r, half):
        o = jnp.concatenate([OF[r, half, 0], OF[r, half, 1]], axis=1)
        return bdot(o, WA[14 + half]), bdot(o, WA[16 + half, :, : D1 - CH])

    def out_own(r):
        if r == 0:
            await_all(WA.at[pl.ds(14, 2)], 3)
            await_all(WA.at[pl.ds(16, 2), :, pl.ds(0, D1 - CH)], 4)
        lo, hi = out_half(r, c)
        ACC[:, :CH] = lo
        ACC[:, CH:] = hi

    def out_rest(r):
        od_recv(r).wait_recv()
        if r == 1:
            od_recv(r, 1).wait_recv()
        lo, hi = out_half(r, co)
        AO[r, :, :CH] = (ACC[:, :CH] + lo).astype(bf16)
        AO[r, :, CH:] = (ACC[:, CH:] + hi).astype(bf16)
        ay_copy(r).start()

    st1_all(1, 3, 0).wait_recv()
    NB[0] = normalize(x_own, ST1[0] + ST1[1] + ST1[2] + ST1[3])
    qkv_mm(0, 0)
    qkv_s1(0, 0)
    qkv_mm(0, 1)
    qkv_s1(0, 1)
    qkv_mm(0, 2)
    for i in range(4):
        wo_load(i).start()
    for j in range(7):
        gu_load(j, 0).start()
        gu_load(j, 1).start()
    x_send.wait_recv()
    st1_all(4, 4, 1).wait_recv()
    NB[1] = normalize(XB[1].astype(f32), ST1[4] + ST1[5] + ST1[6] + ST1[7])
    qkv_s1(0, 2)
    qkv_mm(1, 0)
    qkv_s1(1, 0)
    scores(0)
    qkv_mm_both(1, 1)
    values(0)
    qkv_s1(1, 1)
    qkv_mm_both(1, 2)
    wd_load().start()
    qkv_s1(1, 2)
    o_forward(0)
    out_own(0)
    scores(1)
    out_rest(0)
    values(1, 0)
    values(1, 1)
    o_forward(1, 0)
    o_forward(1, 1)
    out_own(1)
    out_rest(1)
    for j in range(7, NJ):
        gu_load(j, 0).start()
        gu_load(j, 1).start()

    def st2_copy(r, k):
        return rcopy(ST2.at[r, 0], ST2.at[r, k], st2_s.at[r], st2_r.at[r], {"tx": lax.rem(tx + k, 4)})

    def st2_all(r):
        ref = ST2.at[r, pl.ds(1, 3)]
        return rcopy(ref, ref, st2_s.at[r], st2_r.at[r], partner)

    def residual(r):
        ay_copy(1 - r).wait_recv()
        attn = (AO[r].astype(f32) + AR[r].astype(f32)).astype(bf16)
        h = (XB[r].astype(f32) + attn.astype(f32)).astype(bf16)
        HB[r] = h
        ST2[r, 0] = stats_tile(h.astype(f32))
        for k in range(1, 4):
            st2_copy(r, k).start()

    def norm2(r):
        st2_all(r).wait_recv()
        NB[r] = normalize(HB[r].astype(f32), ST2[r, 0] + ST2[r, 1] + ST2[r, 2] + ST2[r, 3])

    residual(1)
    norm2(1)

    def m1_copy(u, j):
        return rcopy(MP.at[lax.rem(u, NP), pl.ds(2 * co, 2)], MR1.at[j], m1_s.at[lax.rem(u, NP)], m1_r.at[lax.rem(u, NP)], partner)

    def m2_copy(u, j):
        return rcopy(MXS.at[j], MR2.at[j], m2_s.at[lax.rem(u, 4)], m2_r.at[j], xpeer)

    def ax_copy(u, j):
        return rcopy(AF.at[j, 2 * c + xx], AF.at[j, 2 * c + xx], ax_s.at[lax.rem(u, 4)], ax_r.at[j], xpeer)

    def ax_recv(u, j):
        return rcopy(AF.at[j, 2 * c + xo], AF.at[j, 2 * c + xo], ax_s.at[lax.rem(u, 4)], ax_r.at[j], xpeer)

    def ad_copy(u, j):
        return rcopy(AF.at[j, pl.ds(2 * c, 2)], AF.at[j, pl.ds(2 * c, 2)], ad_s.at[lax.rem(u, 3)], ad_r.at[j], partner)

    def ad_recv(u, j):
        return rcopy(AF.at[j, pl.ds(2 * co, 2)], AF.at[j, pl.ds(2 * co, 2)], ad_s.at[lax.rem(u, 3)], ad_r.at[j], partner)

    def dy_copy():
        return rcopy(DS, DR, dy_s.at[0], dy_r.at[0], ypeer)

    def stage0(u):
        half, j = lax.div(u, NJ), lax.rem(u, NJ)

        for first, last, sem in ((0, 2, 5), (2, 7, 6), (7, 9, 7)):
            @pl.when(u == first)
            def _(first=first, last=last, sem=sem):
                await_all(WA.at[pl.ds(2 * first, 2 * (last - first))], sem)

        slot = lax.rem(u, NP)
        n = NB[1 - half]
        for which in range(2):
            res = bdot(n, WA[2 * j + which]).astype(bf16)
            for b in range(4):
                MP[slot, b, which] = res[16 * b:16 * (b + 1), :]
        m1_copy(u, j).start()

    def stage1(u):
        j, slot = lax.rem(u, NJ), lax.rem(u, NP)
        m1_copy(u, j).wait_recv()
        MXS[j] = (MP[slot, 2 * c + xo].astype(f32) + MR1[j, xo].astype(f32)).astype(bf16)
        m2_copy(u, j).start()

    def stage2(u):
        j, slot = lax.rem(u, NJ), lax.rem(u, NP)
        m1_copy(u, j).wait_send()
        m2_copy(u, j).wait()
        tot = (MP[slot, 2 * c + xx].astype(f32) + MR1[j, xx].astype(f32) + MR2[j].astype(f32)).astype(bf16).astype(f32)
        gate, up = tot[0], tot[1]
        AF[j, 2 * c + xx] = (gate * jax.nn.sigmoid(gate) * up).astype(bf16)
        ax_copy(u, j).start()

    def stage3(u):
        j = lax.rem(u, NJ)
        ax_copy(u, j).wait_send()
        ax_recv(u, j).wait_recv()
        ad_copy(u, j).start()

    def stage4(u):
        j = lax.rem(u, NJ)

        @pl.when(u == 0)
        def _():
            wd_load().wait()

        ad_recv(u, j).wait_recv()
        a = jnp.concatenate([AF[j, b] for b in range(4)], axis=0)
        prod = bdot(a, WB[pl.ds(pl.multiple_of(j * CH, CH), CH), :])

        @pl.when(j == 0)
        def _():
            ACC[...] = prod

        @pl.when(j > 0)
        def _():
            ACC[...] += prod

        ad_copy(u, j).wait_send()

        @pl.when(u == NJ - 1)
        def _():
            DS[...] = ACC[...].astype(bf16)
            dy_copy().start()

    def step(t, carry):
        @pl.when(t == NJ - 3)
        def _():
            residual(0)

        @pl.when(t == NJ)
        def _():
            norm2(0)

        @pl.when(t < NU)
        def _():
            stage0(t)

        for lag, stage in ((L1, stage1), (L2, stage2), (L3, stage3), (L4, stage4)):
            @pl.when((t >= lag) & (t < NU + lag))
            def _(lag=lag, stage=stage):
                stage(t - lag)

        return carry

    lax.fori_loop(0, NU + L4, step, 0)

    dy_copy().wait_recv()
    mlp = (ACC[...] + DR[...].astype(f32)).astype(bf16)
    ay_copy(0).wait_send()
    AO[0] = (HB[0].astype(f32) + mlp.astype(f32)).astype(bf16)
    y_store = pltpu.make_async_copy(AO.at[0], y_hbm, lsem.at[0])
    y_store.start()
    st1_all(1, 7, 0).wait_send()
    x_send.wait_send()
    for r in range(2):
        for m in range(3):
            if r == 1:
                q1_copy(r, m).wait_send()
                q2_copy(r, m).wait_send()
        if r == 1:
            q2_copy(1, 2, 1).wait_send()
        for p in range(r + 1):
            ox_copy(r, p).wait_send()
            od_copy(r, p).wait_send()
        if r == 1:
            ay_copy(r).wait_send()
        st2_all(r).wait_send()
    dy_copy().wait_send()
    y_store.wait()


def layer_fn(x_blk, w_q, w_k, w_v, w_o, w_gate, w_up, w_down):
    bf16, f32 = jnp.bfloat16, jnp.float32
    cos_t, sin_t = rotary_tables()
    vm, dma = pltpu.VMEM, pltpu.SemaphoreType.DMA
    scratch = [
        vm((2 * NJ, D1, CH), bf16),
        vm((6 * D1, D1), bf16),
        vm((2, S, D1), bf16),
        vm((2, S, D1), bf16),
        vm((2, S, D1), bf16),
        vm((8, 8, 128), f32),
        vm((2, 4, 8, 128), f32),
        vm((3, 2, S, GW), bf16),
        vm((2, 3, 2, S, GW), bf16),
        vm((2, 3, 2, S, GW), bf16),
        vm((3, S, GW), bf16),
        vm((2, 3, S, GW), bf16),
        vm((2, 2, 2, S, GW), bf16),
        vm((2, S, D1), bf16),
        vm((2, S, D1), bf16),
        vm((NP, 4, 2, 16, CH), bf16),
        vm((NJ, 2, 2, 16, CH), bf16),
        vm((NJ, 2, 16, CH), bf16),
        vm((NJ, 2, 16, CH), bf16),
        vm((NJ, 4, 16, CH), bf16),
        vm((S, D1), f32),
        vm((S, D1), bf16),
        vm((S, D1), bf16),
        vm((S, HEAD_DIM), f32),
        vm((S, HEAD_DIM), f32),
        vm((GH, S, S), bf16),
        dma((9,)), dma((3,)), dma((1,)), dma((1,)),
        dma((1,)), dma((2,)), dma((2,)), dma((2,)),
        dma((3,)), dma((2, 3)), dma((4,)), dma((7,)),
        dma((3,)), dma((3,)), dma((3,)), dma((3,)), dma((2,)), dma((2,)),
        dma((NP,)), dma((NP,)), dma((4,)), dma((NJ,)),
        dma((4,)), dma((NJ,)), dma((3,)), dma((NJ,)), dma((1,)), dma((1,)),
    ]
    y = pl.pallas_call(
        kernel,
        out_shape=jax.ShapeDtypeStruct((S, D1), bf16),
        in_specs=[pl.BlockSpec(memory_space=pl.ANY)] * 10,
        out_specs=pl.BlockSpec(memory_space=pl.ANY),
        scratch_shapes=scratch,
        compiler_params=pltpu.CompilerParams(collective_id=0, has_side_effects=True, vmem_limit_bytes=67_043_328),
    )(x_blk.reshape(S, D1), w_q, w_k, w_v, w_o, w_gate, w_up, w_down, jnp.asarray(cos_t), jnp.asarray(sin_t))
    return y.reshape(x_blk.shape)


def solution(mesh):
    act_spec = P(("dp", "ty"), None, "tx")
    col_spec = P("tx", "ty")
    row_spec = P("ty", "tx")
    return jax.shard_map(
        layer_fn,
        mesh=mesh,
        in_specs=(act_spec, col_spec, col_spec, col_spec, row_spec, col_spec, col_spec, row_spec),
        out_specs=act_spec,
        check_vma=False,
    )
```

```python
import functools

import jax
import jax.numpy as jnp
import numpy as np
from jax import lax
from jax.experimental import pallas as pl
from jax.experimental.pallas import tpu as pltpu
from jax.sharding import PartitionSpec as P

HEAD_DIM = 128
EPS = 1e-5
THETA = 10000.0
MESH = pl.DeviceIdType.MESH

S = 64
D1 = 1280
DFULL = 5120
GH = 5
GW = GH * HEAD_DIM
CH = 768
NJ = 9
NU = 2 * NJ
NP = 5
PARTS = ((0, 384), (384, 256))
L1, L2, L3, L4 = 1, 4, 7, 9


def rotary_tables():
    half = HEAD_DIM // 2
    inv_freq = np.float32(THETA) ** (np.float32(-2.0) * np.arange(half, dtype=np.float32) / np.float32(HEAD_DIM))
    angles = np.arange(S, dtype=np.float32)[:, None] * inv_freq.astype(np.float32)[None, :]
    cos_t = np.cos(angles.astype(np.float64)).astype(np.float32)
    sin_t = np.sin(angles.astype(np.float64)).astype(np.float32)
    return np.concatenate([cos_t, cos_t], axis=1), np.concatenate([-sin_t, sin_t], axis=1)


def bdot(a, b):
    return jnp.dot(a, b, preferred_element_type=jnp.float32)


def kernel(
    x_hbm, wq, wk, wv, wo, wg, wu, wd, cos_hbm, sin_hbm, h_hbm, m_hbm,
    WA, WB, XB, NB, HB, ST1, ST2, PS, PO, R1, XS, R2, OF, AO, AR,
    MP, MR1, MXS, MR2, AF, ACC, DS, DR, COS, SIN, PR,
    wsem, lsem, xg_s, xg_r, st1_s, st1_r, st2_s, st2_r,
    q1_s, q1_r, q2_s, q2_r, ox_s, ox_r, od_s, od_r, ob_s, ob_r, ay_s, ay_r,
    m1_s, m1_r, m2_s, m2_r, ax_s, ax_r, ad_s, ad_r, dy_s, dy_r,
):
    f32, bf16 = jnp.float32, jnp.bfloat16
    ty = lax.axis_index("ty")
    tx = lax.axis_index("tx")
    c = lax.rem(tx, 2)
    xx = lax.div(tx, 2)
    co, xo = 1 - c, 1 - xx
    tyo = 1 - ty
    partner = {"tx": 2 * xx + co}
    xpeer = {"tx": 2 * xo + c}
    ypeer = {"ty": tyo}

    def rcopy(src, dst, ss, rs, dev):
        return pltpu.make_async_remote_copy(src_ref=src, dst_ref=dst, send_sem=ss, recv_sem=rs, device_id=dev, device_id_type=MESH)

    x_load = pltpu.make_async_copy(x_hbm, XB.at[0], lsem.at[0])
    x_load.start()
    cos_load = pltpu.make_async_copy(cos_hbm, COS, lsem.at[1])
    sin_load = pltpu.make_async_copy(sin_hbm, SIN, lsem.at[2])

    barrier = pltpu.get_barrier_semaphore()
    for k in range(1, 4):
        pl.semaphore_signal(barrier, inc=1, device_id={"tx": lax.rem(tx + k, 4)}, device_id_type=MESH)
    pl.semaphore_signal(barrier, inc=1, device_id=ypeer, device_id_type=MESH)

    def qkv_load(m, half):
        src = (wq, wk, wv)[m].at[:, pl.ds(half * D1, D1)]
        return pltpu.make_async_copy(src, WB.at[pl.ds((2 * m + half) * D1, D1), :], wsem.at[m])

    def wo_load(i):
        kh, wide = i % 2, i // 2
        if wide == 0:
            return pltpu.make_async_copy(wo.at[pl.ds(kh * D1, D1), pl.ds(0, CH)], WA.at[14 + i], wsem.at[3])
        return pltpu.make_async_copy(wo.at[pl.ds(kh * D1, D1), pl.ds(CH, D1 - CH)], WA.at[14 + i, :, pl.ds(0, D1 - CH)], wsem.at[4])

    def gu_load(j, which):
        group = 5 if j < 2 else 6 if j < 7 else 7
        return pltpu.make_async_copy((wg, wu)[which].at[:, pl.ds(j * CH, CH)], WA.at[2 * j + which], wsem.at[group])

    def wd_load():
        return pltpu.make_async_copy(wd, WB.at[pl.ds(0, NJ * CH), :], wsem.at[8])

    def await_all(ref, sem):
        pltpu.make_async_copy(ref, ref, wsem.at[sem]).wait()

    for m in range(3):
        for half in range(2):
            qkv_load(m, half).start()
    cos_load.start()
    sin_load.start()

    eye = lax.broadcasted_iota(jnp.int32, (S, 128), 0) == lax.broadcasted_iota(jnp.int32, (S, 128), 1)
    row8 = lax.broadcasted_iota(jnp.int32, (8, 128), 0)

    def stats_tile(v):
        s = jnp.sum(v, axis=1, keepdims=True)
        q = jnp.sum(v * v, axis=1, keepdims=True)
        srow = jnp.sum(jnp.where(eye, s, 0.0), axis=0, keepdims=True)
        qrow = jnp.sum(jnp.where(eye, q, 0.0), axis=0, keepdims=True)
        return jnp.where(row8 == 0, srow, jnp.where(row8 == 1, qrow, 0.0))

    def normalize(v, tot):
        mean = tot[0:1, :] / DFULL
        var = tot[1:2, :] / DFULL - mean * mean
        rstd = lax.rsqrt(var + EPS)
        mean_c = jnp.sum(jnp.where(eye, mean, 0.0), axis=1, keepdims=True)
        rstd_c = jnp.sum(jnp.where(eye, rstd, 0.0), axis=1, keepdims=True)
        return ((v - mean_c) * rstd_c).astype(bf16)

    x_load.wait()
    x_own = XB[0].astype(f32)
    ST1[0] = stats_tile(x_own)
    pl.semaphore_wait(barrier, 4)

    def st1_copy(k):
        return rcopy(ST1.at[0], ST1.at[k], st1_s.at[0], st1_r.at[0], {"tx": lax.rem(tx + k, 4)})

    def st1_all():
        ref = ST1.at[pl.ds(1, 3)]
        return rcopy(ref, ref, st1_s.at[0], st1_r.at[0], partner)

    def st1_total():
        return rcopy(ST1.at[4], ST1.at[5], st1_s.at[1], st1_r.at[1], ypeer)

    for k in range(1, 4):
        st1_copy(k).start()
    x_send = rcopy(XB.at[0], XB.at[1], xg_s.at[0], xg_r.at[0], ypeer)
    x_send.start()

    def q1_copy(r, m):
        return rcopy(PS.at[m], R1.at[r, m], q1_s.at[m], q1_r.at[r, m], partner)

    def q2_copy(r, m, p=0):
        lanes = pl.ds(*(PARTS[p] if r == 1 and m == 2 else (0, GW)))
        return rcopy(XS.at[m, :, lanes], R2.at[r, m, :, lanes], q2_s.at[m + p], q2_r.at[3 * r + m + p], xpeer)

    def qkv_dot(r, m, half):
        return bdot(NB[r], WB[pl.ds(pl.multiple_of((2 * m + half) * D1, D1), D1), :]).astype(bf16)

    def put_send(r, m, res):
        if r == 1:
            q1_copy(0, m).wait_send()
        PS[m, 0] = res[:, :GW]
        PS[m, 1] = res[:, GW:]
        q1_copy(r, m).start()

    def put_keep(r, m, res):
        PO[r, m, 0] = res[:, :GW]
        PO[r, m, 1] = res[:, GW:]

    def qkv_mm(r, m):
        if r == 0:
            await_all(WB.at[pl.ds(2 * m * D1, 2 * D1), :], m)
        put_send(r, m, qkv_dot(r, m, co))
        put_keep(r, m, qkv_dot(r, m, c))

    def qkv_mm_both(r, m):
        sent, kept = qkv_dot(r, m, co), qkv_dot(r, m, c)
        put_send(r, m, sent)
        put_keep(r, m, kept)

    def qkv_s1(r, m):
        q1_copy(r, m).wait_recv()
        if r == 1:
            q2_copy(0, m).wait_send()
        XS[m] = (PO[r, m, xo].astype(f32) + R1[r, m, xo].astype(f32)).astype(bf16)
        q2_copy(r, m).start()
        if r == 1 and m == 2:
            q2_copy(r, m, 1).start()

    causal = lax.broadcasted_iota(jnp.int32, (S, S), 0) >= lax.broadcasted_iota(jnp.int32, (S, S), 1)

    def o_lanes(r, p):
        return pl.ds(*(PARTS[p] if r == 1 else (0, GW)))

    def ox_copy(r):
        ref = OF.at[r, c, xx, :, o_lanes(r, 0)]
        return rcopy(ref, ref, ox_s.at[r], ox_r.at[r], xpeer)

    def ox_recv(r):
        ref = OF.at[r, c, xo, :, o_lanes(r, 0)]
        return rcopy(ref, ref, ox_s.at[r], ox_r.at[r], xpeer)

    def od_copy(r):
        ref = OF.at[r, c, :, :, o_lanes(r, 0)]
        return rcopy(ref, ref, od_s.at[r], od_r.at[r], partner)

    def od_recv(r):
        ref = OF.at[r, co, :, :, o_lanes(r, 0)]
        return rcopy(ref, ref, od_s.at[r], od_r.at[r], partner)

    def ob_copy(k):
        ref = OF.at[1, c, xx, :, o_lanes(1, 1)]
        return rcopy(ref, ref, ob_s.at[k - 1], ob_r.at[k - 1], {"tx": lax.rem(tx + k, 4)})

    def ob_recv(k):
        src = lax.rem(tx + 4 - k, 4)
        ref = OF.at[1, lax.rem(src, 2), lax.div(src, 2), :, o_lanes(1, 1)]
        return rcopy(ref, ref, ob_s.at[k - 1], ob_r.at[k - 1], partner)

    def total(r, m, lanes):
        return (PO[r, m, xx, :, lanes].astype(f32) + R1[r, m, xx, :, lanes].astype(f32) + R2[r, m, :, lanes].astype(f32)).astype(bf16)

    def scores(r):
        if r == 0:
            cos_load.wait()
            sin_load.wait()
        cos_t, sin_t = COS[...], SIN[...]
        q2_copy(r, 0).wait_recv()
        q2_copy(r, 1).wait_recv()

        def rot(m, h):
            v = total(r, m, pl.ds(h * HEAD_DIM, HEAD_DIM)).astype(f32)
            return (v * cos_t + pltpu.roll(v, HEAD_DIM // 2, 1) * sin_t).astype(bf16)

        qs, ks = [rot(0, h) for h in range(GH)], [rot(1, h) for h in range(GH)]
        sc = [lax.dot_general(q, k, (((1,), (1,)), ((), ())), preferred_element_type=f32) * HEAD_DIM ** -0.5 for q, k in zip(qs, ks)]
        sc = [jnp.where(causal, v, -1e30) for v in sc]
        ex = [jnp.exp(v - jnp.max(v, axis=1, keepdims=True)) for v in sc]
        for h in range(GH):
            PR[h] = (ex[h] / jnp.sum(ex[h], axis=1, keepdims=True)).astype(bf16)

    def values(r, p=0):
        q2_copy(r, 2, p).wait_recv()
        off, size = PARTS[p] if r == 1 else (0, GW)
        heads = range(off // HEAD_DIM, (off + size) // HEAD_DIM)
        outs = [bdot(PR[h], total(r, 2, pl.ds(h * HEAD_DIM, HEAD_DIM))).astype(bf16) for h in heads]
        OF[r, c, xx, :, off:off + size] = jnp.concatenate(outs, axis=1)
        if p == 0:
            ox_copy(r).start()
        else:
            for k in (2, 1, 3):
                ob_copy(k).start()

    def o_forward(r):
        ox_recv(r).wait_recv()
        od_copy(r).start()

    def ay_copy(r):
        return rcopy(AO.at[r], AR.at[1 - r], ay_s.at[r], ay_r.at[1 - r], ypeer)

    def out_half(r, half):
        o = jnp.concatenate([OF[r, half, 0], OF[r, half, 1]], axis=1)
        return bdot(o, WA[14 + half]), bdot(o, WA[16 + half, :, : D1 - CH])

    def out_own(r):
        if r == 0:
            await_all(WA.at[pl.ds(14, 2)], 3)
            await_all(WA.at[pl.ds(16, 2), :, pl.ds(0, D1 - CH)], 4)
        if r == 1:
            ob_recv(2).wait_recv()
        lo, hi = out_half(r, c)
        ACC[:, :CH] = lo
        ACC[:, CH:] = hi

    def out_rest(r):
        od_recv(r).wait_recv()
        if r == 1:
            ob_recv(1).wait_recv()
            ob_recv(3).wait_recv()
        lo, hi = out_half(r, co)
        AO[r, :, :CH] = (ACC[:, :CH] + lo).astype(bf16)
        AO[r, :, CH:] = (ACC[:, CH:] + hi).astype(bf16)
        ay_copy(r).start()

    st1_all().wait_recv()
    sums = ST1[0] + ST1[1] + ST1[2] + ST1[3]
    ST1[4] = sums
    st1_total().start()
    NB[0] = normalize(x_own, sums)
    qkv_mm(0, 0)
    qkv_s1(0, 0)
    qkv_mm(0, 1)
    qkv_s1(0, 1)
    qkv_mm(0, 2)
    for i in range(4):
        wo_load(i).start()
    for j in range(7):
        gu_load(j, 0).start()
        gu_load(j, 1).start()
    x_send.wait_recv()
    st1_total().wait_recv()
    NB[1] = normalize(XB[1].astype(f32), ST1[5])
    qkv_s1(0, 2)
    qkv_mm(1, 0)
    qkv_s1(1, 0)
    scores(0)
    qkv_mm_both(1, 1)
    values(0)
    qkv_s1(1, 1)
    qkv_mm_both(1, 2)
    wd_load().start()
    qkv_s1(1, 2)
    o_forward(0)
    out_own(0)
    scores(1)
    out_rest(0)
    values(1, 0)
    values(1, 1)
    o_forward(1)
    out_own(1)
    out_rest(1)
    for j in range(7, NJ):
        gu_load(j, 0).start()
        gu_load(j, 1).start()

    def st2_copy(r, k):
        return rcopy(ST2.at[r, 0], ST2.at[r, k], st2_s.at[r], st2_r.at[r], {"tx": lax.rem(tx + k, 4)})

    def st2_all(r):
        ref = ST2.at[r, pl.ds(1, 3)]
        return rcopy(ref, ref, st2_s.at[r], st2_r.at[r], partner)

    def residual(r):
        ay_copy(1 - r).wait_recv()
        attn = (AO[r].astype(f32) + AR[r].astype(f32)).astype(bf16)
        h = (XB[r].astype(f32) + attn.astype(f32)).astype(bf16)
        HB[r] = h
        ST2[r, 0] = stats_tile(h.astype(f32))
        for k in range(1, 4):
            st2_copy(r, k).start()

    def norm2(r):
        st2_all(r).wait_recv()
        NB[r] = normalize(HB[r].astype(f32), ST2[r, 0] + ST2[r, 1] + ST2[r, 2] + ST2[r, 3])

    residual(1)
    norm2(1)

    def m1_copy(u, j):
        return rcopy(MP.at[lax.rem(u, NP), pl.ds(2 * co, 2)], MR1.at[j], m1_s.at[lax.rem(u, NP)], m1_r.at[lax.rem(u, NP)], partner)

    def m2_copy(u, j):
        return rcopy(MXS.at[j], MR2.at[j], m2_s.at[lax.rem(u, 4)], m2_r.at[j], xpeer)

    def ax_copy(u, j):
        return rcopy(AF.at[j, 2 * c + xx], AF.at[j, 2 * c + xx], ax_s.at[lax.rem(u, 4)], ax_r.at[j], xpeer)

    def ax_recv(u, j):
        return rcopy(AF.at[j, 2 * c + xo], AF.at[j, 2 * c + xo], ax_s.at[lax.rem(u, 4)], ax_r.at[j], xpeer)

    def ad_copy(u, j):
        return rcopy(AF.at[j, pl.ds(2 * c, 2)], AF.at[j, pl.ds(2 * c, 2)], ad_s.at[lax.rem(u, 3)], ad_r.at[j], partner)

    def ad_recv(u, j):
        return rcopy(AF.at[j, pl.ds(2 * co, 2)], AF.at[j, pl.ds(2 * co, 2)], ad_s.at[lax.rem(u, 3)], ad_r.at[j], partner)

    def dy_copy():
        return rcopy(DS, DR, dy_s.at[0], dy_r.at[0], ypeer)

    def stage0(u):
        half, j = lax.div(u, NJ), lax.rem(u, NJ)

        for first, last, sem in ((0, 2, 5), (2, 7, 6), (7, 9, 7)):
            @pl.when(u == first)
            def _(first=first, last=last, sem=sem):
                await_all(WA.at[pl.ds(2 * first, 2 * (last - first))], sem)

        slot = lax.rem(u, NP)
        n = NB[1 - half]
        for which in range(2):
            res = bdot(n, WA[2 * j + which]).astype(bf16)
            for b in range(4):
                MP[slot, b, which] = res[16 * b:16 * (b + 1), :]
        m1_copy(u, j).start()

    def stage1(u):
        j, slot = lax.rem(u, NJ), lax.rem(u, NP)
        m1_copy(u, j).wait_recv()
        MXS[j] = (MP[slot, 2 * c + xo].astype(f32) + MR1[j, xo].astype(f32)).astype(bf16)
        m2_copy(u, j).start()

    def stage2(u):
        j, slot = lax.rem(u, NJ), lax.rem(u, NP)
        m1_copy(u, j).wait_send()
        m2_copy(u, j).wait()
        tot = (MP[slot, 2 * c + xx].astype(f32) + MR1[j, xx].astype(f32) + MR2[j].astype(f32)).astype(bf16).astype(f32)
        gate, up = tot[0], tot[1]
        AF[j, 2 * c + xx] = (gate * jax.nn.sigmoid(gate) * up).astype(bf16)
        ax_copy(u, j).start()

    def stage3(u):
        j = lax.rem(u, NJ)
        ax_copy(u, j).wait_send()
        ax_recv(u, j).wait_recv()
        ad_copy(u, j).start()

    def stage4(u):
        j = lax.rem(u, NJ)

        @pl.when(u == 0)
        def _():
            wd_load().wait()

        ad_recv(u, j).wait_recv()
        a = jnp.concatenate([AF[j, b] for b in range(4)], axis=0)
        prod = bdot(a, WB[pl.ds(pl.multiple_of(j * CH, CH), CH), :])

        @pl.when(j == 0)
        def _():
            ACC[...] = prod

        @pl.when(j > 0)
        def _():
            ACC[...] += prod

        ad_copy(u, j).wait_send()

        @pl.when(u == NJ - 1)
        def _():
            DS[...] = ACC[...].astype(bf16)
            dy_copy().start()

    def step(t, carry):
        @pl.when(t == NJ - 3)
        def _():
            residual(0)

        @pl.when(t == NJ)
        def _():
            norm2(0)

        @pl.when(t < NU)
        def _():
            stage0(t)

        for lag, stage in ((L1, stage1), (L2, stage2), (L3, stage3), (L4, stage4)):
            @pl.when((t >= lag) & (t < NU + lag))
            def _(lag=lag, stage=stage):
                stage(t - lag)

        return carry

    lax.fori_loop(0, NU + L4, step, 0)

    h_store = pltpu.make_async_copy(HB.at[0], h_hbm, lsem.at[1])
    h_store.start()
    dy_copy().wait_recv()
    mlp = (ACC[...] + DR[...].astype(f32)).astype(bf16)
    ay_copy(0).wait_send()
    AO[0] = mlp
    m_store = pltpu.make_async_copy(AO.at[0], m_hbm, lsem.at[0])
    m_store.start()
    st1_all().wait_send()
    st1_total().wait_send()
    x_send.wait_send()
    for r in range(2):
        for m in range(3):
            if r == 1:
                q1_copy(r, m).wait_send()
                q2_copy(r, m).wait_send()
        if r == 1:
            q2_copy(1, 2, 1).wait_send()
            for k in range(1, 4):
                ob_copy(k).wait_send()
        ox_copy(r).wait_send()
        od_copy(r).wait_send()
        if r == 1:
            ay_copy(r).wait_send()
        st2_all(r).wait_send()
    dy_copy().wait_send()
    h_store.wait()
    m_store.wait()


def layer_fn(x_blk, w_q, w_k, w_v, w_o, w_gate, w_up, w_down):
    bf16, f32 = jnp.bfloat16, jnp.float32
    cos_t, sin_t = rotary_tables()
    vm, dma = pltpu.VMEM, pltpu.SemaphoreType.DMA
    scratch = [
        vm((2 * NJ, D1, CH), bf16),
        vm((6 * D1, D1), bf16),
        vm((2, S, D1), bf16),
        vm((2, S, D1), bf16),
        vm((2, S, D1), bf16),
        vm((6, 8, 128), f32),
        vm((2, 4, 8, 128), f32),
        vm((3, 2, S, GW), bf16),
        vm((2, 3, 2, S, GW), bf16),
        vm((2, 3, 2, S, GW), bf16),
        vm((3, S, GW), bf16),
        vm((2, 3, S, GW), bf16),
        vm((2, 2, 2, S, GW), bf16),
        vm((2, S, D1), bf16),
        vm((2, S, D1), bf16),
        vm((NP, 4, 2, 16, CH), bf16),
        vm((NJ, 2, 2, 16, CH), bf16),
        vm((NJ, 2, 16, CH), bf16),
        vm((NJ, 2, 16, CH), bf16),
        vm((NJ, 4, 16, CH), bf16),
        vm((S, D1), f32),
        vm((S, D1), bf16),
        vm((S, D1), bf16),
        vm((S, HEAD_DIM), f32),
        vm((S, HEAD_DIM), f32),
        vm((GH, S, S), bf16),
        dma((9,)), dma((3,)), dma((1,)), dma((1,)),
        dma((2,)), dma((2,)), dma((2,)), dma((2,)),
        dma((3,)), dma((2, 3)), dma((4,)), dma((7,)),
        dma((2,)), dma((2,)), dma((2,)), dma((2,)), dma((3,)), dma((3,)), dma((2,)), dma((2,)),
        dma((NP,)), dma((NP,)), dma((4,)), dma((NJ,)),
        dma((4,)), dma((NJ,)), dma((3,)), dma((NJ,)), dma((1,)), dma((1,)),
    ]
    h, mlp = pl.pallas_call(
        kernel,
        out_shape=[jax.ShapeDtypeStruct((S, D1), bf16)] * 2,
        in_specs=[pl.BlockSpec(memory_space=pl.ANY)] * 10,
        out_specs=[pl.BlockSpec(memory_space=pl.ANY)] * 2,
        scratch_shapes=scratch,
        compiler_params=pltpu.CompilerParams(collective_id=0, has_side_effects=True, vmem_limit_bytes=67_043_328),
    )(x_blk.reshape(S, D1), w_q, w_k, w_v, w_o, w_gate, w_up, w_down, jnp.asarray(cos_t), jnp.asarray(sin_t))
    return (h.astype(f32) + mlp.astype(f32)).astype(bf16).reshape(x_blk.shape)


def solution(mesh):
    act_spec = P(("dp", "ty"), None, "tx")
    col_spec = P("tx", "ty")
    row_spec = P("ty", "tx")
    return jax.shard_map(
        layer_fn,
        mesh=mesh,
        in_specs=(act_spec, col_spec, col_spec, col_spec, row_spec, col_spec, col_spec, row_spec),
        out_specs=act_spec,
        check_vma=False,
    )
```

```python
import functools

import jax
import jax.numpy as jnp
import numpy as np
from jax import lax
from jax.experimental import pallas as pl
from jax.experimental.pallas import tpu as pltpu
from jax.sharding import PartitionSpec as P

HEAD_DIM = 128
EPS = 1e-5
THETA = 10000.0
MESH = pl.DeviceIdType.MESH

S = 64
D1 = 1280
DFULL = 5120
GH = 5
GW = GH * HEAD_DIM
CH = 768
NJ = 9
NU = 2 * NJ
NP = 3
PARTS = ((0, 384), (384, 256))
L1, L2, L3, L4 = 1, 4, 7, 9
LATE = 13


def rotary_tables():
    half = HEAD_DIM // 2
    inv_freq = np.float32(THETA) ** (np.float32(-2.0) * np.arange(half, dtype=np.float32) / np.float32(HEAD_DIM))
    angles = np.arange(S, dtype=np.float32)[:, None] * inv_freq.astype(np.float32)[None, :]
    cos_t = np.cos(angles.astype(np.float64)).astype(np.float32)
    sin_t = np.sin(angles.astype(np.float64)).astype(np.float32)
    return np.concatenate([cos_t, cos_t], axis=1), np.concatenate([-sin_t, sin_t], axis=1)


def bdot(a, b):
    return jnp.dot(a, b, preferred_element_type=jnp.float32)


def kernel(
    x_hbm, wq, wk, wv, wo, wg, wu, wd, cos_hbm, sin_hbm, h_hbm, m_hbm,
    WA, WB, XB, NB, HB, ST1, ST2, PS, PO, R1, XS, R2, OF, AO, AR,
    MP, MR1, MXS, MR2, AF, ACC, DS, DR, COS, SIN, PR,
    wsem, lsem, xg_s, xg_r, st1_s, st1_r, st2_s, st2_r,
    q1_s, q1_r, q2_s, q2_r, ox_s, ox_r, od_s, od_r, ob_s, ob_r, ay_s, ay_r,
    m1_s, m1_r, m2_s, m2_r, ax_s, ax_r, ad_s, ad_r, dy_s, dy_r,
):
    f32, bf16 = jnp.float32, jnp.bfloat16
    ty = lax.axis_index("ty")
    tx = lax.axis_index("tx")
    c = lax.rem(tx, 2)
    xx = lax.div(tx, 2)
    co, xo = 1 - c, 1 - xx
    tyo = 1 - ty
    partner = {"tx": 2 * xx + co}
    xpeer = {"tx": 2 * xo + c}
    ypeer = {"ty": tyo}

    def rcopy(src, dst, ss, rs, dev):
        return pltpu.make_async_remote_copy(src_ref=src, dst_ref=dst, send_sem=ss, recv_sem=rs, device_id=dev, device_id_type=MESH)

    x_load = pltpu.make_async_copy(x_hbm, XB.at[0], lsem.at[0])
    x_load.start()
    cos_load = pltpu.make_async_copy(cos_hbm, COS, lsem.at[1])
    sin_load = pltpu.make_async_copy(sin_hbm, SIN, lsem.at[2])

    barrier = pltpu.get_barrier_semaphore()
    for k in range(1, 4):
        pl.semaphore_signal(barrier, inc=1, device_id={"tx": lax.rem(tx + k, 4)}, device_id_type=MESH)
    pl.semaphore_signal(barrier, inc=1, device_id=ypeer, device_id_type=MESH)

    def qkv_load(m, half):
        src = (wq, wk, wv)[m].at[:, pl.ds(half * D1, D1)]
        return pltpu.make_async_copy(src, WB.at[pl.ds((2 * m + half) * D1, D1), :], wsem.at[m])

    def wo_load(i):
        kh, wide = i % 2, i // 2
        if wide == 0:
            return pltpu.make_async_copy(wo.at[pl.ds(kh * D1, D1), pl.ds(0, CH)], WA.at[14 + i], wsem.at[3])
        return pltpu.make_async_copy(wo.at[pl.ds(kh * D1, D1), pl.ds(CH, D1 - CH)], WA.at[14 + i, :, pl.ds(0, D1 - CH)], wsem.at[4])

    def gu_load(j, which):
        group = 5 if j < 2 else 6 if j < 7 else 7
        return pltpu.make_async_copy((wg, wu)[which].at[:, pl.ds(j * CH, CH)], WA.at[2 * j + which], wsem.at[group])

    def wd_load():
        return pltpu.make_async_copy(wd, WB.at[pl.ds(0, NJ * CH), :], wsem.at[8])

    def await_all(ref, sem):
        pltpu.make_async_copy(ref, ref, wsem.at[sem]).wait()

    for m in range(3):
        for half in range(2):
            qkv_load(m, half).start()
    cos_load.start()
    sin_load.start()

    eye = lax.broadcasted_iota(jnp.int32, (S, 128), 0) == lax.broadcasted_iota(jnp.int32, (S, 128), 1)
    row8 = lax.broadcasted_iota(jnp.int32, (8, 128), 0)

    def stats_tile(v):
        s = jnp.sum(v, axis=1, keepdims=True)
        q = jnp.sum(v * v, axis=1, keepdims=True)
        srow = jnp.sum(jnp.where(eye, s, 0.0), axis=0, keepdims=True)
        qrow = jnp.sum(jnp.where(eye, q, 0.0), axis=0, keepdims=True)
        return jnp.where(row8 == 0, srow, jnp.where(row8 == 1, qrow, 0.0))

    def normalize(v, tot):
        mean = tot[0:1, :] / DFULL
        var = tot[1:2, :] / DFULL - mean * mean
        rstd = lax.rsqrt(var + EPS)
        mean_c = jnp.sum(jnp.where(eye, mean, 0.0), axis=1, keepdims=True)
        rstd_c = jnp.sum(jnp.where(eye, rstd, 0.0), axis=1, keepdims=True)
        return ((v - mean_c) * rstd_c).astype(bf16)

    x_load.wait()
    x_own = XB[0].astype(f32)
    ST1[0] = stats_tile(x_own)
    pl.semaphore_wait(barrier, 4)

    def st1_copy(k):
        return rcopy(ST1.at[0], ST1.at[k], st1_s.at[0], st1_r.at[0], {"tx": lax.rem(tx + k, 4)})

    def st1_all():
        ref = ST1.at[pl.ds(1, 3)]
        return rcopy(ref, ref, st1_s.at[0], st1_r.at[0], partner)

    def st1_total():
        return rcopy(ST1.at[4], ST1.at[5], st1_s.at[1], st1_r.at[1], ypeer)

    for k in range(1, 4):
        st1_copy(k).start()
    x_send = rcopy(XB.at[0], XB.at[1], xg_s.at[0], xg_r.at[0], ypeer)
    x_send.start()

    def q1_copy(r, m):
        return rcopy(PS.at[m], R1.at[r, m], q1_s.at[m], q1_r.at[r, m], partner)

    def q2_copy(r, m, p=0):
        lanes = pl.ds(*(PARTS[p] if r == 1 and m == 2 else (0, GW)))
        return rcopy(XS.at[m, :, lanes], R2.at[r, m, :, lanes], q2_s.at[m + p], q2_r.at[3 * r + m + p], xpeer)

    def qkv_dot(r, m, half):
        return bdot(NB[r], WB[pl.ds(pl.multiple_of((2 * m + half) * D1, D1), D1), :]).astype(bf16)

    def put_send(r, m, res):
        if r == 1:
            q1_copy(0, m).wait_send()
        PS[m, 0] = res[:, :GW]
        PS[m, 1] = res[:, GW:]
        q1_copy(r, m).start()

    def put_keep(r, m, res):
        PO[r, m, 0] = res[:, :GW]
        PO[r, m, 1] = res[:, GW:]

    def qkv_mm(r, m):
        if r == 0:
            await_all(WB.at[pl.ds(2 * m * D1, 2 * D1), :], m)
        put_send(r, m, qkv_dot(r, m, co))
        put_keep(r, m, qkv_dot(r, m, c))

    def qkv_mm_both(r, m):
        sent, kept = qkv_dot(r, m, co), qkv_dot(r, m, c)
        put_send(r, m, sent)
        put_keep(r, m, kept)

    def qkv_s1(r, m):
        q1_copy(r, m).wait_recv()
        if r == 1:
            q2_copy(0, m).wait_send()
        XS[m] = (PO[r, m, xo].astype(f32) + R1[r, m, xo].astype(f32)).astype(bf16)
        q2_copy(r, m).start()
        if r == 1 and m == 2:
            q2_copy(r, m, 1).start()

    causal = lax.broadcasted_iota(jnp.int32, (S, S), 0) >= lax.broadcasted_iota(jnp.int32, (S, S), 1)

    def o_lanes(r, p):
        return pl.ds(*(PARTS[p] if r == 1 else (0, GW)))

    def ox_copy(r):
        ref = OF.at[r, c, xx, :, o_lanes(r, 0)]
        return rcopy(ref, ref, ox_s.at[r], ox_r.at[r], xpeer)

    def ox_recv(r):
        ref = OF.at[r, c, xo, :, o_lanes(r, 0)]
        return rcopy(ref, ref, ox_s.at[r], ox_r.at[r], xpeer)

    def od_copy(r):
        ref = OF.at[r, c, :, :, o_lanes(r, 0)]
        return rcopy(ref, ref, od_s.at[r], od_r.at[r], partner)

    def od_recv(r):
        ref = OF.at[r, co, :, :, o_lanes(r, 0)]
        return rcopy(ref, ref, od_s.at[r], od_r.at[r], partner)

    def ob_copy(k):
        ref = OF.at[1, c, xx, :, o_lanes(1, 1)]
        return rcopy(ref, ref, ob_s.at[k - 1], ob_r.at[k - 1], {"tx": lax.rem(tx + k, 4)})

    def ob_recv(k):
        src = lax.rem(tx + 4 - k, 4)
        ref = OF.at[1, lax.rem(src, 2), lax.div(src, 2), :, o_lanes(1, 1)]
        return rcopy(ref, ref, ob_s.at[k - 1], ob_r.at[k - 1], partner)

    def total(r, m, lanes):
        return (PO[r, m, xx, :, lanes].astype(f32) + R1[r, m, xx, :, lanes].astype(f32) + R2[r, m, :, lanes].astype(f32)).astype(bf16)

    def scores(r):
        if r == 0:
            cos_load.wait()
            sin_load.wait()
        cos_t, sin_t = COS[...], SIN[...]
        q2_copy(r, 0).wait_recv()
        q2_copy(r, 1).wait_recv()

        def rot(m, h):
            v = total(r, m, pl.ds(h * HEAD_DIM, HEAD_DIM)).astype(f32)
            return (v * cos_t + pltpu.roll(v, HEAD_DIM // 2, 1) * sin_t).astype(bf16)

        qs, ks = [rot(0, h) for h in range(GH)], [rot(1, h) for h in range(GH)]
        sc = [lax.dot_general(q, k, (((1,), (1,)), ((), ())), preferred_element_type=f32) * HEAD_DIM ** -0.5 for q, k in zip(qs, ks)]
        sc = [jnp.where(causal, v, -1e30) for v in sc]
        ex = [jnp.exp(v - jnp.max(v, axis=1, keepdims=True)) for v in sc]
        for h in range(GH):
            PR[h] = (ex[h] / jnp.sum(ex[h], axis=1, keepdims=True)).astype(bf16)

    def values(r, p=0):
        q2_copy(r, 2, p).wait_recv()
        off, size = PARTS[p] if r == 1 else (0, GW)
        heads = range(off // HEAD_DIM, (off + size) // HEAD_DIM)
        outs = [bdot(PR[h], total(r, 2, pl.ds(h * HEAD_DIM, HEAD_DIM))).astype(bf16) for h in heads]
        OF[r, c, xx, :, off:off + size] = jnp.concatenate(outs, axis=1)
        if p == 0:
            ox_copy(r).start()
        else:
            for k in (2, 1, 3):
                ob_copy(k).start()

    def o_forward(r):
        ox_recv(r).wait_recv()
        od_copy(r).start()

    def ay_copy(r, p):
        cols = pl.ds(*((0, CH), (CH, D1 - CH))[p])
        return rcopy(AO.at[r, :, cols], AR.at[1 - r, :, cols], ay_s.at[r, p], ay_r.at[1 - r, p], ypeer)

    def heads_of(r, half):
        return jnp.concatenate([OF[r, half, 0], OF[r, half, 1]], axis=1)

    def out_own(r):
        if r == 0:
            await_all(WA.at[pl.ds(14, 2)], 3)
            await_all(WA.at[pl.ds(16, 2), :, pl.ds(0, D1 - CH)], 4)
        if r == 1:
            ob_recv(2).wait_recv()
        o = heads_of(r, c)
        ACC[:, :CH] = bdot(o, WA[14 + c])
        ACC[:, CH:] = bdot(o, WA[16 + c, :, : D1 - CH])

    def out_rest(r):
        od_recv(r).wait_recv()
        if r == 1:
            ob_recv(1).wait_recv()
            ob_recv(3).wait_recv()
        o = heads_of(r, co)
        AO[r, :, :CH] = (ACC[:, :CH] + bdot(o, WA[14 + co])).astype(bf16)
        ay_copy(r, 0).start()
        AO[r, :, CH:] = (ACC[:, CH:] + bdot(o, WA[16 + co, :, : D1 - CH])).astype(bf16)
        ay_copy(r, 1).start()

    st1_all().wait_recv()
    sums = ST1[0] + ST1[1] + ST1[2] + ST1[3]
    ST1[4] = sums
    st1_total().start()
    NB[0] = normalize(x_own, sums)
    qkv_mm(0, 0)
    qkv_s1(0, 0)
    qkv_mm(0, 1)
    qkv_s1(0, 1)
    qkv_mm(0, 2)
    for i in range(4):
        wo_load(i).start()
    for j in range(7):
        gu_load(j, 0).start()
        gu_load(j, 1).start()
    x_send.wait_recv()
    st1_total().wait_recv()
    NB[1] = normalize(XB[1].astype(f32), ST1[5])
    qkv_s1(0, 2)
    qkv_mm(1, 0)
    qkv_s1(1, 0)
    scores(0)
    qkv_mm_both(1, 1)
    values(0)
    qkv_s1(1, 1)
    qkv_mm_both(1, 2)
    wd_load().start()
    qkv_s1(1, 2)
    o_forward(0)
    out_own(0)
    out_rest(0)
    scores(1)
    values(1, 0)
    values(1, 1)
    o_forward(1)
    out_own(1)
    out_rest(1)
    for j in range(7, NJ):
        gu_load(j, 0).start()
        gu_load(j, 1).start()

    def st2_copy(r, k):
        return rcopy(ST2.at[r, 0], ST2.at[r, k], st2_s.at[r], st2_r.at[r], {"tx": lax.rem(tx + k, 4)})

    def st2_all(r):
        ref = ST2.at[r, pl.ds(1, 3)]
        return rcopy(ref, ref, st2_s.at[r], st2_r.at[r], partner)

    def residual(r):
        ay_copy(1 - r, 0).wait_recv()
        ay_copy(1 - r, 1).wait_recv()
        attn = (AO[r].astype(f32) + AR[r].astype(f32)).astype(bf16)
        h = (XB[r].astype(f32) + attn.astype(f32)).astype(bf16)
        HB[r] = h
        ST2[r, 0] = stats_tile(h.astype(f32))
        for k in range(1, 4):
            st2_copy(r, k).start()

    def norm2(r):
        st2_all(r).wait_recv()
        NB[r] = normalize(HB[r].astype(f32), ST2[r, 0] + ST2[r, 1] + ST2[r, 2] + ST2[r, 3])

    residual(1)
    norm2(1)

    def m1_copy(u, j):
        return rcopy(MP.at[lax.rem(u, NP), pl.ds(2 * co, 2)], MR1.at[j], m1_s.at[lax.rem(u, NP)], m1_r.at[lax.rem(u, 5)], partner)

    def m2_copy(u, j):
        return rcopy(MXS.at[j], MR2.at[u], m2_s.at[j], m2_r.at[u], xpeer)

    def ax_copy(u, j):
        return rcopy(AF.at[j, 2 * c + xx], AF.at[j, 2 * c + xx], ax_s.at[j], ax_r.at[j], xpeer)

    def ax_recv(u, j):
        return rcopy(AF.at[j, 2 * c + xo], AF.at[j, 2 * c + xo], ax_s.at[j], ax_r.at[j], xpeer)

    def ad_copy(u, j):
        return rcopy(AF.at[j, pl.ds(2 * c, 2)], AF.at[j, pl.ds(2 * c, 2)], ad_s.at[lax.rem(u, 3)], ad_r.at[j], partner)

    def ad_recv(u, j):
        return rcopy(AF.at[j, pl.ds(2 * co, 2)], AF.at[j, pl.ds(2 * co, 2)], ad_s.at[lax.rem(u, 3)], ad_r.at[j], partner)

    def dy_copy():
        return rcopy(DS, DR, dy_s.at[0], dy_r.at[0], ypeer)

    def stage0(u):
        half, j = lax.div(u, NJ), lax.rem(u, NJ)

        for first, last, sem in ((0, 2, 5), (2, 7, 6), (7, 9, 7)):
            @pl.when(u == first)
            def _(first=first, last=last, sem=sem):
                await_all(WA.at[pl.ds(2 * first, 2 * (last - first))], sem)

        slot = lax.rem(u, NP)
        n = NB[1 - half]
        for which in range(2):
            res = bdot(n, WA[2 * j + which]).astype(bf16)
            for b in range(4):
                MP[slot, b, which] = res[16 * b:16 * (b + 1), :]
        m1_copy(u, j).start()

    def stage1(u):
        j, slot = lax.rem(u, NJ), lax.rem(u, NP)
        m1_copy(u, j).wait_recv()
        MXS[j] = (MP[slot, 2 * c + xo].astype(f32) + MR1[j, xo].astype(f32)).astype(bf16)
        m2_copy(u, j).start()
        MR1[j, xx] = (MP[slot, 2 * c + xx].astype(f32) + MR1[j, xx].astype(f32)).astype(bf16)
        m1_copy(u, j).wait_send()

    def stage2(u):
        j = lax.rem(u, NJ)
        m2_copy(u, j).wait()
        tot = (MR1[j, xx].astype(f32) + MR2[u].astype(f32)).astype(bf16).astype(f32)
        gate, up = tot[0], tot[1]
        AF[j, 2 * c + xx] = (gate * jax.nn.sigmoid(gate) * up).astype(bf16)
        ax_copy(u, j).start()

    def stage3(u):
        j = lax.rem(u, NJ)
        ax_copy(u, j).wait_send()
        ax_recv(u, j).wait_recv()
        ad_copy(u, j).start()

    def stage4(u):
        j = lax.rem(u, NJ)

        @pl.when(u == 0)
        def _():
            wd_load().wait()

        ad_recv(u, j).wait_recv()
        a = jnp.concatenate([AF[j, b] for b in range(4)], axis=0)
        prod = bdot(a, WB[pl.ds(pl.multiple_of(j * CH, CH), CH), :])

        @pl.when(j == 0)
        def _():
            ACC[...] = prod

        @pl.when(j > 0)
        def _():
            ACC[...] += prod

        ad_copy(u, j).wait_send()

        @pl.when(u == NJ - 1)
        def _():
            DS[...] = ACC[...].astype(bf16)
            dy_copy().start()

    def step(t, carry):
        @pl.when(t == NJ - 3)
        def _():
            residual(0)

        @pl.when(t == NJ)
        def _():
            norm2(0)

        @pl.when(t < NU)
        def _():
            stage0(t)

        @pl.when((t >= L1) & (t < NU + L1))
        def _():
            stage1(t - L1)

        @pl.when((t >= L2) & (t < LATE))
        def _():
            stage2(t - L2)

        @pl.when(t == NU)
        def _():
            lax.fori_loop(LATE - L2, NU - L2, lambda u, x: (stage2(u), x)[1], 0)

        @pl.when((t >= NU) & (t < NU + L2))
        def _():
            stage2(t - L2)

        @pl.when((t >= L3) & (t < LATE - L2 + L3))
        def _():
            stage3(t - L3)

        @pl.when(t >= NU)
        def _():
            @pl.when(t < NU + LATE - L2)
            def _():
                stage3(t - (LATE - L2))

        @pl.when((t >= L4) & (t < NU))
        def _():
            stage4(t - L4)

        @pl.when(t > NU)
        def _():
            stage4(t - L4 - 1)

        return carry

    lax.fori_loop(0, NU + L4 + 1, step, 0)

    h_store = pltpu.make_async_copy(HB.at[0], h_hbm, lsem.at[1])
    h_store.start()
    dy_copy().wait_recv()
    mlp = (ACC[...] + DR[...].astype(f32)).astype(bf16)
    ay_copy(0, 0).wait_send()
    ay_copy(0, 1).wait_send()
    AO[0] = mlp
    m_store = pltpu.make_async_copy(AO.at[0], m_hbm, lsem.at[0])
    m_store.start()
    st1_all().wait_send()
    st1_total().wait_send()
    x_send.wait_send()
    for r in range(2):
        for m in range(3):
            if r == 1:
                q1_copy(r, m).wait_send()
                q2_copy(r, m).wait_send()
        if r == 1:
            q2_copy(1, 2, 1).wait_send()
            for k in range(1, 4):
                ob_copy(k).wait_send()
        ox_copy(r).wait_send()
        od_copy(r).wait_send()
        if r == 1:
            ay_copy(r, 0).wait_send()
            ay_copy(r, 1).wait_send()
        st2_all(r).wait_send()
    dy_copy().wait_send()
    h_store.wait()
    m_store.wait()


def layer_fn(x_blk, w_q, w_k, w_v, w_o, w_gate, w_up, w_down):
    bf16, f32 = jnp.bfloat16, jnp.float32
    cos_t, sin_t = rotary_tables()
    vm, dma = pltpu.VMEM, pltpu.SemaphoreType.DMA
    scratch = [
        vm((2 * NJ, D1, CH), bf16),
        vm((6 * D1, D1), bf16),
        vm((2, S, D1), bf16),
        vm((2, S, D1), bf16),
        vm((2, S, D1), bf16),
        vm((6, 8, 128), f32),
        vm((2, 4, 8, 128), f32),
        vm((3, 2, S, GW), bf16),
        vm((2, 3, 2, S, GW), bf16),
        vm((2, 3, 2, S, GW), bf16),
        vm((3, S, GW), bf16),
        vm((2, 3, S, GW), bf16),
        vm((2, 2, 2, S, GW), bf16),
        vm((2, S, D1), bf16),
        vm((2, S, D1), bf16),
        vm((NP, 4, 2, 16, CH), bf16),
        vm((NJ, 2, 2, 16, CH), bf16),
        vm((NJ, 2, 16, CH), bf16),
        vm((NU, 2, 16, CH), bf16),
        vm((NJ, 4, 16, CH), bf16),
        vm((S, D1), f32),
        vm((S, D1), bf16),
        vm((S, D1), bf16),
        vm((S, HEAD_DIM), f32),
        vm((S, HEAD_DIM), f32),
        vm((GH, S, S), bf16),
        dma((9,)), dma((3,)), dma((1,)), dma((1,)),
        dma((2,)), dma((2,)), dma((2,)), dma((2,)),
        dma((3,)), dma((2, 3)), dma((4,)), dma((7,)),
        dma((2,)), dma((2,)), dma((2,)), dma((2,)), dma((3,)), dma((3,)), dma((2, 2)), dma((2, 2)),
        dma((NP,)), dma((5,)), dma((NJ,)), dma((NU,)),
        dma((NJ,)), dma((NJ,)), dma((3,)), dma((NJ,)), dma((1,)), dma((1,)),
    ]
    h, mlp = pl.pallas_call(
        kernel,
        out_shape=[jax.ShapeDtypeStruct((S, D1), bf16)] * 2,
        in_specs=[pl.BlockSpec(memory_space=pl.ANY)] * 10,
        out_specs=[pl.BlockSpec(memory_space=pl.ANY)] * 2,
        scratch_shapes=scratch,
        compiler_params=pltpu.CompilerParams(collective_id=0, has_side_effects=True, vmem_limit_bytes=67_043_328),
    )(x_blk.reshape(S, D1), w_q, w_k, w_v, w_o, w_gate, w_up, w_down, jnp.asarray(cos_t), jnp.asarray(sin_t))
    return (h.astype(f32) + mlp.astype(f32)).astype(bf16).reshape(x_blk.shape)


def solution(mesh):
    act_spec = P(("dp", "ty"), None, "tx")
    col_spec = P("tx", "ty")
    row_spec = P("ty", "tx")
    return jax.shard_map(
        layer_fn,
        mesh=mesh,
        in_specs=(act_spec, col_spec, col_spec, col_spec, row_spec, col_spec, col_spec, row_spec),
        out_specs=act_spec,
        check_vma=False,
    )
```

```python
import functools

import jax
import jax.numpy as jnp
import numpy as np
from jax import lax
from jax.experimental import pallas as pl
from jax.experimental.pallas import tpu as pltpu
from jax.sharding import PartitionSpec as P

HEAD_DIM = 128
EPS = 1e-5
THETA = 10000.0
MESH = pl.DeviceIdType.MESH

S = 64
D1 = 1280
DFULL = 5120
GH = 5
GW = GH * HEAD_DIM
CH = 768
NJ = 9
NU = 2 * NJ
NP = 3
PARTS = ((0, 384), (384, 256))
L1, L2, L3, L4 = 1, 4, 7, 9


def rotary_tables():
    half = HEAD_DIM // 2
    inv_freq = np.float32(THETA) ** (np.float32(-2.0) * np.arange(half, dtype=np.float32) / np.float32(HEAD_DIM))
    angles = np.arange(S, dtype=np.float32)[:, None] * inv_freq.astype(np.float32)[None, :]
    cos_t = np.cos(angles.astype(np.float64)).astype(np.float32)
    sin_t = np.sin(angles.astype(np.float64)).astype(np.float32)
    return np.concatenate([cos_t, cos_t], axis=1), np.concatenate([-sin_t, sin_t], axis=1)


def bdot(a, b):
    return jnp.dot(a, b, preferred_element_type=jnp.float32)


def kernel(
    x_hbm, wq, wk, wv, wo, wg, wu, wd, cos_hbm, sin_hbm, h_hbm, m_hbm,
    WA, WB, XB, NB, HB, ST1, ST2, PS, PO, R1, XS, R2, OF, AO, AR,
    MP, MR1, MXS, MR2, AF, AZ, ACC, DS, DR, COS, SIN, PR,
    wsem, lsem, xg_s, xg_r, st1_s, st1_r, st2_s, st2_r,
    q1_s, q1_r, q2_s, q2_r, ox_s, ox_r, od_s, od_r, ay_s, ay_r,
    m1_s, m1_r, m2_s, m2_r, ax_s, ax_r, ad_s, ad_r, az_s, az_r, dy_s, dy_r,
):
    f32, bf16 = jnp.float32, jnp.bfloat16
    ty = lax.axis_index("ty")
    tx = lax.axis_index("tx")
    c = lax.rem(tx, 2)
    xx = lax.div(tx, 2)
    co, xo = 1 - c, 1 - xx
    tyo = 1 - ty
    partner = {"tx": 2 * xx + co}
    xpeer = {"tx": 2 * xo + c}
    ypeer = {"ty": tyo}

    def rcopy(src, dst, ss, rs, dev):
        return pltpu.make_async_remote_copy(src_ref=src, dst_ref=dst, send_sem=ss, recv_sem=rs, device_id=dev, device_id_type=MESH)

    x_load = pltpu.make_async_copy(x_hbm, XB.at[0], lsem.at[0])
    x_load.start()
    cos_load = pltpu.make_async_copy(cos_hbm, COS, lsem.at[1])
    sin_load = pltpu.make_async_copy(sin_hbm, SIN, lsem.at[2])

    barrier = pltpu.get_barrier_semaphore()
    for k in range(1, 4):
        pl.semaphore_signal(barrier, inc=1, device_id={"tx": lax.rem(tx + k, 4)}, device_id_type=MESH)
    pl.semaphore_signal(barrier, inc=1, device_id=ypeer, device_id_type=MESH)

    def qkv_load(m, half):
        src = (wq, wk, wv)[m].at[:, pl.ds(half * D1, D1)]
        return pltpu.make_async_copy(src, WB.at[pl.ds((2 * m + half) * D1, D1), :], wsem.at[m])

    def wo_load(i):
        kh, wide = i % 2, i // 2
        if wide == 0:
            return pltpu.make_async_copy(wo.at[pl.ds(kh * D1, D1), pl.ds(0, CH)], WA.at[14 + i], wsem.at[3])
        return pltpu.make_async_copy(wo.at[pl.ds(kh * D1, D1), pl.ds(CH, D1 - CH)], WA.at[14 + i, :, pl.ds(0, D1 - CH)], wsem.at[4])

    def gu_load(j, which):
        group = 5 if j < 2 else 6 if j < 7 else 7
        return pltpu.make_async_copy((wg, wu)[which].at[:, pl.ds(j * CH, CH)], WA.at[2 * j + which], wsem.at[group])

    def wd_load():
        return pltpu.make_async_copy(wd, WB.at[pl.ds(0, NJ * CH), :], wsem.at[8])

    def await_all(ref, sem):
        pltpu.make_async_copy(ref, ref, wsem.at[sem]).wait()

    for m in range(3):
        for half in range(2):
            qkv_load(m, half).start()
    cos_load.start()
    sin_load.start()

    eye = lax.broadcasted_iota(jnp.int32, (S, 128), 0) == lax.broadcasted_iota(jnp.int32, (S, 128), 1)
    row8 = lax.broadcasted_iota(jnp.int32, (8, 128), 0)

    def stats_tile(v):
        s = jnp.sum(v, axis=1, keepdims=True)
        q = jnp.sum(v * v, axis=1, keepdims=True)
        srow = jnp.sum(jnp.where(eye, s, 0.0), axis=0, keepdims=True)
        qrow = jnp.sum(jnp.where(eye, q, 0.0), axis=0, keepdims=True)
        return jnp.where(row8 == 0, srow, jnp.where(row8 == 1, qrow, 0.0))

    def normalize(v, tot):
        mean = tot[0:1, :] / DFULL
        var = tot[1:2, :] / DFULL - mean * mean
        rstd = lax.rsqrt(var + EPS)
        mean_c = jnp.sum(jnp.where(eye, mean, 0.0), axis=1, keepdims=True)
        rstd_c = jnp.sum(jnp.where(eye, rstd, 0.0), axis=1, keepdims=True)
        return ((v - mean_c) * rstd_c).astype(bf16)

    x_load.wait()
    x_own = XB[0].astype(f32)
    ST1[0] = stats_tile(x_own)
    pl.semaphore_wait(barrier, 4)

    def st1_copy(k):
        return rcopy(ST1.at[0], ST1.at[k], st1_s.at[0], st1_r.at[0], {"tx": lax.rem(tx + k, 4)})

    def st1_all():
        ref = ST1.at[pl.ds(1, 3)]
        return rcopy(ref, ref, st1_s.at[0], st1_r.at[0], partner)

    def st1_total():
        return rcopy(ST1.at[4], ST1.at[5], st1_s.at[1], st1_r.at[1], ypeer)

    for k in range(1, 4):
        st1_copy(k).start()
    x_send = rcopy(XB.at[0], XB.at[1], xg_s.at[0], xg_r.at[0], ypeer)
    x_send.start()

    def q1_copy(r, m):
        return rcopy(PS.at[m], R1.at[r, m], q1_s.at[m], q1_r.at[r, m], partner)

    def q2_copy(r, m, p=0):
        lanes = pl.ds(*(PARTS[p] if r == 1 and m == 2 else (0, GW)))
        return rcopy(XS.at[m, :, lanes], R2.at[r, m, :, lanes], q2_s.at[m + p], q2_r.at[3 * r + m + p], xpeer)

    def qkv_dot(r, m, half):
        return bdot(NB[r], WB[pl.ds(pl.multiple_of((2 * m + half) * D1, D1), D1), :]).astype(bf16)

    def put_send(r, m, res):
        if r == 1:
            q1_copy(0, m).wait_send()
        PS[m, 0] = res[:, :GW]
        PS[m, 1] = res[:, GW:]
        q1_copy(r, m).start()

    def put_keep(r, m, res):
        PO[r, m, 0] = res[:, :GW]
        PO[r, m, 1] = res[:, GW:]

    def qkv_mm(r, m):
        if r == 0:
            await_all(WB.at[pl.ds(2 * m * D1, 2 * D1), :], m)
        put_send(r, m, qkv_dot(r, m, co))
        put_keep(r, m, qkv_dot(r, m, c))

    def qkv_mm_both(r, m):
        sent, kept = qkv_dot(r, m, co), qkv_dot(r, m, c)
        put_send(r, m, sent)
        put_keep(r, m, kept)

    def qkv_s1(r, m):
        q1_copy(r, m).wait_recv()
        if r == 1:
            q2_copy(0, m).wait_send()
        XS[m] = (PO[r, m, xo].astype(f32) + R1[r, m, xo].astype(f32)).astype(bf16)
        q2_copy(r, m).start()
        if r == 1 and m == 2:
            q2_copy(r, m, 1).start()

    causal = lax.broadcasted_iota(jnp.int32, (S, S), 0) >= lax.broadcasted_iota(jnp.int32, (S, S), 1)

    def o_lanes(r, p):
        return pl.ds(*(PARTS[p] if r == 1 else (0, GW)))

    def ox_copy(r, p=0):
        ref = OF.at[r, c, xx, :, o_lanes(r, p)]
        return rcopy(ref, ref, ox_s.at[r + p], ox_r.at[r + p], xpeer)

    def ox_recv(r, p=0):
        ref = OF.at[r, c, xo, :, o_lanes(r, p)]
        return rcopy(ref, ref, ox_s.at[r + p], ox_r.at[r + p], xpeer)

    def od_copy(r, p=0):
        ref = OF.at[r, c, :, :, o_lanes(r, p)]
        return rcopy(ref, ref, od_s.at[r + p], od_r.at[r + p], partner)

    def od_recv(r, p=0):
        ref = OF.at[r, co, :, :, o_lanes(r, p)]
        return rcopy(ref, ref, od_s.at[r + p], od_r.at[r + p], partner)

    def total(r, m, lanes):
        return (PO[r, m, xx, :, lanes].astype(f32) + R1[r, m, xx, :, lanes].astype(f32) + R2[r, m, :, lanes].astype(f32)).astype(bf16)

    def scores(r):
        if r == 0:
            cos_load.wait()
            sin_load.wait()
        cos_t, sin_t = COS[...], SIN[...]
        q2_copy(r, 0).wait_recv()
        q2_copy(r, 1).wait_recv()

        def rot(m, h):
            v = total(r, m, pl.ds(h * HEAD_DIM, HEAD_DIM)).astype(f32)
            return (v * cos_t + pltpu.roll(v, HEAD_DIM // 2, 1) * sin_t).astype(bf16)

        qs, ks = [rot(0, h) for h in range(GH)], [rot(1, h) for h in range(GH)]
        sc = [lax.dot_general(q, k, (((1,), (1,)), ((), ())), preferred_element_type=f32) * HEAD_DIM ** -0.5 for q, k in zip(qs, ks)]
        sc = [jnp.where(causal, v, -1e30) for v in sc]
        ex = [jnp.exp(v - jnp.max(v, axis=1, keepdims=True)) for v in sc]
        for h in range(GH):
            PR[h] = (ex[h] / jnp.sum(ex[h], axis=1, keepdims=True)).astype(bf16)

    def values(r, p=0):
        q2_copy(r, 2, p).wait_recv()
        off, size = PARTS[p] if r == 1 else (0, GW)
        heads = range(off // HEAD_DIM, (off + size) // HEAD_DIM)
        outs = [bdot(PR[h], total(r, 2, pl.ds(h * HEAD_DIM, HEAD_DIM))).astype(bf16) for h in heads]
        OF[r, c, xx, :, off:off + size] = jnp.concatenate(outs, axis=1)
        ox_copy(r, p).start()

    def o_forward(r, p=0):
        ox_recv(r, p).wait_recv()
        od_copy(r, p).start()

    def ay_copy(r, p):
        cols = pl.ds(*((0, CH), (CH, D1 - CH))[p])
        return rcopy(AO.at[r, :, cols], AR.at[1 - r, :, cols], ay_s.at[r, p], ay_r.at[1 - r, p], ypeer)

    def heads_of(r, half):
        return jnp.concatenate([OF[r, half, 0], OF[r, half, 1]], axis=1)

    def out_own(r):
        if r == 0:
            await_all(WA.at[pl.ds(14, 2)], 3)
            await_all(WA.at[pl.ds(16, 2), :, pl.ds(0, D1 - CH)], 4)
        o = heads_of(r, c)
        ACC[:, :CH] = bdot(o, WA[14 + c])
        ACC[:, CH:] = bdot(o, WA[16 + c, :, : D1 - CH])

    def out_rest(r):
        od_recv(r).wait_recv()
        if r == 1:
            od_recv(r, 1).wait_recv()
        o = heads_of(r, co)
        AO[r, :, :CH] = (ACC[:, :CH] + bdot(o, WA[14 + co])).astype(bf16)
        ay_copy(r, 0).start()
        AO[r, :, CH:] = (ACC[:, CH:] + bdot(o, WA[16 + co, :, : D1 - CH])).astype(bf16)
        ay_copy(r, 1).start()

    st1_all().wait_recv()
    sums = ST1[0] + ST1[1] + ST1[2] + ST1[3]
    ST1[4] = sums
    st1_total().start()
    NB[0] = normalize(x_own, sums)
    qkv_mm(0, 0)
    qkv_s1(0, 0)
    qkv_mm(0, 1)
    qkv_s1(0, 1)
    qkv_mm(0, 2)
    for i in range(4):
        wo_load(i).start()
    for j in range(7):
        gu_load(j, 0).start()
        gu_load(j, 1).start()
    x_send.wait_recv()
    st1_total().wait_recv()
    NB[1] = normalize(XB[1].astype(f32), ST1[5])
    qkv_s1(0, 2)
    qkv_mm(1, 0)
    qkv_s1(1, 0)
    scores(0)
    qkv_mm_both(1, 1)
    values(0)
    qkv_s1(1, 1)
    qkv_mm_both(1, 2)
    wd_load().start()
    qkv_s1(1, 2)
    o_forward(0)
    out_own(0)
    out_rest(0)
    scores(1)
    values(1, 0)
    values(1, 1)
    o_forward(1, 0)
    o_forward(1, 1)
    out_own(1)
    out_rest(1)
    for j in range(7, NJ):
        gu_load(j, 0).start()
        gu_load(j, 1).start()

    def st2_copy(r, k):
        return rcopy(ST2.at[r, 0], ST2.at[r, k], st2_s.at[r], st2_r.at[r], {"tx": lax.rem(tx + k, 4)})

    def st2_all(r):
        ref = ST2.at[r, pl.ds(1, 3)]
        return rcopy(ref, ref, st2_s.at[r], st2_r.at[r], partner)

    def residual(r):
        ay_copy(1 - r, 0).wait_recv()
        ay_copy(1 - r, 1).wait_recv()
        attn = (AO[r].astype(f32) + AR[r].astype(f32)).astype(bf16)
        h = (XB[r].astype(f32) + attn.astype(f32)).astype(bf16)
        HB[r] = h
        ST2[r, 0] = stats_tile(h.astype(f32))
        for k in range(1, 4):
            st2_copy(r, k).start()

    def norm2(r):
        st2_all(r).wait_recv()
        NB[r] = normalize(HB[r].astype(f32), ST2[r, 0] + ST2[r, 1] + ST2[r, 2] + ST2[r, 3])

    residual(1)
    norm2(1)

    def m1_copy(u, j):
        return rcopy(MP.at[lax.rem(u, NP), pl.ds(2 * co, 2)], MR1.at[j], m1_s.at[lax.rem(u, NP)], m1_r.at[lax.rem(u, 5)], partner)

    def m2_copy(u, j):
        return rcopy(MXS.at[lax.rem(u, 5)], MR2.at[j], m2_s.at[lax.rem(u, 5)], m2_r.at[j], xpeer)

    def ax_copy(u, j):
        return rcopy(AF.at[j, 2 * c + xx], AF.at[j, 2 * c + xx], ax_s.at[lax.rem(u, 4)], ax_r.at[j], xpeer)

    def ax_recv(u, j):
        return rcopy(AF.at[j, 2 * c + xo], AF.at[j, 2 * c + xo], ax_s.at[lax.rem(u, 4)], ax_r.at[j], xpeer)

    def ad_copy(u, j):
        return rcopy(AF.at[j, pl.ds(2 * c, 2)], AF.at[j, pl.ds(2 * c, 2)], ad_s.at[lax.rem(u, 3)], ad_r.at[j], partner)

    def ad_recv(u, j):
        return rcopy(AF.at[j, pl.ds(2 * co, 2)], AF.at[j, pl.ds(2 * co, 2)], ad_s.at[lax.rem(u, 3)], ad_r.at[j], partner)

    def az_copy(k):
        return rcopy(AZ.at[2 * c + xx], AZ.at[2 * c + xx], az_s.at[k - 1], az_r.at[k - 1], {"tx": lax.rem(tx + k, 4)})

    def az_recv(k):
        src = lax.rem(tx + 4 - k, 4)
        block = AZ.at[2 * lax.rem(src, 2) + lax.div(src, 2)]
        return rcopy(block, block, az_s.at[k - 1], az_r.at[k - 1], partner)

    def dy_copy():
        return rcopy(DS, DR, dy_s.at[0], dy_r.at[0], ypeer)

    def stage0(u):
        half, j = lax.div(u, NJ), lax.rem(u, NJ)

        for first, last, sem in ((0, 2, 5), (2, 7, 6), (7, 9, 7)):
            @pl.when(u == first)
            def _(first=first, last=last, sem=sem):
                await_all(WA.at[pl.ds(2 * first, 2 * (last - first))], sem)

        slot = lax.rem(u, NP)
        n = NB[1 - half]
        for which in range(2):
            res = bdot(n, WA[2 * j + which]).astype(bf16)
            for b in range(4):
                MP[slot, b, which] = res[16 * b:16 * (b + 1), :]
        m1_copy(u, j).start()

    def stage1(u):
        j, slot = lax.rem(u, NJ), lax.rem(u, NP)
        m1_copy(u, j).wait_recv()
        MXS[lax.rem(u, 5)] = (MP[slot, 2 * c + xo].astype(f32) + MR1[j, xo].astype(f32)).astype(bf16)
        m2_copy(u, j).start()
        MR1[j, xx] = (MP[slot, 2 * c + xx].astype(f32) + MR1[j, xx].astype(f32)).astype(bf16)
        m1_copy(u, j).wait_send()

    def stage2(u):
        j = lax.rem(u, NJ)
        m2_copy(u, j).wait()
        tot = (MR1[j, xx].astype(f32) + MR2[j].astype(f32)).astype(bf16).astype(f32)
        gate, up = tot[0], tot[1]
        act = (gate * jax.nn.sigmoid(gate) * up).astype(bf16)

        @pl.when(u < NU - 1)
        def _():
            AF[j, 2 * c + xx] = act
            ax_copy(u, j).start()

        @pl.when(u == NU - 1)
        def _():
            AZ[2 * c + xx] = act
            for k in (2, 1, 3):
                az_copy(k).start()

    def stage3(u):
        j = lax.rem(u, NJ)
        ax_copy(u, j).wait_send()
        ax_recv(u, j).wait_recv()
        ad_copy(u, j).start()

    def stage4(u):
        j = lax.rem(u, NJ)

        @pl.when(u == 0)
        def _():
            wd_load().wait()

        ad_recv(u, j).wait_recv()
        a = jnp.concatenate([AF[j, b] for b in range(4)], axis=0)
        prod = bdot(a, WB[pl.ds(pl.multiple_of(j * CH, CH), CH), :])

        @pl.when(j == 0)
        def _():
            ACC[...] = prod

        @pl.when(j > 0)
        def _():
            ACC[...] += prod

        ad_copy(u, j).wait_send()

        @pl.when(u == NJ - 1)
        def _():
            DS[...] = ACC[...].astype(bf16)
            dy_copy().start()

    def step(t, carry):
        @pl.when(t == NJ - 3)
        def _():
            residual(0)

        @pl.when(t == NJ)
        def _():
            norm2(0)

        @pl.when(t < NU)
        def _():
            stage0(t)

        for lag, stage in ((L1, stage1), (L2, stage2), (L3, stage3), (L4, stage4)):
            @pl.when((t >= lag) & (t < NU + lag - (lag >= L3)))
            def _(lag=lag, stage=stage):
                stage(t - lag)

        return carry

    lax.fori_loop(0, NU + L4 - 1, step, 0)

    h_store = pltpu.make_async_copy(HB.at[0], h_hbm, lsem.at[1])
    h_store.start()
    dy_copy().wait_recv()
    for k in range(1, 4):
        az_recv(k).wait_recv()
    last = bdot(jnp.concatenate([AZ[b] for b in range(4)], axis=0), WB[(NJ - 1) * CH:NJ * CH, :])
    mlp = (ACC[...] + last + DR[...].astype(f32)).astype(bf16)
    ay_copy(0, 0).wait_send()
    ay_copy(0, 1).wait_send()
    AO[0] = mlp
    m_store = pltpu.make_async_copy(AO.at[0], m_hbm, lsem.at[0])
    m_store.start()
    st1_all().wait_send()
    st1_total().wait_send()
    x_send.wait_send()
    for r in range(2):
        for m in range(3):
            if r == 1:
                q1_copy(r, m).wait_send()
                q2_copy(r, m).wait_send()
        if r == 1:
            q2_copy(1, 2, 1).wait_send()
        for p in range(r + 1):
            ox_copy(r, p).wait_send()
            od_copy(r, p).wait_send()
        if r == 1:
            ay_copy(r, 0).wait_send()
            ay_copy(r, 1).wait_send()
        st2_all(r).wait_send()
    dy_copy().wait_send()
    for k in range(1, 4):
        az_copy(k).wait_send()
    h_store.wait()
    m_store.wait()


def layer_fn(x_blk, w_q, w_k, w_v, w_o, w_gate, w_up, w_down):
    bf16, f32 = jnp.bfloat16, jnp.float32
    cos_t, sin_t = rotary_tables()
    vm, dma = pltpu.VMEM, pltpu.SemaphoreType.DMA
    scratch = [
        vm((2 * NJ, D1, CH), bf16),
        vm((6 * D1, D1), bf16),
        vm((2, S, D1), bf16),
        vm((2, S, D1), bf16),
        vm((2, S, D1), bf16),
        vm((6, 8, 128), f32),
        vm((2, 4, 8, 128), f32),
        vm((3, 2, S, GW), bf16),
        vm((2, 3, 2, S, GW), bf16),
        vm((2, 3, 2, S, GW), bf16),
        vm((3, S, GW), bf16),
        vm((2, 3, S, GW), bf16),
        vm((2, 2, 2, S, GW), bf16),
        vm((2, S, D1), bf16),
        vm((2, S, D1), bf16),
        vm((NP, 4, 2, 16, CH), bf16),
        vm((NJ, 2, 2, 16, CH), bf16),
        vm((5, 2, 16, CH), bf16),
        vm((NJ, 2, 16, CH), bf16),
        vm((NJ, 4, 16, CH), bf16),
        vm((4, 16, CH), bf16),
        vm((S, D1), f32),
        vm((S, D1), bf16),
        vm((S, D1), bf16),
        vm((S, HEAD_DIM), f32),
        vm((S, HEAD_DIM), f32),
        vm((GH, S, S), bf16),
        dma((9,)), dma((3,)), dma((1,)), dma((1,)),
        dma((2,)), dma((2,)), dma((2,)), dma((2,)),
        dma((3,)), dma((2, 3)), dma((4,)), dma((7,)),
        dma((3,)), dma((3,)), dma((3,)), dma((3,)), dma((2, 2)), dma((2, 2)),
        dma((NP,)), dma((5,)), dma((5,)), dma((NJ,)),
        dma((4,)), dma((NJ,)), dma((3,)), dma((NJ,)), dma((3,)), dma((3,)), dma((1,)), dma((1,)),
    ]
    h, mlp = pl.pallas_call(
        kernel,
        out_shape=[jax.ShapeDtypeStruct((S, D1), bf16)] * 2,
        in_specs=[pl.BlockSpec(memory_space=pl.ANY)] * 10,
        out_specs=[pl.BlockSpec(memory_space=pl.ANY)] * 2,
        scratch_shapes=scratch,
        compiler_params=pltpu.CompilerParams(collective_id=0, has_side_effects=True, vmem_limit_bytes=67_043_328),
    )(x_blk.reshape(S, D1), w_q, w_k, w_v, w_o, w_gate, w_up, w_down, jnp.asarray(cos_t), jnp.asarray(sin_t))
    return (h.astype(f32) + mlp.astype(f32)).astype(bf16).reshape(x_blk.shape)


def solution(mesh):
    act_spec = P(("dp", "ty"), None, "tx")
    col_spec = P("tx", "ty")
    row_spec = P("ty", "tx")
    return jax.shard_map(
        layer_fn,
        mesh=mesh,
        in_specs=(act_spec, col_spec, col_spec, col_spec, row_spec, col_spec, col_spec, row_spec),
        out_specs=act_spec,
        check_vma=False,
    )
```

```python
import functools

import jax
import jax.numpy as jnp
import numpy as np
from jax import lax
from jax.experimental import pallas as pl
from jax.experimental.pallas import tpu as pltpu
from jax.sharding import PartitionSpec as P

HEAD_DIM = 128
EPS = 1e-5
THETA = 10000.0
MESH = pl.DeviceIdType.MESH

S = 64
D1 = 1280
DFULL = 5120
GH = 5
GW = GH * HEAD_DIM
CH = 768
NJ = 9
NU = 2 * NJ
NP = 3
PARTS = ((0, 384), (384, 256))
L1, L2, L3, L4 = 1, 4, 7, 9


def rotary_tables():
    half = HEAD_DIM // 2
    inv_freq = np.float32(THETA) ** (np.float32(-2.0) * np.arange(half, dtype=np.float32) / np.float32(HEAD_DIM))
    angles = np.arange(S, dtype=np.float32)[:, None] * inv_freq.astype(np.float32)[None, :]
    cos_t = np.cos(angles.astype(np.float64)).astype(np.float32)
    sin_t = np.sin(angles.astype(np.float64)).astype(np.float32)
    return np.concatenate([cos_t, cos_t], axis=1), np.concatenate([-sin_t, sin_t], axis=1)


def bdot(a, b):
    return jnp.dot(a, b, preferred_element_type=jnp.float32)


def kernel(
    x_hbm, wq, wk, wv, wo, wg, wu, wd, cos_hbm, sin_hbm, h_hbm, m_hbm,
    WA, WB, XB, NB, HB, ST1, ST2, PS, PO, R1, XS, R2, OF, AO, AR,
    MP, MR1, MXS, MR2, AF, AZ, ACC, DS, DR, COS, SIN, PR,
    wsem, lsem, xg_s, xg_r, st1_s, st1_r, st2_s, st2_r,
    q1_s, q1_r, q2_s, q2_r, ox_s, ox_r, od_s, od_r, oe_s, oe_r, ay_s, ay_r,
    az_s, az_r, dy_s, dy_r,
):
    f32, bf16 = jnp.float32, jnp.bfloat16
    ty = lax.axis_index("ty")
    tx = lax.axis_index("tx")
    c = lax.rem(tx, 2)
    xx = lax.div(tx, 2)
    co, xo = 1 - c, 1 - xx
    tyo = 1 - ty
    partner = {"tx": 2 * xx + co}
    xpeer = {"tx": 2 * xo + c}
    ypeer = {"ty": tyo}

    def rcopy(src, dst, ss, rs, dev):
        return pltpu.make_async_remote_copy(src_ref=src, dst_ref=dst, send_sem=ss, recv_sem=rs, device_id=dev, device_id_type=MESH)

    x_load = pltpu.make_async_copy(x_hbm, XB.at[0], lsem.at[0])
    x_load.start()
    cos_load = pltpu.make_async_copy(cos_hbm, COS, lsem.at[1])
    sin_load = pltpu.make_async_copy(sin_hbm, SIN, lsem.at[2])

    barrier = pltpu.get_barrier_semaphore()
    for k in range(1, 4):
        pl.semaphore_signal(barrier, inc=1, device_id={"tx": lax.rem(tx + k, 4)}, device_id_type=MESH)
    pl.semaphore_signal(barrier, inc=1, device_id=ypeer, device_id_type=MESH)

    def qkv_load(m, half):
        src = (wq, wk, wv)[m].at[:, pl.ds(half * D1, D1)]
        return pltpu.make_async_copy(src, WB.at[pl.ds((2 * m + half) * D1, D1), :], wsem.at[m])

    def wo_load(i):
        kh, wide = i % 2, i // 2
        if wide == 0:
            return pltpu.make_async_copy(wo.at[pl.ds(kh * D1, D1), pl.ds(0, CH)], WA.at[14 + i], wsem.at[3])
        return pltpu.make_async_copy(wo.at[pl.ds(kh * D1, D1), pl.ds(CH, D1 - CH)], WA.at[14 + i, :, pl.ds(0, D1 - CH)], wsem.at[4])

    def gu_load(j, which):
        group = 5 if j < 2 else 6 if j < 7 else 7
        return pltpu.make_async_copy((wg, wu)[which].at[:, pl.ds(j * CH, CH)], WA.at[2 * j + which], wsem.at[group])

    def wd_load():
        return pltpu.make_async_copy(wd, WB.at[pl.ds(0, NJ * CH), :], wsem.at[8])

    def await_all(ref, sem):
        pltpu.make_async_copy(ref, ref, wsem.at[sem]).wait()

    for m in range(3):
        for half in range(2):
            qkv_load(m, half).start()
    cos_load.start()
    sin_load.start()

    eye = lax.broadcasted_iota(jnp.int32, (S, 128), 0) == lax.broadcasted_iota(jnp.int32, (S, 128), 1)
    row8 = lax.broadcasted_iota(jnp.int32, (8, 128), 0)

    def stats_tile(v):
        s = jnp.sum(v, axis=1, keepdims=True)
        q = jnp.sum(v * v, axis=1, keepdims=True)
        srow = jnp.sum(jnp.where(eye, s, 0.0), axis=0, keepdims=True)
        qrow = jnp.sum(jnp.where(eye, q, 0.0), axis=0, keepdims=True)
        return jnp.where(row8 == 0, srow, jnp.where(row8 == 1, qrow, 0.0))

    def normalize(v, tot):
        mean = tot[0:1, :] / DFULL
        var = tot[1:2, :] / DFULL - mean * mean
        rstd = lax.rsqrt(var + EPS)
        mean_c = jnp.sum(jnp.where(eye, mean, 0.0), axis=1, keepdims=True)
        rstd_c = jnp.sum(jnp.where(eye, rstd, 0.0), axis=1, keepdims=True)
        return ((v - mean_c) * rstd_c).astype(bf16)

    x_load.wait()
    x_own = XB[0].astype(f32)
    ST1[0] = stats_tile(x_own)
    pl.semaphore_wait(barrier, 4)

    def st1_copy(k):
        return rcopy(ST1.at[0], ST1.at[k], st1_s.at[0], st1_r.at[0], {"tx": lax.rem(tx + k, 4)})

    def st1_all():
        ref = ST1.at[pl.ds(1, 3)]
        return rcopy(ref, ref, st1_s.at[0], st1_r.at[0], partner)

    def st1_total():
        return rcopy(ST1.at[4], ST1.at[5], st1_s.at[1], st1_r.at[1], ypeer)

    for k in range(1, 4):
        st1_copy(k).start()
    x_send = rcopy(XB.at[0], XB.at[1], xg_s.at[0], xg_r.at[0], ypeer)
    x_send.start()

    def q1_copy(r, m):
        return rcopy(PS.at[m], R1.at[r, m], q1_s.at[m], q1_r.at[3 * r + m], partner)

    def q2_copy(r, m, p=0):
        lanes = pl.ds(*(PARTS[p] if r == 1 and m == 2 else (0, GW)))
        return rcopy(XS.at[m, :, lanes], R2.at[r, m, :, lanes], q2_s.at[m + p], q2_r.at[3 * r + m + p], xpeer)

    def qkv_dot(r, m, half):
        return bdot(NB[r], WB[pl.ds(pl.multiple_of((2 * m + half) * D1, D1), D1), :]).astype(bf16)

    def put_send(r, m, res):
        if r == 1:
            q1_copy(0, m).wait_send()
        PS[m, 0] = res[:, :GW]
        PS[m, 1] = res[:, GW:]
        q1_copy(r, m).start()

    def put_keep(r, m, res):
        PO[r, m, 0] = res[:, :GW]
        PO[r, m, 1] = res[:, GW:]

    def qkv_mm(r, m):
        if r == 0:
            await_all(WB.at[pl.ds(2 * m * D1, 2 * D1), :], m)
        put_send(r, m, qkv_dot(r, m, co))
        put_keep(r, m, qkv_dot(r, m, c))

    def qkv_mm_both(r, m):
        sent, kept = qkv_dot(r, m, co), qkv_dot(r, m, c)
        put_send(r, m, sent)
        put_keep(r, m, kept)

    def qkv_s1(r, m):
        q1_copy(r, m).wait_recv()
        if r == 1:
            q2_copy(0, m).wait_send()
        XS[m] = (PO[r, m, xo].astype(f32) + R1[r, m, xo].astype(f32)).astype(bf16)
        q2_copy(r, m).start()
        if r == 1 and m == 2:
            q2_copy(r, m, 1).start()

    causal = lax.broadcasted_iota(jnp.int32, (S, S), 0) >= lax.broadcasted_iota(jnp.int32, (S, S), 1)

    def o_lanes(r, p):
        return pl.ds(*(PARTS[p] if r == 1 else (0, GW)))

    def ox_copy(r, p=0):
        ref = OF.at[r, c, xx, :, o_lanes(r, p)]
        return rcopy(ref, ref, ox_s.at[r + p], ox_r.at[r + p], xpeer)

    def ox_recv(r, p=0):
        ref = OF.at[r, c, xo, :, o_lanes(r, p)]
        return rcopy(ref, ref, ox_s.at[r + p], ox_r.at[r + p], xpeer)

    def od_copy(r, p=0):
        ref = OF.at[r, c, xo, :, o_lanes(r, p)]
        return rcopy(ref, ref, od_s.at[r + p], od_r.at[r + p], partner)

    def od_recv(r, p=0):
        ref = OF.at[r, co, xo, :, o_lanes(r, p)]
        return rcopy(ref, ref, od_s.at[r + p], od_r.at[r + p], partner)

    def oe_copy(r):
        return rcopy(OF.at[r, c, xx], OF.at[r, c, xx], oe_s.at[r], oe_r.at[r], partner)

    def oe_recv(r):
        return rcopy(OF.at[r, co, xx], OF.at[r, co, xx], oe_s.at[r], oe_r.at[r], partner)

    def total(r, m, lanes):
        return (PO[r, m, xx, :, lanes].astype(f32) + R1[r, m, xx, :, lanes].astype(f32) + R2[r, m, :, lanes].astype(f32)).astype(bf16)

    def scores(r):
        if r == 0:
            cos_load.wait()
            sin_load.wait()
        cos_t, sin_t = COS[...], SIN[...]
        q2_copy(r, 0).wait_recv()
        q2_copy(r, 1).wait_recv()

        def rot(m, h):
            v = total(r, m, pl.ds(h * HEAD_DIM, HEAD_DIM)).astype(f32)
            return (v * cos_t + pltpu.roll(v, HEAD_DIM // 2, 1) * sin_t).astype(bf16)

        qs, ks = [rot(0, h) for h in range(GH)], [rot(1, h) for h in range(GH)]
        sc = [lax.dot_general(q, k, (((1,), (1,)), ((), ())), preferred_element_type=f32) * HEAD_DIM ** -0.5 for q, k in zip(qs, ks)]
        sc = [jnp.where(causal, v, -1e30) for v in sc]
        ex = [jnp.exp(v - jnp.max(v, axis=1, keepdims=True)) for v in sc]
        for h in range(GH):
            PR[h] = (ex[h] / jnp.sum(ex[h], axis=1, keepdims=True)).astype(bf16)

    def values(r, p=0):
        q2_copy(r, 2, p).wait_recv()
        off, size = PARTS[p] if r == 1 else (0, GW)
        heads = range(off // HEAD_DIM, (off + size) // HEAD_DIM)
        outs = [bdot(PR[h], total(r, 2, pl.ds(h * HEAD_DIM, HEAD_DIM))).astype(bf16) for h in heads]
        OF[r, c, xx, :, off:off + size] = jnp.concatenate(outs, axis=1)
        ox_copy(r, p).start()
        if r == 0 or p == 1:
            oe_copy(r).start()

    def o_forward(r, p=0):
        ox_recv(r, p).wait_recv()
        od_copy(r, p).start()

    def ay_copy(r, p):
        cols = pl.ds(*((0, CH), (CH, D1 - CH))[p])
        return rcopy(AO.at[r, :, cols], AR.at[1 - r, :, cols], ay_s.at[r, p], ay_r.at[1 - r, p], ypeer)

    def out_block(r, cb, xb, first=False):
        o, rows = OF[r, cb, xb], pl.ds(pl.multiple_of(xb * GW, GW), GW)
        for cols, prod in ((slice(0, CH), bdot(o, WA[14 + cb, rows, :])), (slice(CH, D1), bdot(o, WA[16 + cb, rows, : D1 - CH]))):
            ACC[:, cols] = prod if first else ACC[:, cols] + prod

    def out_last(r):
        od_recv(r).wait_recv()
        if r == 1:
            od_recv(r, 1).wait_recv()
        o, rows = OF[r, co, xo], pl.ds(pl.multiple_of(xo * GW, GW), GW)
        AO[r, :, :CH] = (ACC[:, :CH] + bdot(o, WA[14 + co, rows, :])).astype(bf16)
        ay_copy(r, 0).start()
        AO[r, :, CH:] = (ACC[:, CH:] + bdot(o, WA[16 + co, rows, : D1 - CH])).astype(bf16)
        ay_copy(r, 1).start()

    st1_all().wait_recv()
    sums = ST1[0] + ST1[1] + ST1[2] + ST1[3]
    ST1[4] = sums
    st1_total().start()
    NB[0] = normalize(x_own, sums)
    qkv_mm(0, 0)
    qkv_s1(0, 0)
    qkv_mm(0, 1)
    qkv_s1(0, 1)
    qkv_mm(0, 2)
    for i in range(4):
        wo_load(i).start()
    for j in range(7):
        gu_load(j, 0).start()
        gu_load(j, 1).start()
    x_send.wait_recv()
    st1_total().wait_recv()
    NB[1] = normalize(XB[1].astype(f32), ST1[5])
    qkv_s1(0, 2)
    qkv_mm(1, 0)
    qkv_s1(1, 0)
    scores(0)
    qkv_mm_both(1, 1)
    values(0)
    qkv_s1(1, 1)
    qkv_mm_both(1, 2)
    wd_load().start()
    qkv_s1(1, 2)
    await_all(WA.at[pl.ds(14, 2)], 3)
    await_all(WA.at[pl.ds(16, 2), :, pl.ds(0, D1 - CH)], 4)
    out_block(0, c, xx, True)
    o_forward(0)
    oe_recv(0).wait_recv()
    out_block(0, co, xx)
    out_block(0, c, xo)
    out_last(0)
    scores(1)
    values(1, 0)
    values(1, 1)
    out_block(1, c, xx, True)
    oe_recv(1).wait_recv()
    out_block(1, co, xx)
    o_forward(1, 0)
    o_forward(1, 1)
    out_block(1, c, xo)
    out_last(1)
    for j in range(7, NJ):
        gu_load(j, 0).start()
        gu_load(j, 1).start()

    def st2_copy(r, k):
        return rcopy(ST2.at[r, 0], ST2.at[r, k], st2_s.at[r], st2_r.at[r], {"tx": lax.rem(tx + k, 4)})

    def st2_all(r):
        ref = ST2.at[r, pl.ds(1, 3)]
        return rcopy(ref, ref, st2_s.at[r], st2_r.at[r], partner)

    def residual(r):
        ay_copy(1 - r, 0).wait_recv()
        ay_copy(1 - r, 1).wait_recv()
        attn = (AO[r].astype(f32) + AR[r].astype(f32)).astype(bf16)
        h = (XB[r].astype(f32) + attn.astype(f32)).astype(bf16)
        HB[r] = h
        ST2[r, 0] = stats_tile(h.astype(f32))
        for k in range(1, 4):
            st2_copy(r, k).start()

    def norm2(r):
        st2_all(r).wait_recv()
        NB[r] = normalize(HB[r].astype(f32), ST2[r, 0] + ST2[r, 1] + ST2[r, 2] + ST2[r, 3])

    residual(1)
    for m in range(3):
        q1_copy(1, m).wait_send()
        q2_copy(1, m).wait_send()
    q2_copy(1, 2, 1).wait_send()
    for r, p in ((0, 0), (1, 0), (1, 1)):
        ox_copy(r, p).wait_send()
        od_copy(r, p).wait_send()
    for r in range(2):
        oe_copy(r).wait_send()
    norm2(1)

    def m1_copy(u, j):
        return rcopy(MP.at[lax.rem(u, NP), pl.ds(2 * co, 2)], MR1.at[j], q1_s.at[lax.rem(u, NP)], q1_r.at[lax.rem(u, 5)], partner)

    def m2_copy(u, j):
        return rcopy(MXS.at[lax.rem(u, 5)], MR2.at[j], q2_s.at[lax.rem(u, 5)], q2_r.at[j], xpeer)

    def ax_copy(u, j):
        return rcopy(AF.at[j, 2 * c + xx], AF.at[j, 2 * c + xx], ox_s.at[lax.rem(u, 4)], ox_r.at[j], xpeer)

    def ax_recv(u, j):
        return rcopy(AF.at[j, 2 * c + xo], AF.at[j, 2 * c + xo], ox_s.at[lax.rem(u, 4)], ox_r.at[j], xpeer)

    def ad_copy(u, j):
        return rcopy(AF.at[j, pl.ds(2 * c, 2)], AF.at[j, pl.ds(2 * c, 2)], od_s.at[lax.rem(u, 3)], od_r.at[j], partner)

    def ad_recv(u, j):
        return rcopy(AF.at[j, pl.ds(2 * co, 2)], AF.at[j, pl.ds(2 * co, 2)], od_s.at[lax.rem(u, 3)], od_r.at[j], partner)

    def az_copy(k):
        return rcopy(AZ.at[2 * c + xx], AZ.at[2 * c + xx], az_s.at[k - 1], az_r.at[k - 1], {"tx": lax.rem(tx + k, 4)})

    def az_recv(k):
        src = lax.rem(tx + 4 - k, 4)
        block = AZ.at[2 * lax.rem(src, 2) + lax.div(src, 2)]
        return rcopy(block, block, az_s.at[k - 1], az_r.at[k - 1], partner)

    def dy_copy():
        return rcopy(DS, DR, dy_s.at[0], dy_r.at[0], ypeer)

    def stage0(u):
        half, j = lax.div(u, NJ), lax.rem(u, NJ)

        for first, last, sem in ((0, 2, 5), (2, 7, 6), (7, 9, 7)):
            @pl.when(u == first)
            def _(first=first, last=last, sem=sem):
                await_all(WA.at[pl.ds(2 * first, 2 * (last - first))], sem)

        slot = lax.rem(u, NP)
        n = NB[1 - half]
        for which in range(2):
            res = bdot(n, WA[2 * j + which]).astype(bf16)
            for b in range(4):
                MP[slot, b, which] = res[16 * b:16 * (b + 1), :]
        m1_copy(u, j).start()

    def stage1(u):
        j, slot = lax.rem(u, NJ), lax.rem(u, NP)
        m1_copy(u, j).wait_recv()
        MXS[lax.rem(u, 5)] = (MP[slot, 2 * c + xo].astype(f32) + MR1[j, xo].astype(f32)).astype(bf16)
        m2_copy(u, j).start()
        MR1[j, xx] = (MP[slot, 2 * c + xx].astype(f32) + MR1[j, xx].astype(f32)).astype(bf16)
        m1_copy(u, j).wait_send()

    def stage2(u):
        j = lax.rem(u, NJ)
        m2_copy(u, j).wait()
        tot = (MR1[j, xx].astype(f32) + MR2[j].astype(f32)).astype(bf16).astype(f32)
        gate, up = tot[0], tot[1]
        act = (gate * jax.nn.sigmoid(gate) * up).astype(bf16)

        @pl.when(u < NU - 1)
        def _():
            AF[j, 2 * c + xx] = act
            ax_copy(u, j).start()

        @pl.when(u == NU - 1)
        def _():
            AZ[2 * c + xx] = act
            for k in (2, 1, 3):
                az_copy(k).start()

    def stage3(u):
        j = lax.rem(u, NJ)
        ax_copy(u, j).wait_send()
        ax_recv(u, j).wait_recv()
        ad_copy(u, j).start()

    def stage4(u):
        j = lax.rem(u, NJ)

        @pl.when(u == 0)
        def _():
            wd_load().wait()

        ad_recv(u, j).wait_recv()
        a = jnp.concatenate([AF[j, b] for b in range(4)], axis=0)
        prod = bdot(a, WB[pl.ds(pl.multiple_of(j * CH, CH), CH), :])

        @pl.when(j == 0)
        def _():
            ACC[...] = prod

        @pl.when(j > 0)
        def _():
            ACC[...] += prod

        ad_copy(u, j).wait_send()

        @pl.when(u == NJ - 1)
        def _():
            DS[...] = ACC[...].astype(bf16)
            dy_copy().start()

    def step(t, carry):
        @pl.when(t == NJ - 3)
        def _():
            residual(0)

        @pl.when(t == NJ)
        def _():
            norm2(0)

        @pl.when(t < NU)
        def _():
            stage0(t)

        for lag, stage in ((L1, stage1), (L2, stage2), (L3, stage3), (L4, stage4)):
            @pl.when((t >= lag) & (t < NU + lag - (lag >= L3)))
            def _(lag=lag, stage=stage):
                stage(t - lag)

        return carry

    lax.fori_loop(0, NU + L4 - 1, step, 0)

    h_store = pltpu.make_async_copy(HB.at[0], h_hbm, lsem.at[1])
    h_store.start()
    dy_copy().wait_recv()
    for k in range(1, 4):
        az_recv(k).wait_recv()
    last = bdot(jnp.concatenate([AZ[b] for b in range(4)], axis=0), WB[(NJ - 1) * CH:NJ * CH, :])
    mlp = (ACC[...] + last + DR[...].astype(f32)).astype(bf16)
    ay_copy(0, 0).wait_send()
    ay_copy(0, 1).wait_send()
    AO[0] = mlp
    m_store = pltpu.make_async_copy(AO.at[0], m_hbm, lsem.at[0])
    m_store.start()
    st1_all().wait_send()
    st1_total().wait_send()
    x_send.wait_send()
    ay_copy(1, 0).wait_send()
    ay_copy(1, 1).wait_send()
    for r in range(2):
        st2_all(r).wait_send()
    dy_copy().wait_send()
    for k in range(1, 4):
        az_copy(k).wait_send()
    h_store.wait()
    m_store.wait()


def layer_fn(x_blk, w_q, w_k, w_v, w_o, w_gate, w_up, w_down):
    bf16, f32 = jnp.bfloat16, jnp.float32
    cos_t, sin_t = rotary_tables()
    vm, dma = pltpu.VMEM, pltpu.SemaphoreType.DMA
    scratch = [
        vm((2 * NJ, D1, CH), bf16),
        vm((6 * D1, D1), bf16),
        vm((2, S, D1), bf16),
        vm((2, S, D1), bf16),
        vm((2, S, D1), bf16),
        vm((6, 8, 128), f32),
        vm((2, 4, 8, 128), f32),
        vm((3, 2, S, GW), bf16),
        vm((2, 3, 2, S, GW), bf16),
        vm((2, 3, 2, S, GW), bf16),
        vm((3, S, GW), bf16),
        vm((2, 3, S, GW), bf16),
        vm((2, 2, 2, S, GW), bf16),
        vm((2, S, D1), bf16),
        vm((2, S, D1), bf16),
        vm((NP, 4, 2, 16, CH), bf16),
        vm((NJ, 2, 2, 16, CH), bf16),
        vm((5, 2, 16, CH), bf16),
        vm((NJ, 2, 16, CH), bf16),
        vm((NJ, 4, 16, CH), bf16),
        vm((4, 16, CH), bf16),
        vm((S, D1), f32),
        vm((S, D1), bf16),
        vm((S, D1), bf16),
        vm((S, HEAD_DIM), f32),
        vm((S, HEAD_DIM), f32),
        vm((GH, S, S), bf16),
        dma((9,)), dma((3,)), dma((1,)), dma((1,)),
        dma((2,)), dma((2,)), dma((2,)), dma((2,)),
        dma((3,)), dma((6,)), dma((5,)), dma((NJ,)),
        dma((4,)), dma((NJ,)), dma((3,)), dma((NJ,)), dma((2,)), dma((2,)), dma((2, 2)), dma((2, 2)),
        dma((3,)), dma((3,)), dma((1,)), dma((1,)),
    ]
    h, mlp = pl.pallas_call(
        kernel,
        out_shape=[jax.ShapeDtypeStruct((S, D1), bf16)] * 2,
        in_specs=[pl.BlockSpec(memory_space=pl.ANY)] * 10,
        out_specs=[pl.BlockSpec(memory_space=pl.ANY)] * 2,
        scratch_shapes=scratch,
        compiler_params=pltpu.CompilerParams(collective_id=0, has_side_effects=True, vmem_limit_bytes=67_043_328),
    )(x_blk.reshape(S, D1), w_q, w_k, w_v, w_o, w_gate, w_up, w_down, jnp.asarray(cos_t), jnp.asarray(sin_t))
    return (h.astype(f32) + mlp.astype(f32)).astype(bf16).reshape(x_blk.shape)


def solution(mesh):
    act_spec = P(("dp", "ty"), None, "tx")
    col_spec = P("tx", "ty")
    row_spec = P("ty", "tx")
    return jax.shard_map(
        layer_fn,
        mesh=mesh,
        in_specs=(act_spec, col_spec, col_spec, col_spec, row_spec, col_spec, col_spec, row_spec),
        out_specs=act_spec,
        check_vma=False,
    )
```

```python
import functools

import jax
import jax.numpy as jnp
import numpy as np
from jax import lax
from jax.experimental import pallas as pl
from jax.experimental.pallas import tpu as pltpu
from jax.sharding import PartitionSpec as P

HEAD_DIM = 128
EPS = 1e-5
THETA = 10000.0
MESH = pl.DeviceIdType.MESH

S = 64
D1 = 1280
DFULL = 5120
GH = 5
GW = GH * HEAD_DIM
CH = 768
NJ = 9
NU = 2 * NJ
NP = 3
PARTS = ((0, 384), (384, 256))
L1, L2, L3, L4 = 1, 4, 6, 8


def rotary_tables():
    half = HEAD_DIM // 2
    inv_freq = np.float32(THETA) ** (np.float32(-2.0) * np.arange(half, dtype=np.float32) / np.float32(HEAD_DIM))
    angles = np.arange(S, dtype=np.float32)[:, None] * inv_freq.astype(np.float32)[None, :]
    cos_t = np.cos(angles.astype(np.float64)).astype(np.float32)
    sin_t = np.sin(angles.astype(np.float64)).astype(np.float32)
    return np.concatenate([cos_t, cos_t], axis=1), np.concatenate([-sin_t, sin_t], axis=1)


def bdot(a, b):
    return jnp.dot(a, b, preferred_element_type=jnp.float32)


def kernel(
    x_hbm, wq, wk, wv, wo, wg, wu, wd, cos_hbm, sin_hbm, y_hbm,
    WA, WB, XB, NB, HB, ST1, ST2, PS, PO, R1, XS, R2, OF, AO, AR,
    MP, MR1, MXS, MR2, AF, AZ, ACC, DS, DR, COS, SIN, PR,
    wsem, lsem, xg_s, xg_r, st1_s, st1_r, st2_s, st2_r,
    q1_s, q1_r, q2_s, q2_r, ox_s, ox_r, od_s, od_r, oe_s, oe_r, ay_s, ay_r,
    az_s, az_r, dy_s, dy_r,
):
    f32, bf16 = jnp.float32, jnp.bfloat16
    ty = lax.axis_index("ty")
    tx = lax.axis_index("tx")
    c = lax.rem(tx, 2)
    xx = lax.div(tx, 2)
    co, xo = 1 - c, 1 - xx
    tyo = 1 - ty
    partner = {"tx": 2 * xx + co}
    xpeer = {"tx": 2 * xo + c}
    ypeer = {"ty": tyo}

    def rcopy(src, dst, ss, rs, dev):
        return pltpu.make_async_remote_copy(src_ref=src, dst_ref=dst, send_sem=ss, recv_sem=rs, device_id=dev, device_id_type=MESH)

    x_load = pltpu.make_async_copy(x_hbm, XB.at[0], lsem.at[0])
    x_load.start()
    cos_load = pltpu.make_async_copy(cos_hbm, COS, lsem.at[1])
    sin_load = pltpu.make_async_copy(sin_hbm, SIN, lsem.at[2])

    barrier = pltpu.get_barrier_semaphore()
    for k in range(1, 4):
        pl.semaphore_signal(barrier, inc=1, device_id={"tx": lax.rem(tx + k, 4)}, device_id_type=MESH)
    pl.semaphore_signal(barrier, inc=1, device_id=ypeer, device_id_type=MESH)

    def qkv_load(m, half):
        src = (wq, wk, wv)[m].at[:, pl.ds(half * D1, D1)]
        return pltpu.make_async_copy(src, WB.at[pl.ds((2 * m + half) * D1, D1), :], wsem.at[m])

    def wo_load(i):
        kh, wide = i % 2, i // 2
        if wide == 0:
            return pltpu.make_async_copy(wo.at[pl.ds(kh * D1, D1), pl.ds(0, CH)], WA.at[14 + i], wsem.at[3])
        return pltpu.make_async_copy(wo.at[pl.ds(kh * D1, D1), pl.ds(CH, D1 - CH)], WA.at[14 + i, :, pl.ds(0, D1 - CH)], wsem.at[4])

    def gu_load(j, which):
        group = 5 if j < 2 else 6 if j < 7 else 7
        return pltpu.make_async_copy((wg, wu)[which].at[:, pl.ds(j * CH, CH)], WA.at[2 * j + which], wsem.at[group])

    def wd_load():
        return pltpu.make_async_copy(wd, WB.at[pl.ds(0, NJ * CH), :], wsem.at[8])

    def await_all(ref, sem):
        pltpu.make_async_copy(ref, ref, wsem.at[sem]).wait()

    for m in range(3):
        for half in range(2):
            qkv_load(m, half).start()
    cos_load.start()
    sin_load.start()

    eye = lax.broadcasted_iota(jnp.int32, (S, 128), 0) == lax.broadcasted_iota(jnp.int32, (S, 128), 1)
    row8 = lax.broadcasted_iota(jnp.int32, (8, 128), 0)

    def stats_tile(v):
        s = jnp.sum(v, axis=1, keepdims=True)
        q = jnp.sum(v * v, axis=1, keepdims=True)
        srow = jnp.sum(jnp.where(eye, s, 0.0), axis=0, keepdims=True)
        qrow = jnp.sum(jnp.where(eye, q, 0.0), axis=0, keepdims=True)
        return jnp.where(row8 == 0, srow, jnp.where(row8 == 1, qrow, 0.0))

    def normalize(v, tot):
        mean = tot[0:1, :] / DFULL
        var = tot[1:2, :] / DFULL - mean * mean
        rstd = lax.rsqrt(var + EPS)
        mean_c = jnp.sum(jnp.where(eye, mean, 0.0), axis=1, keepdims=True)
        rstd_c = jnp.sum(jnp.where(eye, rstd, 0.0), axis=1, keepdims=True)
        return ((v - mean_c) * rstd_c).astype(bf16)

    x_load.wait()
    x_own = XB[0].astype(f32)
    ST1[0] = stats_tile(x_own)
    pl.semaphore_wait(barrier, 4)

    def st1_copy(k):
        return rcopy(ST1.at[0], ST1.at[k], st1_s.at[0], st1_r.at[0], {"tx": lax.rem(tx + k, 4)})

    def st1_all():
        ref = ST1.at[pl.ds(1, 3)]
        return rcopy(ref, ref, st1_s.at[0], st1_r.at[0], partner)

    def st1_total():
        return rcopy(ST1.at[4], ST1.at[5], st1_s.at[1], st1_r.at[1], ypeer)

    for k in range(1, 4):
        st1_copy(k).start()
    x_send = rcopy(XB.at[0], XB.at[1], xg_s.at[0], xg_r.at[0], ypeer)
    x_send.start()

    def q1_copy(r, m):
        return rcopy(PS.at[m], R1.at[r, m], q1_s.at[m], q1_r.at[3 * r + m], partner)

    def q2_copy(r, m, p=0):
        lanes = pl.ds(*(PARTS[p] if r == 1 and m == 2 else (0, GW)))
        return rcopy(XS.at[m, :, lanes], R2.at[r, m, :, lanes], q2_s.at[m + p], q2_r.at[3 * r + m + p], xpeer)

    def qkv_dot(r, m, half):
        return bdot(NB[r], WB[pl.ds(pl.multiple_of((2 * m + half) * D1, D1), D1), :]).astype(bf16)

    def put_send(r, m, res):
        if r == 1:
            q1_copy(0, m).wait_send()
        PS[m, 0] = res[:, :GW]
        PS[m, 1] = res[:, GW:]
        q1_copy(r, m).start()

    def put_keep(r, m, res):
        PO[r, m, 0] = res[:, :GW]
        PO[r, m, 1] = res[:, GW:]

    def qkv_mm(r, m):
        if r == 0:
            await_all(WB.at[pl.ds(2 * m * D1, 2 * D1), :], m)
        put_send(r, m, qkv_dot(r, m, co))
        put_keep(r, m, qkv_dot(r, m, c))

    def qkv_mm_both(r, m):
        sent, kept = qkv_dot(r, m, co), qkv_dot(r, m, c)
        put_send(r, m, sent)
        put_keep(r, m, kept)

    def qkv_s1(r, m):
        q1_copy(r, m).wait_recv()
        if r == 1:
            q2_copy(0, m).wait_send()
        XS[m] = (PO[r, m, xo].astype(f32) + R1[r, m, xo].astype(f32)).astype(bf16)
        q2_copy(r, m).start()
        if r == 1 and m == 2:
            q2_copy(r, m, 1).start()

    causal = lax.broadcasted_iota(jnp.int32, (S, S), 0) >= lax.broadcasted_iota(jnp.int32, (S, S), 1)

    def o_lanes(r, p):
        return pl.ds(*(PARTS[p] if r == 1 else (0, GW)))

    def ox_copy(r, p=0):
        ref = OF.at[r, c, xx, :, o_lanes(r, p)]
        return rcopy(ref, ref, ox_s.at[r + p], ox_r.at[r + p], xpeer)

    def ox_recv(r, p=0):
        ref = OF.at[r, c, xo, :, o_lanes(r, p)]
        return rcopy(ref, ref, ox_s.at[r + p], ox_r.at[r + p], xpeer)

    def od_copy(r, p=0):
        ref = OF.at[r, c, xo, :, o_lanes(r, p)]
        return rcopy(ref, ref, od_s.at[r + p], od_r.at[r + p], partner)

    def od_recv(r, p=0):
        ref = OF.at[r, co, xo, :, o_lanes(r, p)]
        return rcopy(ref, ref, od_s.at[r + p], od_r.at[r + p], partner)

    def oe_copy(r):
        return rcopy(OF.at[r, c, xx], OF.at[r, c, xx], oe_s.at[r], oe_r.at[r], partner)

    def oe_recv(r):
        return rcopy(OF.at[r, co, xx], OF.at[r, co, xx], oe_s.at[r], oe_r.at[r], partner)

    def total(r, m, lanes):
        return (PO[r, m, xx, :, lanes].astype(f32) + R1[r, m, xx, :, lanes].astype(f32) + R2[r, m, :, lanes].astype(f32)).astype(bf16)

    def scores(r):
        if r == 0:
            cos_load.wait()
            sin_load.wait()
        cos_t, sin_t = COS[...], SIN[...]
        q2_copy(r, 0).wait_recv()
        q2_copy(r, 1).wait_recv()

        def rot(m, h):
            v = total(r, m, pl.ds(h * HEAD_DIM, HEAD_DIM)).astype(f32)
            return (v * cos_t + pltpu.roll(v, HEAD_DIM // 2, 1) * sin_t).astype(bf16)

        qs, ks = [rot(0, h) for h in range(GH)], [rot(1, h) for h in range(GH)]
        sc = [lax.dot_general(q, k, (((1,), (1,)), ((), ())), preferred_element_type=f32) * HEAD_DIM ** -0.5 for q, k in zip(qs, ks)]
        sc = [jnp.where(causal, v, -1e30) for v in sc]
        ex = [jnp.exp(v - jnp.max(v, axis=1, keepdims=True)) for v in sc]
        for h in range(GH):
            PR[h] = (ex[h] / jnp.sum(ex[h], axis=1, keepdims=True)).astype(bf16)

    def values(r, p=0):
        q2_copy(r, 2, p).wait_recv()
        off, size = PARTS[p] if r == 1 else (0, GW)
        heads = range(off // HEAD_DIM, (off + size) // HEAD_DIM)
        outs = [bdot(PR[h], total(r, 2, pl.ds(h * HEAD_DIM, HEAD_DIM))).astype(bf16) for h in heads]
        OF[r, c, xx, :, off:off + size] = jnp.concatenate(outs, axis=1)
        ox_copy(r, p).start()
        if r == 0 or p == 1:
            oe_copy(r).start()

    def o_forward(r, p=0):
        ox_recv(r, p).wait_recv()
        od_copy(r, p).start()

    def ay_copy(r, p):
        cols = pl.ds(*((0, CH), (CH, D1 - CH))[p])
        return rcopy(AO.at[r, :, cols], AR.at[1 - r, :, cols], ay_s.at[r, p], ay_r.at[1 - r, p], ypeer)

    def out_block(r, cb, xb, first=False):
        o, rows = OF[r, cb, xb], pl.ds(pl.multiple_of(xb * GW, GW), GW)
        for cols, prod in ((slice(0, CH), bdot(o, WA[14 + cb, rows, :])), (slice(CH, D1), bdot(o, WA[16 + cb, rows, : D1 - CH]))):
            ACC[:, cols] = prod if first else ACC[:, cols] + prod

    def out_last(r):
        od_recv(r).wait_recv()
        if r == 1:
            od_recv(r, 1).wait_recv()
        o, rows = OF[r, co, xo], pl.ds(pl.multiple_of(xo * GW, GW), GW)
        AO[r, :, :CH] = (ACC[:, :CH] + bdot(o, WA[14 + co, rows, :])).astype(bf16)
        ay_copy(r, 0).start()
        AO[r, :, CH:] = (ACC[:, CH:] + bdot(o, WA[16 + co, rows, : D1 - CH])).astype(bf16)
        ay_copy(r, 1).start()

    st1_all().wait_recv()
    sums = ST1[0] + ST1[1] + ST1[2] + ST1[3]
    ST1[4] = sums
    st1_total().start()
    NB[0] = normalize(x_own, sums)
    qkv_mm(0, 0)
    qkv_s1(0, 0)
    qkv_mm(0, 1)
    qkv_s1(0, 1)
    qkv_mm(0, 2)
    for i in range(4):
        wo_load(i).start()
    for j in range(7):
        gu_load(j, 0).start()
        gu_load(j, 1).start()
    x_send.wait_recv()
    st1_total().wait_recv()
    NB[1] = normalize(XB[1].astype(f32), ST1[5])
    qkv_s1(0, 2)
    qkv_mm(1, 0)
    qkv_s1(1, 0)
    scores(0)
    qkv_mm_both(1, 1)
    values(0)
    qkv_s1(1, 1)
    qkv_mm_both(1, 2)
    wd_load().start()
    qkv_s1(1, 2)
    await_all(WA.at[pl.ds(14, 2)], 3)
    await_all(WA.at[pl.ds(16, 2), :, pl.ds(0, D1 - CH)], 4)
    out_block(0, c, xx, True)
    o_forward(0)
    oe_recv(0).wait_recv()
    out_block(0, co, xx)
    out_block(0, c, xo)
    out_last(0)
    scores(1)
    values(1, 0)
    values(1, 1)
    out_block(1, c, xx, True)
    oe_recv(1).wait_recv()
    out_block(1, co, xx)
    o_forward(1, 0)
    o_forward(1, 1)
    out_block(1, c, xo)
    out_last(1)
    for j in range(7, NJ):
        gu_load(j, 0).start()
        gu_load(j, 1).start()

    def st2_copy(r, k):
        return rcopy(ST2.at[r, 0], ST2.at[r, k], st2_s.at[r], st2_r.at[r], {"tx": lax.rem(tx + k, 4)})

    def st2_all(r):
        ref = ST2.at[r, pl.ds(1, 3)]
        return rcopy(ref, ref, st2_s.at[r], st2_r.at[r], partner)

    def residual(r):
        ay_copy(1 - r, 0).wait_recv()
        ay_copy(1 - r, 1).wait_recv()
        attn = (AO[r].astype(f32) + AR[r].astype(f32)).astype(bf16)
        h = (XB[r].astype(f32) + attn.astype(f32)).astype(bf16)
        HB[r] = h
        ST2[r, 0] = stats_tile(h.astype(f32))
        for k in range(1, 4):
            st2_copy(r, k).start()

    def norm2(r):
        st2_all(r).wait_recv()
        NB[r] = normalize(HB[r].astype(f32), ST2[r, 0] + ST2[r, 1] + ST2[r, 2] + ST2[r, 3])

    residual(1)
    for m in range(3):
        q1_copy(1, m).wait_send()
        q2_copy(1, m).wait_send()
    q2_copy(1, 2, 1).wait_send()
    for r, p in ((0, 0), (1, 0), (1, 1)):
        ox_copy(r, p).wait_send()
        od_copy(r, p).wait_send()
    for r in range(2):
        oe_copy(r).wait_send()
    norm2(1)

    def m1_copy(u, j):
        return rcopy(MP.at[lax.rem(u, NP), pl.ds(2 * co, 2)], MR1.at[j], q1_s.at[lax.rem(u, NP)], q1_r.at[lax.rem(u, 5)], partner)

    def m2_copy(u, j):
        return rcopy(MXS.at[lax.rem(u, 5)], MR2.at[j], q2_s.at[lax.rem(u, 5)], q2_r.at[j], xpeer)

    def ax_copy(u, j):
        return rcopy(AF.at[j, 2 * c + xx], AF.at[j, 2 * c + xx], ox_s.at[lax.rem(u, 4)], ox_r.at[j], xpeer)

    def ax_recv(u, j):
        return rcopy(AF.at[j, 2 * c + xo], AF.at[j, 2 * c + xo], ox_s.at[lax.rem(u, 4)], ox_r.at[j], xpeer)

    def ad_copy(u, j):
        return rcopy(AF.at[j, pl.ds(2 * c, 2)], AF.at[j, pl.ds(2 * c, 2)], od_s.at[lax.rem(u, 3)], od_r.at[j], partner)

    def ad_recv(u, j):
        return rcopy(AF.at[j, pl.ds(2 * co, 2)], AF.at[j, pl.ds(2 * co, 2)], od_s.at[lax.rem(u, 3)], od_r.at[j], partner)

    def az_copy(k):
        return rcopy(AZ.at[2 * c + xx], AZ.at[2 * c + xx], az_s.at[k - 1], az_r.at[k - 1], {"tx": lax.rem(tx + k, 4)})

    def az_recv(k):
        src = lax.rem(tx + 4 - k, 4)
        block = AZ.at[2 * lax.rem(src, 2) + lax.div(src, 2)]
        return rcopy(block, block, az_s.at[k - 1], az_r.at[k - 1], partner)

    def dy_copy():
        return rcopy(DS, DR, dy_s.at[0], dy_r.at[0], ypeer)

    def stage0(u):
        half, j = lax.div(u, NJ), lax.rem(u, NJ)

        for first, last, sem in ((0, 2, 5), (2, 7, 6), (7, 9, 7)):
            @pl.when(u == first)
            def _(first=first, last=last, sem=sem):
                await_all(WA.at[pl.ds(2 * first, 2 * (last - first))], sem)

        slot = lax.rem(u, NP)
        n = NB[1 - half]
        for which in range(2):
            res = bdot(n, WA[2 * j + which]).astype(bf16)
            for b in range(4):
                MP[slot, b, which] = res[16 * b:16 * (b + 1), :]
        m1_copy(u, j).start()

    def stage1(u):
        j, slot = lax.rem(u, NJ), lax.rem(u, NP)
        m1_copy(u, j).wait_recv()
        MXS[lax.rem(u, 5)] = (MP[slot, 2 * c + xo].astype(f32) + MR1[j, xo].astype(f32)).astype(bf16)
        m2_copy(u, j).start()
        MR1[j, xx] = (MP[slot, 2 * c + xx].astype(f32) + MR1[j, xx].astype(f32)).astype(bf16)
        m1_copy(u, j).wait_send()

    def stage2(u):
        j = lax.rem(u, NJ)
        m2_copy(u, j).wait()
        tot = (MR1[j, xx].astype(f32) + MR2[j].astype(f32)).astype(bf16).astype(f32)
        gate, up = tot[0], tot[1]
        act = (gate * jax.nn.sigmoid(gate) * up).astype(bf16)

        @pl.when(u < NU - 1)
        def _():
            AF[j, 2 * c + xx] = act
            ax_copy(u, j).start()

        @pl.when(u == NU - 1)
        def _():
            AZ[2 * c + xx] = act
            for k in (2, 1, 3):
                az_copy(k).start()

    def stage3(u):
        j = lax.rem(u, NJ)
        ax_copy(u, j).wait_send()
        ax_recv(u, j).wait_recv()
        ad_copy(u, j).start()

    def stage4(u):
        j = lax.rem(u, NJ)

        @pl.when(u == 0)
        def _():
            wd_load().wait()

        ad_recv(u, j).wait_recv()
        a = jnp.concatenate([AF[j, b] for b in range(4)], axis=0)
        prod = bdot(a, WB[pl.ds(pl.multiple_of(j * CH, CH), CH), :])

        @pl.when(j == 0)
        def _():
            ACC[...] = prod

        @pl.when(j > 0)
        def _():
            ACC[...] += prod

        ad_copy(u, j).wait_send()

        @pl.when(u == NJ - 1)
        def _():
            DS[...] = ACC[...].astype(bf16)
            dy_copy().start()

    def step(t, carry):
        @pl.when(t == NJ - 3)
        def _():
            residual(0)

        @pl.when(t == NJ)
        def _():
            norm2(0)

        @pl.when(t < NU)
        def _():
            stage0(t)

        for lag, stage in ((L1, stage1), (L2, stage2), (L3, stage3), (L4, stage4)):
            @pl.when((t >= lag) & (t < NU + lag - (lag >= L3)))
            def _(lag=lag, stage=stage):
                stage(t - lag)

        return carry

    lax.fori_loop(0, NU + L4 - 1, step, 0)

    dy_copy().wait_recv()
    for k in range(1, 4):
        az_recv(k).wait_recv()
    last = bdot(jnp.concatenate([AZ[b] for b in range(4)], axis=0), WB[(NJ - 1) * CH:NJ * CH, :])
    mlp = (ACC[...] + last + DR[...].astype(f32)).astype(bf16)
    ay_copy(0, 0).wait_send()
    ay_copy(0, 1).wait_send()
    AO[0] = (HB[0].astype(f32) + mlp.astype(f32)).astype(bf16)
    y_store = pltpu.make_async_copy(AO.at[0], y_hbm, lsem.at[0])
    y_store.start()
    st1_all().wait_send()
    st1_total().wait_send()
    x_send.wait_send()
    ay_copy(1, 0).wait_send()
    ay_copy(1, 1).wait_send()
    for r in range(2):
        st2_all(r).wait_send()
    dy_copy().wait_send()
    for k in range(1, 4):
        az_copy(k).wait_send()
    y_store.wait()


def layer_fn(x_blk, w_q, w_k, w_v, w_o, w_gate, w_up, w_down):
    bf16, f32 = jnp.bfloat16, jnp.float32
    cos_t, sin_t = rotary_tables()
    vm, dma = pltpu.VMEM, pltpu.SemaphoreType.DMA
    scratch = [
        vm((2 * NJ, D1, CH), bf16),
        vm((6 * D1, D1), bf16),
        vm((2, S, D1), bf16),
        vm((2, S, D1), bf16),
        vm((2, S, D1), bf16),
        vm((6, 8, 128), f32),
        vm((2, 4, 8, 128), f32),
        vm((3, 2, S, GW), bf16),
        vm((2, 3, 2, S, GW), bf16),
        vm((2, 3, 2, S, GW), bf16),
        vm((3, S, GW), bf16),
        vm((2, 3, S, GW), bf16),
        vm((2, 2, 2, S, GW), bf16),
        vm((2, S, D1), bf16),
        vm((2, S, D1), bf16),
        vm((NP, 4, 2, 16, CH), bf16),
        vm((NJ, 2, 2, 16, CH), bf16),
        vm((5, 2, 16, CH), bf16),
        vm((NJ, 2, 16, CH), bf16),
        vm((NJ, 4, 16, CH), bf16),
        vm((4, 16, CH), bf16),
        vm((S, D1), f32),
        vm((S, D1), bf16),
        vm((S, D1), bf16),
        vm((S, HEAD_DIM), f32),
        vm((S, HEAD_DIM), f32),
        vm((GH, S, S), bf16),
        dma((9,)), dma((3,)), dma((1,)), dma((1,)),
        dma((2,)), dma((2,)), dma((2,)), dma((2,)),
        dma((3,)), dma((6,)), dma((5,)), dma((NJ,)),
        dma((4,)), dma((NJ,)), dma((3,)), dma((NJ,)), dma((2,)), dma((2,)), dma((2, 2)), dma((2, 2)),
        dma((3,)), dma((3,)), dma((1,)), dma((1,)),
    ]
    y = pl.pallas_call(
        kernel,
        out_shape=jax.ShapeDtypeStruct((S, D1), bf16),
        in_specs=[pl.BlockSpec(memory_space=pl.ANY)] * 10,
        out_specs=pl.BlockSpec(memory_space=pl.ANY),
        scratch_shapes=scratch,
        compiler_params=pltpu.CompilerParams(collective_id=0, has_side_effects=True, vmem_limit_bytes=67_043_328),
    )(x_blk.reshape(S, D1), w_q, w_k, w_v, w_o, w_gate, w_up, w_down, jnp.asarray(cos_t), jnp.asarray(sin_t))
    return y.reshape(x_blk.shape)


def solution(mesh):
    act_spec = P(("dp", "ty"), None, "tx")
    col_spec = P("tx", "ty")
    row_spec = P("ty", "tx")
    return jax.shard_map(
        layer_fn,
        mesh=mesh,
        in_specs=(act_spec, col_spec, col_spec, col_spec, row_spec, col_spec, col_spec, row_spec),
        out_specs=act_spec,
        check_vma=False,
    )
```

```python
import functools

import jax
import jax.numpy as jnp
import numpy as np
from jax import lax
from jax.experimental import pallas as pl
from jax.experimental.pallas import tpu as pltpu
from jax.sharding import PartitionSpec as P

HEAD_DIM = 128
EPS = 1e-5
THETA = 10000.0
MESH = pl.DeviceIdType.MESH

S = 64
D1 = 1280
DFULL = 5120
GH = 5
GW = GH * HEAD_DIM
CH = 768
NJ = 9
NU = 2 * NJ
NP = 3
PARTS = ((0, 384), (384, 256))
NA = 11
L1, L2, L3, L4 = 1, 4, 8, 10


def rotary_tables():
    half = HEAD_DIM // 2
    inv_freq = np.float32(THETA) ** (np.float32(-2.0) * np.arange(half, dtype=np.float32) / np.float32(HEAD_DIM))
    angles = np.arange(S, dtype=np.float32)[:, None] * inv_freq.astype(np.float32)[None, :]
    cos_t = np.cos(angles.astype(np.float64)).astype(np.float32)
    sin_t = np.sin(angles.astype(np.float64)).astype(np.float32)
    return np.concatenate([cos_t, cos_t], axis=1), np.concatenate([-sin_t, sin_t], axis=1)


def bdot(a, b):
    return jnp.dot(a, b, preferred_element_type=jnp.float32)


def kernel(
    x_hbm, wq, wk, wv, wo, wg, wu, wd, cos_hbm, sin_hbm, y_hbm,
    WA, WB, XB, NB, HB, ST1, ST2, PS, PO, R1, XS, R2, OF, AO, AR,
    MP, MR1, MXS, MR2, AF, AZ, ACC, DS, DR, COS, SIN, PR,
    wsem, lsem, xg_s, xg_r, st1_s, st1_r, st2_s, st2_r,
    q1_s, q1_r, q2_s, q2_r, ox_s, ox_r, od_s, od_r, oe_s, oe_r, ay_s, ay_r,
    az_s, az_r, dy_s, dy_r,
):
    f32, bf16 = jnp.float32, jnp.bfloat16
    ty = lax.axis_index("ty")
    tx = lax.axis_index("tx")
    c = lax.rem(tx, 2)
    xx = lax.div(tx, 2)
    co, xo = 1 - c, 1 - xx
    tyo = 1 - ty
    partner = {"tx": 2 * xx + co}
    xpeer = {"tx": 2 * xo + c}
    ypeer = {"ty": tyo}

    def rcopy(src, dst, ss, rs, dev):
        return pltpu.make_async_remote_copy(src_ref=src, dst_ref=dst, send_sem=ss, recv_sem=rs, device_id=dev, device_id_type=MESH)

    x_load = pltpu.make_async_copy(x_hbm, XB.at[0], lsem.at[0])
    x_load.start()
    cos_load = pltpu.make_async_copy(cos_hbm, COS, lsem.at[1])
    sin_load = pltpu.make_async_copy(sin_hbm, SIN, lsem.at[2])

    barrier = pltpu.get_barrier_semaphore()
    for k in range(1, 4):
        pl.semaphore_signal(barrier, inc=1, device_id={"tx": lax.rem(tx + k, 4)}, device_id_type=MESH)
    pl.semaphore_signal(barrier, inc=1, device_id=ypeer, device_id_type=MESH)

    def qkv_load(m, half):
        src = (wq, wk, wv)[m].at[:, pl.ds(half * D1, D1)]
        return pltpu.make_async_copy(src, WB.at[pl.ds((2 * m + half) * D1, D1), :], wsem.at[m])

    def wo_load(i):
        kh, wide = i % 2, i // 2
        if wide == 0:
            return pltpu.make_async_copy(wo.at[pl.ds(kh * D1, D1), pl.ds(0, CH)], WA.at[14 + i], wsem.at[3])
        return pltpu.make_async_copy(wo.at[pl.ds(kh * D1, D1), pl.ds(CH, D1 - CH)], WA.at[14 + i, :, pl.ds(0, D1 - CH)], wsem.at[4])

    def gu_load(j, which):
        group = 5 if j < 2 else 6 if j < 7 else 7
        return pltpu.make_async_copy((wg, wu)[which].at[:, pl.ds(j * CH, CH)], WA.at[2 * j + which], wsem.at[group])

    def wd_load():
        return pltpu.make_async_copy(wd, WB.at[pl.ds(0, NJ * CH), :], wsem.at[8])

    def await_all(ref, sem):
        pltpu.make_async_copy(ref, ref, wsem.at[sem]).wait()

    for m in range(3):
        for half in range(2):
            qkv_load(m, half).start()
    cos_load.start()
    sin_load.start()

    eye = lax.broadcasted_iota(jnp.int32, (S, 128), 0) == lax.broadcasted_iota(jnp.int32, (S, 128), 1)
    row8 = lax.broadcasted_iota(jnp.int32, (8, 128), 0)

    def stats_tile(v):
        s = jnp.sum(v, axis=1, keepdims=True)
        q = jnp.sum(v * v, axis=1, keepdims=True)
        srow = jnp.sum(jnp.where(eye, s, 0.0), axis=0, keepdims=True)
        qrow = jnp.sum(jnp.where(eye, q, 0.0), axis=0, keepdims=True)
        return jnp.where(row8 == 0, srow, jnp.where(row8 == 1, qrow, 0.0))

    def normalize(v, tot):
        mean = tot[0:1, :] / DFULL
        var = tot[1:2, :] / DFULL - mean * mean
        rstd = lax.rsqrt(var + EPS)
        mean_c = jnp.sum(jnp.where(eye, mean, 0.0), axis=1, keepdims=True)
        rstd_c = jnp.sum(jnp.where(eye, rstd, 0.0), axis=1, keepdims=True)
        return ((v - mean_c) * rstd_c).astype(bf16)

    x_load.wait()
    x_own = XB[0].astype(f32)
    ST1[0] = stats_tile(x_own)
    pl.semaphore_wait(barrier, 4)

    def st1_copy(k):
        return rcopy(ST1.at[0], ST1.at[k], st1_s.at[0], st1_r.at[0], {"tx": lax.rem(tx + k, 4)})

    def st1_all():
        ref = ST1.at[pl.ds(1, 3)]
        return rcopy(ref, ref, st1_s.at[0], st1_r.at[0], partner)

    def st1_total():
        return rcopy(ST1.at[4], ST1.at[5], st1_s.at[1], st1_r.at[1], ypeer)

    for k in range(1, 4):
        st1_copy(k).start()
    x_send = rcopy(XB.at[0], XB.at[1], xg_s.at[0], xg_r.at[0], ypeer)
    x_send.start()

    def q1_copy(r, m):
        return rcopy(PS.at[m], R1.at[r, m], q1_s.at[m], q1_r.at[3 * r + m], partner)

    def q2_copy(r, m, p=0):
        lanes = pl.ds(*(PARTS[p] if r == 1 and m == 2 else (0, GW)))
        return rcopy(XS.at[m, :, lanes], R2.at[r, m, :, lanes], q2_s.at[m + p], q2_r.at[3 * r + m + p], xpeer)

    def qkv_dot(r, m, half):
        return bdot(NB[r], WB[pl.ds(pl.multiple_of((2 * m + half) * D1, D1), D1), :]).astype(bf16)

    def put_send(r, m, res):
        if r == 1:
            q1_copy(0, m).wait_send()
        PS[m, 0] = res[:, :GW]
        PS[m, 1] = res[:, GW:]
        q1_copy(r, m).start()

    def put_keep(r, m, res):
        PO[r, m, 0] = res[:, :GW]
        PO[r, m, 1] = res[:, GW:]

    def qkv_mm(r, m):
        if r == 0:
            await_all(WB.at[pl.ds(2 * m * D1, 2 * D1), :], m)
        put_send(r, m, qkv_dot(r, m, co))
        put_keep(r, m, qkv_dot(r, m, c))

    def qkv_mm_both(r, m):
        sent, kept = qkv_dot(r, m, co), qkv_dot(r, m, c)
        put_send(r, m, sent)
        put_keep(r, m, kept)

    def qkv_s1(r, m):
        q1_copy(r, m).wait_recv()
        if r == 1:
            q2_copy(0, m).wait_send()
        XS[m] = (PO[r, m, xo].astype(f32) + R1[r, m, xo].astype(f32)).astype(bf16)
        q2_copy(r, m).start()
        if r == 1 and m == 2:
            q2_copy(r, m, 1).start()

    causal = lax.broadcasted_iota(jnp.int32, (S, S), 0) >= lax.broadcasted_iota(jnp.int32, (S, S), 1)

    def o_lanes(r, p):
        return pl.ds(*(PARTS[p] if r == 1 else (0, GW)))

    def ox_copy(r, p=0):
        ref = OF.at[r, c, xx, :, o_lanes(r, p)]
        return rcopy(ref, ref, ox_s.at[r + p], ox_r.at[r + p], xpeer)

    def ox_recv(r, p=0):
        ref = OF.at[r, c, xo, :, o_lanes(r, p)]
        return rcopy(ref, ref, ox_s.at[r + p], ox_r.at[r + p], xpeer)

    def od_copy(r, p=0):
        ref = OF.at[r, c, xo, :, o_lanes(r, p)]
        return rcopy(ref, ref, od_s.at[r + p], od_r.at[r + p], partner)

    def od_recv(r, p=0):
        ref = OF.at[r, co, xo, :, o_lanes(r, p)]
        return rcopy(ref, ref, od_s.at[r + p], od_r.at[r + p], partner)

    def oe_copy(r):
        return rcopy(OF.at[r, c, xx], OF.at[r, c, xx], oe_s.at[r], oe_r.at[r], partner)

    def oe_recv(r):
        return rcopy(OF.at[r, co, xx], OF.at[r, co, xx], oe_s.at[r], oe_r.at[r], partner)

    def total(r, m, lanes):
        return (PO[r, m, xx, :, lanes].astype(f32) + R1[r, m, xx, :, lanes].astype(f32) + R2[r, m, :, lanes].astype(f32)).astype(bf16)

    def scores(r):
        if r == 0:
            cos_load.wait()
            sin_load.wait()
        cos_t, sin_t = COS[...], SIN[...]
        q2_copy(r, 0).wait_recv()
        q2_copy(r, 1).wait_recv()

        def rot(m, h):
            v = total(r, m, pl.ds(h * HEAD_DIM, HEAD_DIM)).astype(f32)
            return (v * cos_t + pltpu.roll(v, HEAD_DIM // 2, 1) * sin_t).astype(bf16)

        qs, ks = [rot(0, h) for h in range(GH)], [rot(1, h) for h in range(GH)]
        sc = [lax.dot_general(q, k, (((1,), (1,)), ((), ())), preferred_element_type=f32) * HEAD_DIM ** -0.5 for q, k in zip(qs, ks)]
        sc = [jnp.where(causal, v, -1e30) for v in sc]
        ex = [jnp.exp(v - jnp.max(v, axis=1, keepdims=True)) for v in sc]
        for h in range(GH):
            PR[h] = (ex[h] / jnp.sum(ex[h], axis=1, keepdims=True)).astype(bf16)

    def values(r, p=0):
        q2_copy(r, 2, p).wait_recv()
        off, size = PARTS[p] if r == 1 else (0, GW)
        heads = range(off // HEAD_DIM, (off + size) // HEAD_DIM)
        outs = [bdot(PR[h], total(r, 2, pl.ds(h * HEAD_DIM, HEAD_DIM))).astype(bf16) for h in heads]
        OF[r, c, xx, :, off:off + size] = jnp.concatenate(outs, axis=1)
        ox_copy(r, p).start()
        if r == 0 or p == 1:
            oe_copy(r).start()

    def o_forward(r, p=0):
        ox_recv(r, p).wait_recv()
        od_copy(r, p).start()

    def ay_copy(r, p):
        cols = pl.ds(*((0, CH), (CH, D1 - CH))[p])
        return rcopy(AO.at[r, :, cols], AR.at[1 - r, :, cols], ay_s.at[r, p], ay_r.at[1 - r, p], ypeer)

    def out_block(r, cb, xb, first=False):
        o, rows = OF[r, cb, xb], pl.ds(pl.multiple_of(xb * GW, GW), GW)
        for cols, prod in ((slice(0, CH), bdot(o, WA[14 + cb, rows, :])), (slice(CH, D1), bdot(o, WA[16 + cb, rows, : D1 - CH]))):
            ACC[:, cols] = prod if first else ACC[:, cols] + prod

    def out_last(r):
        od_recv(r).wait_recv()
        if r == 1:
            od_recv(r, 1).wait_recv()
        o, rows = OF[r, co, xo], pl.ds(pl.multiple_of(xo * GW, GW), GW)
        AO[r, :, :CH] = (ACC[:, :CH] + bdot(o, WA[14 + co, rows, :])).astype(bf16)
        ay_copy(r, 0).start()
        AO[r, :, CH:] = (ACC[:, CH:] + bdot(o, WA[16 + co, rows, : D1 - CH])).astype(bf16)
        ay_copy(r, 1).start()

    st1_all().wait_recv()
    sums = ST1[0] + ST1[1] + ST1[2] + ST1[3]
    ST1[4] = sums
    st1_total().start()
    NB[0] = normalize(x_own, sums)
    qkv_mm(0, 0)
    qkv_s1(0, 0)
    qkv_mm(0, 1)
    qkv_s1(0, 1)
    qkv_mm(0, 2)
    for i in range(4):
        wo_load(i).start()
    for j in range(7):
        gu_load(j, 0).start()
        gu_load(j, 1).start()
    x_send.wait_recv()
    st1_total().wait_recv()
    NB[1] = normalize(XB[1].astype(f32), ST1[5])
    qkv_s1(0, 2)
    qkv_mm(1, 0)
    qkv_s1(1, 0)
    scores(0)
    qkv_mm_both(1, 1)
    values(0)
    qkv_s1(1, 1)
    qkv_mm_both(1, 2)
    wd_load().start()
    qkv_s1(1, 2)
    await_all(WA.at[pl.ds(14, 2)], 3)
    await_all(WA.at[pl.ds(16, 2), :, pl.ds(0, D1 - CH)], 4)
    out_block(0, c, xx, True)
    o_forward(0)
    oe_recv(0).wait_recv()
    out_block(0, co, xx)
    out_block(0, c, xo)
    out_last(0)
    scores(1)
    values(1, 0)
    values(1, 1)
    out_block(1, c, xx, True)
    oe_recv(1).wait_recv()
    out_block(1, co, xx)
    o_forward(1, 0)
    o_forward(1, 1)
    out_block(1, c, xo)
    out_last(1)
    for j in range(7, NJ):
        gu_load(j, 0).start()
        gu_load(j, 1).start()

    def st2_copy(r, k):
        return rcopy(ST2.at[r, 0], ST2.at[r, k], st2_s.at[r], st2_r.at[r], {"tx": lax.rem(tx + k, 4)})

    def st2_all(r):
        ref = ST2.at[r, pl.ds(1, 3)]
        return rcopy(ref, ref, st2_s.at[r], st2_r.at[r], partner)

    def residual(r):
        ay_copy(1 - r, 0).wait_recv()
        ay_copy(1 - r, 1).wait_recv()
        attn = (AO[r].astype(f32) + AR[r].astype(f32)).astype(bf16)
        h = (XB[r].astype(f32) + attn.astype(f32)).astype(bf16)
        HB[r] = h
        ST2[r, 0] = stats_tile(h.astype(f32))
        for k in range(1, 4):
            st2_copy(r, k).start()

    def norm2(r):
        st2_all(r).wait_recv()
        NB[r] = normalize(HB[r].astype(f32), ST2[r, 0] + ST2[r, 1] + ST2[r, 2] + ST2[r, 3])

    residual(1)
    for m in range(3):
        q1_copy(1, m).wait_send()
        q2_copy(1, m).wait_send()
    q2_copy(1, 2, 1).wait_send()
    for r, p in ((0, 0), (1, 0), (1, 1)):
        ox_copy(r, p).wait_send()
        od_copy(r, p).wait_send()
    for r in range(2):
        oe_copy(r).wait_send()
    norm2(1)

    def m1_copy(u, j):
        return rcopy(MP.at[lax.rem(u, NP), pl.ds(2 * co, 2)], MR1.at[j], q1_s.at[lax.rem(u, NP)], q1_r.at[lax.rem(u, 5)], partner)

    def m2_copy(u, j):
        return rcopy(MXS.at[lax.rem(u, 5)], MR2.at[j], q2_s.at[lax.rem(u, 5)], q2_r.at[j], xpeer)

    def ax_copy(u, j):
        return rcopy(AF.at[lax.rem(u, NA), 2 * c + xx], AF.at[lax.rem(u, NA), 2 * c + xx], ox_s.at[lax.rem(u, 5)], ox_r.at[j], xpeer)

    def ax_recv(u, j):
        return rcopy(AF.at[lax.rem(u, NA), 2 * c + xo], AF.at[lax.rem(u, NA), 2 * c + xo], ox_s.at[lax.rem(u, 5)], ox_r.at[j], xpeer)

    def ad_copy(u, j):
        return rcopy(AF.at[lax.rem(u, NA), pl.ds(2 * c, 2)], AF.at[lax.rem(u, NA), pl.ds(2 * c, 2)], od_s.at[lax.rem(u, 3)], od_r.at[j], partner)

    def ad_recv(u, j):
        return rcopy(AF.at[lax.rem(u, NA), pl.ds(2 * co, 2)], AF.at[lax.rem(u, NA), pl.ds(2 * co, 2)], od_s.at[lax.rem(u, 3)], od_r.at[j], partner)

    def az_copy(k):
        return rcopy(AZ.at[2 * c + xx], AZ.at[2 * c + xx], az_s.at[k - 1], az_r.at[k - 1], {"tx": lax.rem(tx + k, 4)})

    def az_recv(k):
        src = lax.rem(tx + 4 - k, 4)
        block = AZ.at[2 * lax.rem(src, 2) + lax.div(src, 2)]
        return rcopy(block, block, az_s.at[k - 1], az_r.at[k - 1], partner)

    def dy_copy():
        return rcopy(DS, DR, dy_s.at[0], dy_r.at[0], ypeer)

    def stage0(u):
        half, j = lax.div(u, NJ), lax.rem(u, NJ)

        for first, last, sem in ((0, 2, 5), (2, 7, 6), (7, 9, 7)):
            @pl.when(u == first)
            def _(first=first, last=last, sem=sem):
                await_all(WA.at[pl.ds(2 * first, 2 * (last - first))], sem)

        slot = lax.rem(u, NP)
        n = NB[1 - half]
        for which in range(2):
            res = bdot(n, WA[2 * j + which]).astype(bf16)
            for b in range(4):
                MP[slot, b, which] = res[16 * b:16 * (b + 1), :]
        m1_copy(u, j).start()

    def stage1(u):
        j, slot = lax.rem(u, NJ), lax.rem(u, NP)
        m1_copy(u, j).wait_recv()
        MXS[lax.rem(u, 5)] = (MP[slot, 2 * c + xo].astype(f32) + MR1[j, xo].astype(f32)).astype(bf16)
        m2_copy(u, j).start()
        MR1[j, xx] = (MP[slot, 2 * c + xx].astype(f32) + MR1[j, xx].astype(f32)).astype(bf16)
        m1_copy(u, j).wait_send()

    def stage2(u):
        j = lax.rem(u, NJ)
        m2_copy(u, j).wait()
        tot = (MR1[j, xx].astype(f32) + MR2[j].astype(f32)).astype(bf16).astype(f32)
        gate, up = tot[0], tot[1]
        act = (gate * jax.nn.sigmoid(gate) * up).astype(bf16)

        @pl.when(u < NU - 1)
        def _():
            AF[lax.rem(u, NA), 2 * c + xx] = act
            ax_copy(u, j).start()

        @pl.when(u == NU - 1)
        def _():
            AZ[2 * c + xx] = act
            for k in (2, 1, 3):
                az_copy(k).start()

    def stage3(u):
        j = lax.rem(u, NJ)
        ax_copy(u, j).wait_send()
        ax_recv(u, j).wait_recv()
        ad_copy(u, j).start()

    def stage4(u):
        j = lax.rem(u, NJ)

        @pl.when(u == 0)
        def _():
            wd_load().wait()

        ad_recv(u, j).wait_recv()
        a = jnp.concatenate([AF[lax.rem(u, NA), b] for b in range(4)], axis=0)
        prod = bdot(a, WB[pl.ds(pl.multiple_of(j * CH, CH), CH), :])

        @pl.when(j == 0)
        def _():
            ACC[...] = prod

        @pl.when(j > 0)
        def _():
            ACC[...] += prod

        ad_copy(u, j).wait_send()

        @pl.when(u == NJ - 1)
        def _():
            DS[...] = ACC[...].astype(bf16)
            dy_copy().start()

    def step(t, carry):
        @pl.when(t == NJ - 3)
        def _():
            residual(0)

        @pl.when(t == NJ)
        def _():
            norm2(0)

        @pl.when(t < NU)
        def _():
            stage0(t)

        for lag, stage in ((L1, stage1), (L2, stage2), (L3, stage3), (L4, stage4)):
            @pl.when((t >= lag) & (t < NU + lag - (lag >= L3)))
            def _(lag=lag, stage=stage):
                stage(t - lag)

        return carry

    lax.fori_loop(0, NU + L4 - 1, step, 0)

    dy_copy().wait_recv()
    for k in range(1, 4):
        az_recv(k).wait_recv()
    last = bdot(jnp.concatenate([AZ[b] for b in range(4)], axis=0), WB[(NJ - 1) * CH:NJ * CH, :])
    mlp = (ACC[...] + last + DR[...].astype(f32)).astype(bf16)
    ay_copy(0, 0).wait_send()
    ay_copy(0, 1).wait_send()
    AO[0] = (HB[0].astype(f32) + mlp.astype(f32)).astype(bf16)
    y_store = pltpu.make_async_copy(AO.at[0], y_hbm, lsem.at[0])
    y_store.start()
    st1_all().wait_send()
    st1_total().wait_send()
    x_send.wait_send()
    ay_copy(1, 0).wait_send()
    ay_copy(1, 1).wait_send()
    for r in range(2):
        st2_all(r).wait_send()
    dy_copy().wait_send()
    for k in range(1, 4):
        az_copy(k).wait_send()
    y_store.wait()


def layer_fn(x_blk, w_q, w_k, w_v, w_o, w_gate, w_up, w_down):
    bf16, f32 = jnp.bfloat16, jnp.float32
    cos_t, sin_t = rotary_tables()
    vm, dma = pltpu.VMEM, pltpu.SemaphoreType.DMA
    scratch = [
        vm((2 * NJ, D1, CH), bf16),
        vm((6 * D1, D1), bf16),
        vm((2, S, D1), bf16),
        vm((2, S, D1), bf16),
        vm((2, S, D1), bf16),
        vm((6, 8, 128), f32),
        vm((2, 4, 8, 128), f32),
        vm((3, 2, S, GW), bf16),
        vm((2, 3, 2, S, GW), bf16),
        vm((2, 3, 2, S, GW), bf16),
        vm((3, S, GW), bf16),
        vm((2, 3, S, GW), bf16),
        vm((2, 2, 2, S, GW), bf16),
        vm((2, S, D1), bf16),
        vm((2, S, D1), bf16),
        vm((NP, 4, 2, 16, CH), bf16),
        vm((NJ, 2, 2, 16, CH), bf16),
        vm((5, 2, 16, CH), bf16),
        vm((NJ, 2, 16, CH), bf16),
        vm((NA, 4, 16, CH), bf16),
        vm((4, 16, CH), bf16),
        vm((S, D1), f32),
        vm((S, D1), bf16),
        vm((S, D1), bf16),
        vm((S, HEAD_DIM), f32),
        vm((S, HEAD_DIM), f32),
        vm((GH, S, S), bf16),
        dma((9,)), dma((3,)), dma((1,)), dma((1,)),
        dma((2,)), dma((2,)), dma((2,)), dma((2,)),
        dma((3,)), dma((6,)), dma((5,)), dma((NJ,)),
        dma((5,)), dma((NJ,)), dma((3,)), dma((NJ,)), dma((2,)), dma((2,)), dma((2, 2)), dma((2, 2)),
        dma((3,)), dma((3,)), dma((1,)), dma((1,)),
    ]
    y = pl.pallas_call(
        kernel,
        out_shape=jax.ShapeDtypeStruct((S, D1), bf16),
        in_specs=[pl.BlockSpec(memory_space=pl.ANY)] * 10,
        out_specs=pl.BlockSpec(memory_space=pl.ANY),
        scratch_shapes=scratch,
        compiler_params=pltpu.CompilerParams(collective_id=0, has_side_effects=True, vmem_limit_bytes=67_043_328),
    )(x_blk.reshape(S, D1), w_q, w_k, w_v, w_o, w_gate, w_up, w_down, jnp.asarray(cos_t), jnp.asarray(sin_t))
    return y.reshape(x_blk.shape)


def solution(mesh):
    act_spec = P(("dp", "ty"), None, "tx")
    col_spec = P("tx", "ty")
    row_spec = P("ty", "tx")
    return jax.shard_map(
        layer_fn,
        mesh=mesh,
        in_specs=(act_spec, col_spec, col_spec, col_spec, row_spec, col_spec, col_spec, row_spec),
        out_specs=act_spec,
        check_vma=False,
    )
```
